32 devices in a mesh: box: 32 (over z, y, x, core).
Axes of the slice: x: 2, y: 2, z: 4, core: 2. Of those that a mesh axis runs over, the one named last changes fastest.
Arguments:
- basis_vector: float32 [16, 131072], P(None, 'box'), may hold values from -600 to 600
- diagonal: float32 [131072], P('box'), may hold values from 0.25 to 2
- coords: int32 [2, 131072], P(None, 'box'), may hold values from 0 to 4095
- phase_scale: int32 [1], replicated, may hold values from 1 to 8190
- sketch_rows: int32 [131072], P('box'), may hold values from 0 to 2047
- sketch_signs: int32 [131072], P('box'), may hold values from 0 to 1
Outputs:
- new_basis: float32 [16, 131072], P(None, 'box')
- sketch: float32 [16, 2048], replicated
- arnoldi: float32 [2, 16], replicated
The draws below stay inside these ranges and needn't reach their ends.
All inputs are finite; a program needn't handle non-finite values.
Results may differ from the reference program's by a relative error of at most 0.00019.
Values sent between devices are 32-bit elements; how exact they have to be, the bound alone decides.
A program may use at most 64 MiB of HBM per device.

```python
import math
import jax
import jax.numpy as jnp
from jax import lax

RANK = 16
WIDTH = 32
LEAF = 32
GRID = 4096
SKETCH = 2048
NRHS = 16
BOX_DEV = 128
NPTS = 131072
SECTIONS = 5
N_BOX = 32


def draw_basis_vector(key, part):
    key_scale, key_normal = jax.random.split(key, 2)
    position = jnp.arange(NPTS, dtype=jnp.float32) / NPTS
    row_scale = jnp.exp(jax.random.uniform(key_scale, (NPTS,), jnp.float32, 0.0, math.log(10.0))) * jnp.exp(position * math.log(3.0))
    normal_part = jax.random.normal(key_normal, (NRHS, NPTS), jnp.float32)
    return jnp.clip(normal_part, -4.0, 4.0) * row_scale[None, :]


def with_ends(drawn, own_key, low, largest):
    spot = [jax.random.randint(jax.random.fold_in(own_key, axis), (), 0, length) for axis, length in enumerate(drawn.shape)]
    widest = drawn.shape.index(max(drawn.shape))
    next_to = spot[:widest] + [(spot[widest] + 1) % drawn.shape[widest]] + spot[widest + 1:]
    return drawn.at[tuple(spot)].set(low).at[tuple(next_to)].set(largest)


def levels(own_key, shape, pieces, low, top_value):
    gain, own = 1.0, jax.random.fold_in(own_key, 6)
    for dim, shards_of in pieces:
        steps = jnp.exp(jax.random.uniform(jax.random.fold_in(own, dim), (shards_of,), jnp.float32, low / len(pieces), top_value / len(pieces)))
        gain = gain * jnp.repeat(steps, shape[dim] // shards_of).reshape([-1 if axis == dim else 1 for axis in range(len(shape))])
    return gain


def setup_inputs(seed: int = 0) -> dict:
    keys = jax.random.split(jax.random.key(seed), 7)
    basis_vector = draw_basis_vector(jax.random.fold_in(keys[6], 71), 0)
    diagonal = jnp.clip(jnp.exp(math.log(2.0) - 2.0794415 * jax.random.uniform(keys[1], (NPTS,), jnp.float32) ** levels(keys[1], (NPTS,), ((0, 32),), -0.2, 0.2)), 0.25, 2.0)
    coords = with_ends(jax.random.randint(keys[2], (2, NPTS), 0, GRID), jax.random.fold_in(keys[2], 1), 0, GRID - 1).astype(jnp.int32)
    phase_scale = jax.random.randint(keys[3], (1,), 1, 8191).astype(jnp.int32)
    sketch_rows = with_ends(jax.random.randint(keys[4], (NPTS,), 0, SKETCH), jax.random.fold_in(keys[4], 1), 0, SKETCH - 1).astype(jnp.int32)
    sketch_signs = with_ends(jax.random.randint(keys[5], (NPTS,), 0, 2), jax.random.fold_in(keys[5], 1), 0, 1).astype(jnp.int32)
    return {"basis_vector": basis_vector, "diagonal": diagonal, "coords": coords, "phase_scale": phase_scale, "sketch_rows": sketch_rows, "sketch_signs": sketch_signs}


modulus = 8191
epsilon = 1e-06

def leaf_table(coords, phase_scale):
    scale_mod = phase_scale[0] % modulus
    freq = jnp.arange(RANK, dtype=jnp.int32)
    freq_first = freq % 4 + 1
    freq_second = freq // 4 + 1
    linear = (freq_first[:, None] * coords[0][None, :] + freq_second[:, None] * coords[1][None, :]) % modulus
    phase = scale_mod * linear % modulus
    angle = phase.astype(jnp.float32) * (2.0 * math.pi / modulus)
    return jnp.concatenate([jnp.cos(angle), jnp.sin(angle)], 0) * (1.0 / math.sqrt(LEAF))

def translations(box_ids, segment_num, phase_scale):
    scale_mod = phase_scale[0] % modulus
    base_key = (box_ids * 37 + 101 * segment_num) % (modulus - 1) + 1
    unit_phase = scale_mod * base_key % modulus
    indices = jnp.arange(WIDTH, dtype=jnp.int32)
    prod_a = (indices[:, None] + 1) * (indices[None, :] + 2) % modulus
    prod_b = (indices[:, None] + 3) * (indices[None, :] + 1) % modulus
    phase_a = prod_a[:, :, None] * unit_phase[None, None, :] % modulus
    phase_b = (prod_b[:, :, None] * unit_phase[None, None, :] + 4096) % modulus
    factor = 2.0 * math.pi / modulus
    ident = jnp.eye(WIDTH, dtype=jnp.float32)[:, :, None]
    own_map = 0.85 * ident + 0.35 / math.sqrt(WIDTH) * jnp.cos(phase_a.astype(jnp.float32) * factor)
    cross_map = 0.6 / math.sqrt(WIDTH) * jnp.cos(phase_b.astype(jnp.float32) * factor)
    return (own_map, cross_map)

def reference(basis_vector, diagonal, coords, phase_scale, sketch_rows, sketch_signs):
    highest = lax.Precision.HIGHEST
    columns = basis_vector.shape[0]
    points = basis_vector.shape[1]
    box_count = points // LEAF
    leaf_map = leaf_table(coords, phase_scale)
    leaf_boxes = leaf_map.reshape(WIDTH, box_count, LEAF)
    blocks = basis_vector.reshape(columns, box_count, LEAF)
    coeffs = jnp.einsum('wbs,qbs->wqb', leaf_boxes, blocks, precision=highest)
    coeffs = coeffs.reshape(WIDTH, columns, N_BOX, BOX_DEV)
    box_ids = jnp.arange(box_count, dtype=jnp.int32)
    for segment_num in range(SECTIONS):
        stride = 2 ** segment_num
        grouped = coeffs.reshape(WIDTH, columns, N_BOX // (2 * stride), 2, stride, BOX_DEV)
        partner = grouped[:, :, :, ::-1].reshape(WIDTH, columns, N_BOX, BOX_DEV)
        own_map, cross_map = translations(box_ids, segment_num, phase_scale)
        own_map = own_map.reshape(WIDTH, WIDTH, N_BOX, BOX_DEV)
        cross_map = cross_map.reshape(WIDTH, WIDTH, N_BOX, BOX_DEV)
        coeffs = jnp.einsum('wvdg,vqdg->wqdg', own_map, coeffs, precision=highest) + jnp.einsum('wvdg,vqdg->wqdg', cross_map, partner, precision=highest)
    target_coef = coeffs.reshape(WIDTH, columns, box_count)
    applied = jnp.einsum('wbs,wqb->qbs', leaf_boxes, target_coef, precision=highest).reshape(columns, points)
    image = diagonal[None, :] * basis_vector + applied
    inner_vw = lax.optimization_barrier(jnp.mean(basis_vector * image, axis=1))
    square = lax.optimization_barrier(jnp.mean(basis_vector * basis_vector, axis=1)) + epsilon
    projection = inner_vw / square
    residual = image - projection[:, None] * basis_vector
    spread = jnp.sqrt(lax.optimization_barrier(jnp.mean(residual * residual, axis=1)) + epsilon)
    new_basis = residual / spread[:, None]
    sign_values = (2 * sketch_signs - 1).astype(jnp.float32)
    signed = new_basis * sign_values[None, :]
    sketch = jnp.zeros((columns, SKETCH), jnp.float32).at[:, sketch_rows].add(signed) * math.sqrt(SKETCH / points)
    arnoldi = jnp.stack([projection, spread])
    return (new_basis, sketch, arnoldi)
```

```python
import functools
import math

import jax
import jax.numpy as jnp
import numpy as np
from jax import lax
from jax.experimental import pallas as pl
from jax.experimental.pallas import tpu as pltpu
from jax.sharding import PartitionSpec as P

WIDTH = 32
LEAF = 32
SKETCH = 2048
LANES = 128
HIGH = 8
LOW = SKETCH // HIGH
MODULUS = 8191
EPSILON = 1e-06
MESH = pl.DeviceIdType.MESH
F32 = jnp.float32
BF16 = jnp.bfloat16


def sine_series():
    node = np.cos((np.arange(400) + 0.5) * np.pi / 800)
    basis = np.stack([node ** (2 * i) for i in range(6)], 1)
    exact = np.sin(np.pi * node * 4096 / MODULUS) / node
    return np.linalg.lstsq(basis, exact, rcond=None)[0]


SERIES = sine_series()


def remainder(n):
    return n - jnp.floor(n * (1.0 / MODULUS) + 0.5) * float(MODULUS)


def half_sine(n, gain):
    t = remainder(n) * (1.0 / 4096)
    z = t * t
    total = z * float(SERIES[5] * gain) + float(SERIES[4] * gain)
    for c in SERIES[3::-1]:
        total = total * z + float(c * gain)
    return total * t


def scaled_cos(n, amplitude):
    s = half_sine(n, math.sqrt(2.0 * amplitude))
    return amplitude - s * s


def scaled_sin(n, amplitude):
    return scaled_cos(n - 0.25 * MODULUS, amplitude)


def fold(p):
    return (p & MODULUS) + lax.shift_right_logical(p, 13)


def kernel(devices, stages, total_points, scale_ref, v_ref, coords_ref, diag_ref, rows_ref, signs_ref,
           nb_ref, sketch_ref, arn_ref, raw, pts, leaf, mats, kk, cbuf, part, tbuf, work, onehot, skb, ski,
           a_send, a_recv, b_send, b_recv, sum_send, sum_recv, rs_send, rs_recv, ag_recv, own_chunk,
           a_ss, a_rs, b_ss, b_rs, s_ss, s_rs, r_ss, r_rs, g_ss, g_rs):
    me = lax.axis_index("box")
    columns = nb_ref.shape[0]
    halves = columns // 8
    barrier = pltpu.get_barrier_semaphore()

    @pl.loop(1, devices)
    def _(i):
        pl.semaphore_signal(barrier, inc=1, device_id=(lax.rem(me + i, devices),), device_id_type=MESH)

    lane = lax.broadcasted_iota(jnp.int32, (8, LANES), 1)
    sub = lax.broadcasted_iota(jnp.int32, (8, LANES), 0)
    scale = lax.rem(scale_ref[0], MODULUS)

    for r in range(LANES // 4):
        here = slice(LANES * r, LANES * (r + 1))
        for h in range(halves):
            raw[pl.ds(256 * h + r, 8, stride=32), :] = v_ref[8 * h:8 * h + 8, here]
        pair = coords_ref[:, here].astype(F32)
        raw[columns * 32 + r:columns * 32 + r + 1, :] = pair[0:1]
        raw[columns * 32 + 32 + r:columns * 32 + 33 + r, :] = pair[1:2]
    raw[(columns + 2) * 32:(columns + 3) * 32, :] = diag_ref[...]
    raw[(columns + 3) * 32:(columns + 4) * 32, :] = rows_ref[...].astype(F32)
    raw[(columns + 4) * 32:(columns + 5) * 32, :] = signs_ref[...].astype(F32)
    raw[(columns + 5) * 32:(columns + 8) * 32, :] = jnp.zeros((96, LANES), F32)
    for i in range((columns + 8) // 4):
        flipped = raw[LANES * i:LANES * (i + 1), :].T
        tbuf[0] = flipped
        for j in range(4):
            pts[4 * i + j] = jnp.concatenate(
                [tbuf[0, 32 * g:32 * g + 32, 32 * j:32 * j + 32] for g in range(4)], axis=1)

    def exact_phase(row):
        return fold(pts[columns + row].astype(jnp.int32) * scale).astype(F32)

    work[0] = exact_phase(0)
    work[1] = exact_phase(1)
    fx = (sub % 4 + 1).astype(F32)
    fy = (sub // 4 + 1).astype(F32)
    unit = 1.0 / math.sqrt(LEAF)

    @pl.loop(0, LEAF)
    def _(s):
        px = work[0, pl.ds(s, 1), :]
        py = work[1, pl.ds(s, 1), :]
        for tile in range(2):
            n = fx * px + (fy + 2.0 * tile) * py
            leaf[s, 8 * tile:8 * tile + 8] = scaled_cos(n, unit)
            leaf[s, 16 + 8 * tile:24 + 8 * tile] = scaled_sin(n, unit)

    def gather_half(h):
        def gather(s, acc):
            tiles = [leaf[s, 8 * t:8 * t + 8] for t in range(4)]
            out = []
            for q in range(8):
                row = pts[8 * h + q, pl.ds(s, 1), :]
                for t in range(4):
                    out.append(acc[4 * q + t] + tiles[t] * row)
            return tuple(out)

        acc = lax.fori_loop(0, LEAF, gather, tuple(jnp.zeros((8, LANES), F32) for _ in range(32)), unroll=2)
        for q in range(8):
            for t in range(4):
                cbuf[pl.ds((8 * h + q) * 32 + 8 * t, 8), :] = acc[4 * q + t]

    blocks = 8 * WIDTH // LANES

    def make_maps(low, bits):
        group = 2 ** bits
        places = LANES // group
        mine = lax.rem(me // 2 ** low, group)
        spot = mine * places + lane % places
        box = 4 * (spot % 32) + spot // 32
        member = me + (lane // places - mine) * 2 ** low
        ident = (member * LANES + box) * 37

        @pl.loop(low, low + bits)
        def _(k):
            x = (ident + 101 * k).astype(F32)
            rest = x - jnp.floor(x * (1.0 / (MODULUS - 1))) * float(MODULUS - 1)
            rest = jnp.where(rest < 0.0, rest + float(MODULUS - 1), rest)
            rest = jnp.where(rest >= float(MODULUS - 1), rest - float(MODULUS - 1), rest)
            key = rest.astype(jnp.int32) + 1
            unit_phase = fold(fold(key * scale)).astype(F32)
            wide = sub.astype(F32)
            for m in range(2):
                amplitude = (0.35 if m == 0 else 0.6) / math.sqrt(WIDTH)
                first, second, offset = (1.0, 2.0, 0.0) if m == 0 else (3.0, 1.0, 4096.0)
                mid = unit_phase * (wide + (8.0 + first))
                far = unit_phase * (wide + (16.0 + first))

                @pl.loop(0, WIDTH, unroll=2)
                def _(v):
                    times = v.astype(F32) + second
                    step = scaled_cos(unit_phase * (8.0 * times), 2.0)
                    one = scaled_cos(mid * times + offset, amplitude)
                    two = scaled_cos(far * times + offset, amplitude)
                    mats[2 * k + m, v, 8:16] = one
                    mats[2 * k + m, v, 16:24] = two
                    mats[2 * k + m, v, 0:8] = step * one - two
                    mats[2 * k + m, v, 24:32] = step * two - one

    def exchange(send, recv, ss, rs, low, bits, action):
        group = 2 ** bits
        mine = lax.rem(me // 2 ** low, group)

        @pl.loop(1, group)
        def _(i):
            other = lax.rem(mine + i, group)
            here = other if action is finish_recv else mine
            copy = pltpu.make_async_remote_copy(
                send.at[other], recv.at[here], ss.at[other], rs.at[here],
                device_id=(me + (other - mine) * 2 ** low,), device_id_type=MESH)
            action(copy)
        return mine

    def pack(send, group, h):
        places = LANES // group
        for j in range(blocks):
            at = LANES * (blocks * h + j)
            tbuf[j] = cbuf[at:at + LANES, :].T
        for d in range(group):
            for j in range(blocks):
                send[d, places * j:places * (j + 1), :] = tbuf[j, places * d:places * (d + 1), :]

    def unpack(recv, group, h):
        places = LANES // group
        for j in range(blocks):
            for d in range(group):
                tbuf[j, places * d:places * (d + 1), :] = recv[d, places * j:places * (j + 1), :]
        for j in range(blocks):
            at = LANES * (blocks * h + j)
            cbuf[at:at + LANES, :] = tbuf[j].T

    def sketch_of(values, target, make):
        target[...] = jnp.zeros_like(target)

        @pl.loop(0, LEAF // 4)
        def _(c):
            pieces = []
            for i in range(4):
                s = 4 * c + i
                row = pts[columns + 3, pl.ds(s, 1), :]
                high = jnp.floor(row * (1.0 / LOW))
                if make:
                    low = (row - high * LOW).astype(jnp.int32)
                    ids = lax.broadcasted_iota(jnp.int32, (LOW, LANES), 0)
                    onehot[c, :, LANES * i:LANES * (i + 1)] = jnp.where(ids == low, 1.0, 0.0).astype(BF16)
                sign = 2.0 * pts[columns + 4, pl.ds(s, 1), :] - 1.0
                v = values(s) * sign
                top = v.astype(BF16)
                rest = (v - top.astype(F32)).astype(BF16)
                wide = jnp.broadcast_to(high, (columns, LANES))
                masks = [jnp.where(wide == float(g), 1.0, 0.0).astype(BF16) for g in range(HIGH)]
                pieces.append(jnp.concatenate([top * g for g in masks] + [rest * g for g in masks], axis=0))
            left = jnp.concatenate(pieces, axis=1)
            target[...] += lax.dot_general(left, onehot[c], (((1,), (1,)), ((), ())), preferred_element_type=F32)

    nbt = kk

    def start(copy):
        copy.start()

    def finish_recv(copy):
        copy.wait_recv()

    def finish_send(copy):
        copy.wait_send()

    for index, (low, bits) in enumerate(stages):
        group = 2 ** bits
        places = LANES // group

        def outward(h, action):
            at = halves * index + h
            return exchange(a_send.at[at], a_recv.at[at], a_ss.at[at], a_rs.at[at], low, bits, action)

        def homeward(h, action):
            at = halves * index + h
            return exchange(b_send.at[at], b_recv.at[at], b_ss.at[at], b_rs.at[at], low, bits, action)

        for h in range(halves):
            at = halves * index + h
            if index == 0:
                gather_half(h)
            pack(a_send.at[at], group, h)
            if index == 0 and h == 0:
                pl.semaphore_wait(barrier, devices - 1)
            mine = outward(h, start)
            a_recv[at, mine] = a_send[at, mine]
        make_maps(low, bits)
        if index == 0:
            for q in range(columns):
                for s in range(LEAF):
                    nbt[s, q:q + 1, :] = pts[q, s:s + 1, :]
            sketch_of(lambda s: nbt[s], skb, True)
        for h in range(halves):
            at = halves * index + h
            outward(h, finish_recv)
            unpack(a_recv.at[at], group, h)
            half = slice(256 * h, 256 * (h + 1))
            for k in range(low, low + bits):
                span = places * 2 ** (k - low)
                full = cbuf[half, :]
                wide = lax.broadcasted_iota(jnp.int32, full.shape, 1)
                part[half, :] = jnp.where((wide // span) % 2 == 0,
                                          pltpu.roll(full, LANES - span, 1), pltpu.roll(full, span, 1))

                def mix(v, acc):
                    own = [mats[2 * k, v, 8 * t:8 * t + 8] for t in range(4)]
                    cross = [mats[2 * k + 1, v, 8 * t:8 * t + 8] for t in range(4)]
                    out = []
                    for q in range(8):
                        row = cbuf[pl.ds((8 * h + q) * 32 + v, 1), :]
                        other = part[pl.ds((8 * h + q) * 32 + v, 1), :]
                        for t in range(4):
                            out.append(acc[4 * q + t] + own[t] * row + cross[t] * other)
                    return tuple(out)

                init = tuple(0.85 * cbuf[pl.ds((8 * h + q) * 32 + 8 * t, 8), :] for q in range(8) for t in range(4))
                acc = lax.fori_loop(0, WIDTH, mix, init, unroll=2)
                for q in range(8):
                    for t in range(4):
                        cbuf[pl.ds((8 * h + q) * 32 + 8 * t, 8), :] = acc[4 * q + t]
            pack(b_send.at[at], group, h)
            mine = homeward(h, start)
            b_recv[at, mine] = b_send[at, mine]
        for h in range(halves):
            outward(h, finish_send)
        for h in range(halves):
            homeward(h, finish_recv)
            unpack(b_recv.at[halves * index + h], group, h)
        for h in range(halves):
            homeward(h, finish_send)

    for c in range(LEAF // 8):
        def spread_out(w, acc):
            coef = [cbuf[pl.ds(8 * h * 32 + w, 8, stride=32), :] for h in range(halves)]
            out = []
            for s in range(8):
                row = leaf[8 * c + s, pl.ds(w, 1), :]
                for h in range(halves):
                    out.append(acc[halves * s + h] + coef[h] * row)
            return tuple(out)

        init = tuple(
            jnp.broadcast_to(pts[columns + 2, 8 * c + s:8 * c + s + 1, :], (8, LANES)) * nbt[8 * c + s, 8 * h:8 * h + 8]
            for s in range(8) for h in range(halves))
        acc = lax.fori_loop(0, WIDTH, spread_out, init, unroll=2)
        for s in range(8):
            for h in range(halves):
                part[(8 * c + s) * columns + 8 * h:(8 * c + s) * columns + 8 * h + 8, :] = acc[halves * s + h]

    inner = jnp.zeros((columns, LANES), F32)
    square, energy = inner, inner
    for s in range(LEAF):
        v, image = nbt[s], part[s * columns:(s + 1) * columns, :]
        inner, square, energy = inner + v * image, square + v * v, energy + image * image
    lane_q = lax.broadcasted_iota(jnp.int32, (columns, LANES), 1)
    row_q = lax.broadcasted_iota(jnp.int32, (columns, LANES), 0)
    packed = jnp.zeros((columns, LANES), F32)
    for i, value in enumerate((inner, square, energy)):
        packed = jnp.where(lane_q == row_q + columns * i, jnp.sum(value, axis=1, keepdims=True), packed)
    sum_send[...] = jnp.sum(packed, axis=0, keepdims=True)

    def to_all(source, recv, ss, rs, action):
        @pl.loop(1, devices)
        def _(i):
            other = lax.rem(me + i, devices)
            here = other if action is finish_recv else me
            action(pltpu.make_async_remote_copy(
                source(other), recv.at[here], ss.at[other], rs.at[here],
                device_id=(other,), device_id_type=MESH))

    to_all(lambda d: sum_send, sum_recv, s_ss, s_rs, start)
    sum_recv[me] = sum_send[...]
    sketch_of(lambda s: part[pl.ds(pl.multiple_of(s * columns, columns), columns), :], ski, False)
    to_all(lambda d: sum_send, sum_recv, s_ss, s_rs, finish_recv)
    totals = jnp.sum(sum_recv[...], axis=0)

    def column(i):
        picked = jnp.where(lane_q == row_q + columns * i, jnp.broadcast_to(totals, (columns, LANES)), 0.0)
        return jnp.broadcast_to(jnp.sum(picked, axis=1, keepdims=True) * (1.0 / total_points), (columns, LANES))

    inner_mean, square_mean, energy_mean = column(0), column(1), column(2)
    projection = inner_mean / (square_mean + EPSILON)
    energy = energy_mean - 2.0 * projection * inner_mean + projection * projection * square_mean
    spread = jnp.sqrt(energy + EPSILON)
    inverse = 1.0 / spread
    for i, value in enumerate((projection, spread)):
        arn_ref[i:i + 1, :] = jnp.sum(jnp.where(lane_q == row_q, value, 0.0), axis=0, keepdims=True)[:, :columns]

    rows_each = rs_send.shape[1]
    factor = math.sqrt(SKETCH / total_points)
    lowest = HIGH * columns
    part_tiles = LOW // LANES
    for n in range(devices):
        flat = n * rows_each
        tile, row = flat // 8, flat % 8
        strip, side = tile // part_tiles, tile % part_tiles
        top = strip * 8 + row
        q0 = top % columns
        cols = slice(side * LANES, (side + 1) * LANES)
        img = ski[top:top + rows_each, cols] + ski[lowest + top:lowest + top + rows_each, cols]
        bas = skb[top:top + rows_each, cols] + skb[lowest + top:lowest + top + rows_each, cols]
        rs_send[n] = (img - projection[q0:q0 + rows_each] * bas) * (factor * inverse[q0:q0 + rows_each])
    to_all(lambda d: rs_send.at[d], rs_recv, r_ss, r_rs, start)
    rs_recv[me] = rs_send[me]

    for s in range(LEAF):
        pts_rows = (part[s * columns:(s + 1) * columns, :] - projection * nbt[s]) * inverse
        nbt[s] = pts_rows
    for q in range(columns):
        for s in range(LEAF):
            pts[q, s:s + 1, :] = nbt[s, q:q + 1, :]
    for i in range(columns // 4):
        for j in range(4):
            for g in range(4):
                tbuf[0, 32 * g:32 * g + 32, 32 * j:32 * j + 32] = pts[4 * i + j, :, 32 * g:32 * g + 32]
        raw[LANES * i:LANES * (i + 1), :] = tbuf[0].T
    for r in range(LANES // 4):
        for h in range(halves):
            nb_ref[8 * h:8 * h + 8, LANES * r:LANES * (r + 1)] = raw[pl.ds(256 * h + r, 8, stride=32), :]

    to_all(lambda d: rs_send.at[d], rs_recv, r_ss, r_rs, finish_recv)
    own_chunk[...] = jnp.sum(rs_recv[...], axis=0)
    to_all(lambda d: own_chunk, ag_recv, g_ss, g_rs, start)
    ag_recv[me] = own_chunk[...]
    to_all(lambda d: sum_send, sum_recv, s_ss, s_rs, finish_send)
    to_all(lambda d: rs_send.at[d], rs_recv, r_ss, r_rs, finish_send)
    to_all(lambda d: own_chunk, ag_recv, g_ss, g_rs, finish_recv)
    for n in range(devices):
        flat = n * rows_each
        tile, row = flat // 8, flat % 8
        strip, side = tile // part_tiles, tile % part_tiles
        top = strip * 8 + row
        q0, high = top % columns, top // columns
        begin = high * LOW + side * LANES
        sketch_ref[q0:q0 + rows_each, begin:begin + LANES] = ag_recv[n]
    to_all(lambda d: own_chunk, ag_recv, g_ss, g_rs, finish_send)


def split(x):
    top = x.astype(BF16)
    return top, (x - top.astype(F32)).astype(BF16)


def tile_kernel(devices, total_points, scale_ref, v_ref, coords_ref, diag_ref, rows_ref, signs_ref,
                nb_ref, sketch_ref, arn_ref, small_send, small, vals, phases, steps, mats, leaf, state, coef,
                image, back, skb, ski, proj, sum_send, sum_recv, rb_send, rb_recv, ri_send, ri_recv, ag_recv,
                own_chunk, sems):
    me = lax.axis_index("box")
    columns = nb_ref.shape[0]
    sections = devices.bit_length() - 1
    per_tile = LANES // LEAF
    half = LANES // 2
    barrier = pltpu.get_barrier_semaphore()

    @pl.loop(1, devices)
    def _(i):
        pl.semaphore_signal(barrier, inc=1, device_id=(lax.rem(me + i, devices),), device_id_type=MESH)

    lane = lax.broadcasted_iota(jnp.int32, (8, LANES), 1)
    sub = lax.broadcasted_iota(jnp.int32, (8, LANES), 0)
    scale = lax.rem(scale_ref[0], MODULUS)

    def to_all(source, recv, which):
        @pl.loop(1, devices)
        def _(i):
            other = lax.rem(me + i, devices)
            pltpu.make_async_remote_copy(
                source(other), recv(me), sems.at[2 * which], sems.at[2 * which + 1],
                device_id=(other,), device_id_type=MESH).start()

    def finish(ref, which, side):
        pltpu.make_async_copy(ref, ref, sems.at[2 * which + side]).wait()

    def columns_at(ref, tile):
        return ref.at[:, pl.ds(pl.multiple_of(tile * LANES, LANES), LANES)]

    others = pl.ds(0, devices - 1)
    side_rows = 5
    side_part = pl.ds(0, side_rows)

    rows_f, signs_f = rows_ref[...].astype(F32), signs_ref[...].astype(F32)
    for e in range(devices):
        here = slice(e * LANES, (e + 1) * LANES)
        small_send[e, 0:2, :] = coords_ref[:, here].astype(F32)
        small_send[e, 2:3, :] = diag_ref[e:e + 1, :]
        small_send[e, 3:4, :] = rows_f[e:e + 1, :]
        small_send[e, 4:5, :] = signs_f[e:e + 1, :]
    pl.semaphore_wait(barrier, devices - 1)
    to_all(lambda d: small_send.at[d, side_part], lambda d: small.at[d, side_part], 0)
    to_all(lambda d: columns_at(v_ref, d), lambda d: vals.at[d], 1)
    small[me] = small_send[me]
    vals[me] = columns_at(v_ref, me)[...]

    spot = lane // LEAF
    inner_lane = (lane % LEAF).astype(F32)
    for k in range(sections):
        for g in range(devices // 8):
            ident = ((8 * g + sub) * LANES + per_tile * me + spot) * 37
            x = (ident + 101 * k).astype(F32)
            rest = x - jnp.floor(x * (1.0 / (MODULUS - 1))) * float(MODULUS - 1)
            rest = jnp.where(rest < 0.0, rest + float(MODULUS - 1), rest)
            rest = jnp.where(rest >= float(MODULUS - 1), rest - float(MODULUS - 1), rest)
            key = rest.astype(jnp.int32) + 1
            unit_phase = fold(fold(key * scale)).astype(F32)
            for m, second in enumerate((2.0, 1.0)):
                phi = remainder(unit_phase * (inner_lane + second))
                phases[2 * k + m, 8 * g:8 * g + 8, :] = phi
                steps[2 * k + m, 8 * g:8 * g + 8, :] = scaled_cos(8.0 * phi, 2.0)

    wide_sub = lax.broadcasted_iota(jnp.int32, (WIDTH, LANES), 0)
    wide_lane = lax.broadcasted_iota(jnp.int32, (WIDTH, LANES), 1)
    ident_part = jnp.where(wide_lane % WIDTH == wide_sub, 0.85, 0.0)
    sub_f = sub.astype(F32)
    for k in range(sections):
        stride = 2 ** k

        @pl.loop(0, devices // 2)
        def _(pair):
            first_tile = (pair // stride) * (2 * stride) + pair % stride
            for bit in range(2):
                d = first_tile + stride * bit
                for m in range(2):
                    amplitude = (0.35 if m == 0 else 0.6) / math.sqrt(WIDTH)
                    first, offset = (1.0, 0.0) if m == 0 else (3.0, 4096.0)
                    phi = phases[2 * k + m, pl.ds(d, 1), :]
                    step = steps[2 * k + m, pl.ds(d, 1), :]
                    one = scaled_cos(phi * (sub_f + (8.0 + first)) + offset, amplitude)
                    two = scaled_cos(phi * (sub_f + (16.0 + first)) + offset, amplitude)
                    full = jnp.concatenate([step * one - two, one, two, step * two - one], axis=0)
                    if m == 0:
                        full = full + ident_part
                    top, low = split(full)
                    begin = LANES * (bit if m == 0 else 1 - bit)
                    mats[k, pair, 64 * bit:64 * bit + 32, begin:begin + LANES] = top
                    mats[k, pair, 64 * bit + 32:64 * bit + 64, begin:begin + LANES] = low

    lanes_q = lax.broadcasted_iota(jnp.int32, (columns, LANES), 1)
    rows_q = lax.broadcasted_iota(jnp.int32, (columns, LANES), 0)

    def sketch_of(values, row_of, sign_of, target):
        target[...] = jnp.zeros_like(target)

        @pl.loop(0, devices // 4)
        def _(c):
            pieces, hots = [], []
            for i in range(4):
                s = 4 * c + i
                row = row_of(s)
                high = jnp.floor(row * (1.0 / LOW))
                low = (row - high * LOW).astype(jnp.int32)
                ids = lax.broadcasted_iota(jnp.int32, (LOW, LANES), 0)
                hots.append(jnp.where(ids == low, 1.0, 0.0).astype(BF16))
                sign = 2.0 * sign_of(s) - 1.0
                top, rest = split(values(s) * sign)
                wide = jnp.broadcast_to(high, (columns, LANES))
                masks = [jnp.where(wide == float(g), 1.0, 0.0).astype(BF16) for g in range(HIGH)]
                pieces.append(jnp.concatenate([top * g for g in masks] + [rest * g for g in masks], axis=0))
            left = jnp.concatenate(pieces, axis=1)
            hot = jnp.concatenate(hots, axis=1)
            target[...] += lax.dot_general(left, hot, (((1,), (1,)), ((), ())), preferred_element_type=F32)

    rows_each = rb_send.shape[1]
    factor = math.sqrt(SKETCH / total_points)
    lowest = HIGH * columns
    part_tiles = LOW // LANES

    def pieces_of(sk, send):
        for n in range(devices):
            flat = n * rows_each
            tile, row = flat // 8, flat % 8
            strip, side = tile // part_tiles, tile % part_tiles
            top = strip * 8 + row
            cols = slice(side * LANES, (side + 1) * LANES)
            send[n] = sk[top:top + rows_each, cols] + sk[lowest + top:lowest + top + rows_each, cols]

    sketch_of(lambda s: columns_at(v_ref, s)[...], lambda s: rows_ref[pl.ds(s, 1), :].astype(F32),
              lambda s: signs_ref[pl.ds(s, 1), :].astype(F32), skb)
    pieces_of(skb, rb_send)
    to_all(lambda d: rb_send.at[d], lambda d: rb_recv.at[d], 2)
    rb_recv[me] = rb_send[me]

    finish(small.at[others, side_part], 0, 1)
    fx = (sub % 4 + 1).astype(F32)
    fy = (sub // 4 + 1).astype(F32)
    unit = 1.0 / math.sqrt(LEAF)

    @pl.loop(0, devices)
    def _(d):
        pair = fold(small[d, 0:2, :].astype(jnp.int32) * scale).astype(F32)
        px, py = pair[0:1], pair[1:2]
        phases_of = [fx * px + (fy + 2.0 * t) * py for t in range(2)]
        full = jnp.concatenate([scaled_cos(n, unit) for n in phases_of] + [scaled_sin(n, unit) for n in phases_of], axis=0)
        top, low = split(full)
        leaf[d, 0:32] = top
        leaf[d, 32:64] = low

    finish(vals.at[others], 1, 1)

    point_masks = [jnp.where(lanes_q // LEAF == j, 1.0, 0.0).astype(BF16) for j in range(per_tile)]
    column_masks = [jnp.where((wide_lane % half) // columns == j, 1.0, 0.0).astype(BF16) for j in range(per_tile)]
    first_half = wide_lane < half

    def combine(o):
        s = o[0:32] + o[32:64]
        return s + pltpu.roll(s, half, 1)

    def expand(total):
        top = total.astype(BF16).astype(F32)
        y = jnp.where(first_half, top, total - top).astype(BF16)
        return jnp.concatenate([y * m for m in column_masks], axis=0)

    for d in range(devices):
        top, rest = split(vals[d])
        spread_v = jnp.concatenate([top * m for m in point_masks] + [rest * m for m in point_masks], axis=0)
        o = lax.dot_general(leaf[d], spread_v, (((1,), (1,)), ((), ())), preferred_element_type=F32)
        state[0, d] = expand(combine(o))

    for k in range(sections):
        stride = 2 ** k
        now = k % 2
        for pair in range(devices // 2):
            d0 = (pair // stride) * (2 * stride) + pair % stride
            d1 = d0 + stride
            x = jnp.concatenate([state[now, d0], state[now, d1]], axis=0)
            o = jnp.dot(mats[k, pair], x, preferred_element_type=F32)
            for d, part in ((d0, o[0:64]), (d1, o[64:128])):
                total = combine(part)
                if k == sections - 1:
                    coef[32 * d:32 * d + 32, :] = total
                else:
                    state[1 - now, d] = expand(total)

    tile_lane = lax.broadcasted_iota(jnp.int32, (half, 2 * LANES), 1)
    tile_masks = [jnp.where((tile_lane % LANES) // WIDTH == t, 1.0, 0.0).astype(BF16) for t in range(4)]
    zero = jnp.zeros((columns, LANES), F32)
    inner, square, energy = zero, zero, zero
    for g in range(devices // 4):
        flipped = coef[LANES * g:LANES * (g + 1), :].T
        top, rest = split(flipped[0:half])
        both = jnp.concatenate([top, rest], axis=1)
        left = jnp.concatenate([both * m for m in tile_masks], axis=0)
        tops = jnp.concatenate([leaf[4 * g + t, 0:32] for t in range(4)], axis=0)
        lows = jnp.concatenate([leaf[4 * g + t, 32:64] for t in range(4)], axis=0)
        right = jnp.concatenate([tops, lows], axis=1)
        o = jnp.dot(left, jnp.concatenate([right, right], axis=0), preferred_element_type=F32)
        o = o[:, 0:LANES] + o[:, LANES:2 * LANES]
        for t in range(4):
            d = 4 * g + t
            v = vals[d]
            img = jnp.broadcast_to(small[d, 2:3, :], (columns, LANES)) * v
            for j in range(per_tile):
                begin = half * t + columns * j
                img = img + jnp.where(lanes_q // LEAF == j, o[begin:begin + columns], 0.0)
            image[d] = img
            inner, square, energy = inner + v * img, square + v * v, energy + img * img

    packed = zero
    for i, value in enumerate((inner, square, energy)):
        packed = jnp.where(lanes_q == rows_q + columns * i, jnp.sum(value, axis=1, keepdims=True), packed)
    sum_send[...] = jnp.sum(packed, axis=0, keepdims=True)
    to_all(lambda d: sum_send, lambda d: sum_recv.at[d], 3)
    sum_recv[me] = sum_send[...]

    sketch_of(lambda d: image[d], lambda d: small[d, 3:4, :], lambda d: small[d, 4:5, :], ski)
    pieces_of(ski, ri_send)
    to_all(lambda d: ri_send.at[d], lambda d: ri_recv.at[d], 4)
    ri_recv[me] = ri_send[me]
    to_all(lambda d: image.at[d], lambda d: back.at[d], 5)
    back[me] = image[me]

    finish(small_send.at[others, side_part], 0, 0)
    finish(vals.at[others], 1, 0)
    finish(rb_send.at[others], 2, 0)
    finish(rb_recv.at[others], 2, 1)
    finish(sum_recv.at[others], 3, 0)
    finish(sum_recv.at[others], 3, 1)
    totals = jnp.sum(sum_recv[...], axis=0)

    def column(i):
        picked = jnp.where(lanes_q == rows_q + columns * i, jnp.broadcast_to(totals, (columns, LANES)), 0.0)
        return jnp.broadcast_to(jnp.sum(picked, axis=1, keepdims=True) * (1.0 / total_points), (columns, LANES))

    inner_mean, square_mean, energy_mean = column(0), column(1), column(2)
    projection = inner_mean / (square_mean + EPSILON)
    energy = energy_mean - 2.0 * projection * inner_mean + projection * projection * square_mean
    spread = jnp.sqrt(energy + EPSILON)
    inverse = 1.0 / spread
    for i, value in enumerate((projection, spread)):
        arn_ref[i:i + 1, :] = jnp.sum(jnp.where(lanes_q == rows_q, value, 0.0), axis=0, keepdims=True)[:, :columns]
    proj[0] = projection
    proj[1] = inverse * factor
    mine = pl.ds(pl.multiple_of(lax.rem((me // part_tiles) * rows_each, columns), rows_each), rows_each)
    base = jnp.sum(rb_recv[...], axis=0) * proj[0, mine, :]

    finish(ri_recv.at[others], 4, 1)
    own_chunk[...] = (jnp.sum(ri_recv[...], axis=0) - base) * proj[1, mine, :]
    to_all(lambda d: own_chunk, lambda d: ag_recv.at[d], 6)
    ag_recv[me] = own_chunk[...]
    finish(back.at[others], 5, 1)
    for e in range(devices):
        here = slice(e * LANES, (e + 1) * LANES)
        nb_ref[:, here] = (back[e] - projection * v_ref[:, here]) * inverse
    finish(image.at[others], 5, 0)
    finish(ri_send.at[others], 4, 0)
    finish(ag_recv.at[others], 6, 0)
    finish(ag_recv.at[others], 6, 1)
    for n in range(devices):
        flat = n * rows_each
        tile, row = flat // 8, flat % 8
        strip, side = tile // part_tiles, tile % part_tiles
        top = strip * 8 + row
        q0, high = top % columns, top // columns
        begin = high * LOW + side * LANES
        sketch_ref[q0:q0 + rows_each, begin:begin + LANES] = ag_recv[n]


def together(devices, basis_vector, diagonal, coords, phase_scale, sketch_rows, sketch_signs):
    columns, local_points = basis_vector.shape
    sections = devices.bit_length() - 1
    plane = (local_points // LANES, LANES)
    rows_each = HIGH * columns * LOW // LANES // devices
    vmem = pl.BlockSpec(memory_space=pltpu.VMEM)
    tile = pltpu.VMEM((devices, columns, LANES), F32)
    chunk = pltpu.VMEM((devices, rows_each, LANES), F32)
    return pl.pallas_call(
        functools.partial(tile_kernel, devices, local_points * devices),
        out_shape=(
            jax.ShapeDtypeStruct((columns, local_points), F32),
            jax.ShapeDtypeStruct((columns, SKETCH), F32),
            jax.ShapeDtypeStruct((2, columns), F32)),
        in_specs=[pl.BlockSpec(memory_space=pltpu.SMEM), vmem, vmem, vmem, vmem, vmem],
        out_specs=(vmem, vmem, vmem),
        scratch_shapes=[
            pltpu.VMEM((devices, 8, LANES), F32),
            pltpu.VMEM((devices, 8, LANES), F32),
            tile,
            pltpu.VMEM((2 * sections, devices, LANES), F32),
            pltpu.VMEM((2 * sections, devices, LANES), F32),
            pltpu.VMEM((sections, devices // 2, 4 * WIDTH, 2 * LANES), BF16),
            pltpu.VMEM((devices, 2 * WIDTH, LANES), BF16),
            pltpu.VMEM((2, devices, LANES, LANES), BF16),
            pltpu.VMEM((devices * WIDTH, LANES), F32),
            tile, tile,
            pltpu.VMEM((2 * HIGH * columns, LOW), F32),
            pltpu.VMEM((2 * HIGH * columns, LOW), F32),
            pltpu.VMEM((2, columns, LANES), F32),
            pltpu.VMEM((1, LANES), F32),
            pltpu.VMEM((devices, 1, LANES), F32),
            chunk, chunk, chunk, chunk, chunk,
            pltpu.VMEM((rows_each, LANES), F32),
            pltpu.SemaphoreType.DMA((14,)),
        ],
        compiler_params=pltpu.CompilerParams(
            collective_id=0, has_side_effects=True, vmem_limit_bytes=60 * 2**20),
        name="gmres",
    )(phase_scale, basis_vector, coords, diagonal.reshape(plane), sketch_rows.reshape(plane),
      sketch_signs.reshape(plane))


def body(basis_vector, diagonal, coords, phase_scale, sketch_rows, sketch_signs):
    columns, local_points = basis_vector.shape
    devices = lax.axis_size("box")
    if devices * LANES == local_points:
        return together(devices, basis_vector, diagonal, coords, phase_scale, sketch_rows, sketch_signs)
    sections = devices.bit_length() - 1
    count = -(-sections // 5)
    stages, low = [], 0
    for i in range(count):
        bits = (sections - low) // (count - i)
        stages.append((low, bits))
        low += bits
    group = 2 ** max(bits for _, bits in stages)
    group_rows = [columns * WIDTH // LANES * (LANES // 2 ** bits) for _, bits in stages]
    plane = (local_points // LANES, LANES)
    rows_each = HIGH * columns * LOW // LANES // devices
    vmem = pl.BlockSpec(memory_space=pltpu.VMEM)
    dma = pltpu.SemaphoreType.DMA
    count_rows = max(group_rows)
    halves = columns // 8
    new_basis, sketch, arn = pl.pallas_call(
        functools.partial(kernel, devices, stages, local_points * devices),
        out_shape=(
            jax.ShapeDtypeStruct((columns, local_points), F32),
            jax.ShapeDtypeStruct((columns, SKETCH), F32),
            jax.ShapeDtypeStruct((2, columns), F32)),
        in_specs=[pl.BlockSpec(memory_space=pltpu.SMEM), vmem, vmem, vmem, vmem, vmem],
        out_specs=(vmem, vmem, vmem),
        scratch_shapes=[
            pltpu.VMEM(((columns + 8) * LEAF, LANES), F32),
            pltpu.VMEM((columns + 8, LEAF, LANES), F32),
            pltpu.VMEM((LEAF, WIDTH, LANES), F32),
            pltpu.VMEM((2 * sections, WIDTH, WIDTH, LANES), F32),
            pltpu.VMEM((LEAF, columns, LANES), F32),
            pltpu.VMEM((columns * WIDTH, LANES), F32),
            pltpu.VMEM((columns * WIDTH, LANES), F32),
            pltpu.VMEM((columns * WIDTH // LANES, LANES, LANES), F32),
            pltpu.VMEM((2, LEAF, LANES), F32),
            pltpu.VMEM((LEAF // 4, LOW, 4 * LANES), BF16),
            pltpu.VMEM((2 * HIGH * columns, LOW), F32),
            pltpu.VMEM((2 * HIGH * columns, LOW), F32),
            pltpu.VMEM((count * halves, group, count_rows // halves, LANES), F32),
            pltpu.VMEM((count * halves, group, count_rows // halves, LANES), F32),
            pltpu.VMEM((count * halves, group, count_rows // halves, LANES), F32),
            pltpu.VMEM((count * halves, group, count_rows // halves, LANES), F32),
            pltpu.VMEM((1, LANES), F32),
            pltpu.VMEM((devices, 1, LANES), F32),
            pltpu.VMEM((devices, rows_each, LANES), F32),
            pltpu.VMEM((devices, rows_each, LANES), F32),
            pltpu.VMEM((devices, rows_each, LANES), F32),
            pltpu.VMEM((rows_each, LANES), F32),
            dma((count * halves, group)), dma((count * halves, group)), dma((count * halves, group)), dma((count * halves, group)),
            dma((devices,)), dma((devices,)), dma((devices,)), dma((devices,)), dma((devices,)), dma((devices,)),
        ],
        compiler_params=pltpu.CompilerParams(
            collective_id=0, has_side_effects=True, vmem_limit_bytes=60 * 2**20),
        name="gmres",
    )(phase_scale, basis_vector, coords, diagonal.reshape(plane), sketch_rows.reshape(plane),
      sketch_signs.reshape(plane))
    return new_basis, sketch, arn


def solution(mesh):
    placed = (P(None, "box"), P("box"), P(None, "box"), P(), P("box"), P("box"))
    return jax.shard_map(
        body, mesh=mesh, in_specs=placed, out_specs=(P(None, "box"), P(), P()), check_vma=False
    )
```

```python
import functools
import math

import jax
import jax.numpy as jnp
import numpy as np
from jax import lax
from jax.experimental import pallas as pl
from jax.experimental.pallas import tpu as pltpu
from jax.sharding import PartitionSpec as P

WIDTH = 32
LEAF = 32
SKETCH = 2048
LANES = 128
HIGH = 8
LOW = SKETCH // HIGH
MODULUS = 8191
EPSILON = 1e-06
MESH = pl.DeviceIdType.MESH
F32 = jnp.float32
BF16 = jnp.bfloat16


def sine_series():
    node = np.cos((np.arange(400) + 0.5) * np.pi / 800)
    basis = np.stack([node ** (2 * i) for i in range(6)], 1)
    exact = np.sin(np.pi * node * 4096 / MODULUS) / node
    return np.linalg.lstsq(basis, exact, rcond=None)[0]


SERIES = sine_series()


def remainder(n):
    return n - jnp.floor(n * (1.0 / MODULUS) + 0.5) * float(MODULUS)


def half_sine(n, gain):
    t = remainder(n) * (1.0 / 4096)
    z = t * t
    total = z * float(SERIES[5] * gain) + float(SERIES[4] * gain)
    for c in SERIES[3::-1]:
        total = total * z + float(c * gain)
    return total * t


def scaled_cos(n, amplitude):
    s = half_sine(n, math.sqrt(2.0 * amplitude))
    return amplitude - s * s


def scaled_sin(n, amplitude):
    return scaled_cos(n - 0.25 * MODULUS, amplitude)


def fold(p):
    return (p & MODULUS) + lax.shift_right_logical(p, 13)


def kernel(devices, stages, total_points, scale_ref, v_ref, coords_ref, diag_ref, rows_ref, signs_ref,
           nb_ref, sketch_ref, arn_ref, raw, pts, leaf, mats, kk, cbuf, part, tbuf, work, onehot, skb, ski,
           a_send, a_recv, b_send, b_recv, sum_send, sum_recv, rs_send, rs_recv, ag_recv, own_chunk,
           a_ss, a_rs, b_ss, b_rs, s_ss, s_rs, r_ss, r_rs, g_ss, g_rs):
    me = lax.axis_index("box")
    columns = nb_ref.shape[0]
    halves = columns // 8
    barrier = pltpu.get_barrier_semaphore()

    @pl.loop(1, devices)
    def _(i):
        pl.semaphore_signal(barrier, inc=1, device_id=(lax.rem(me + i, devices),), device_id_type=MESH)

    lane = lax.broadcasted_iota(jnp.int32, (8, LANES), 1)
    sub = lax.broadcasted_iota(jnp.int32, (8, LANES), 0)
    scale = lax.rem(scale_ref[0], MODULUS)

    for r in range(LANES // 4):
        here = slice(LANES * r, LANES * (r + 1))
        for h in range(halves):
            raw[pl.ds(256 * h + r, 8, stride=32), :] = v_ref[8 * h:8 * h + 8, here]
        pair = coords_ref[:, here].astype(F32)
        raw[columns * 32 + r:columns * 32 + r + 1, :] = pair[0:1]
        raw[columns * 32 + 32 + r:columns * 32 + 33 + r, :] = pair[1:2]
    raw[(columns + 2) * 32:(columns + 3) * 32, :] = diag_ref[...]
    raw[(columns + 3) * 32:(columns + 4) * 32, :] = rows_ref[...].astype(F32)
    raw[(columns + 4) * 32:(columns + 5) * 32, :] = signs_ref[...].astype(F32)
    raw[(columns + 5) * 32:(columns + 8) * 32, :] = jnp.zeros((96, LANES), F32)
    for i in range((columns + 8) // 4):
        flipped = raw[LANES * i:LANES * (i + 1), :].T
        tbuf[0] = flipped
        for j in range(4):
            pts[4 * i + j] = jnp.concatenate(
                [tbuf[0, 32 * g:32 * g + 32, 32 * j:32 * j + 32] for g in range(4)], axis=1)

    def exact_phase(row):
        return fold(pts[columns + row].astype(jnp.int32) * scale).astype(F32)

    work[0] = exact_phase(0)
    work[1] = exact_phase(1)
    fx = (sub % 4 + 1).astype(F32)
    fy = (sub // 4 + 1).astype(F32)
    unit = 1.0 / math.sqrt(LEAF)

    @pl.loop(0, LEAF)
    def _(s):
        px = work[0, pl.ds(s, 1), :]
        py = work[1, pl.ds(s, 1), :]
        for tile in range(2):
            n = fx * px + (fy + 2.0 * tile) * py
            leaf[s, 8 * tile:8 * tile + 8] = scaled_cos(n, unit)
            leaf[s, 16 + 8 * tile:24 + 8 * tile] = scaled_sin(n, unit)

    def gather_half(h):
        def gather(s, acc):
            tiles = [leaf[s, 8 * t:8 * t + 8] for t in range(4)]
            out = []
            for q in range(8):
                row = pts[8 * h + q, pl.ds(s, 1), :]
                for t in range(4):
                    out.append(acc[4 * q + t] + tiles[t] * row)
            return tuple(out)

        acc = lax.fori_loop(0, LEAF, gather, tuple(jnp.zeros((8, LANES), F32) for _ in range(32)), unroll=2)
        for q in range(8):
            for t in range(4):
                cbuf[pl.ds((8 * h + q) * 32 + 8 * t, 8), :] = acc[4 * q + t]

    blocks = 8 * WIDTH // LANES

    def make_maps(low, bits):
        group = 2 ** bits
        places = LANES // group
        mine = lax.rem(me // 2 ** low, group)
        spot = mine * places + lane % places
        box = 4 * (spot % 32) + spot // 32
        member = me + (lane // places - mine) * 2 ** low
        ident = (member * LANES + box) * 37

        @pl.loop(low, low + bits)
        def _(k):
            x = (ident + 101 * k).astype(F32)
            rest = x - jnp.floor(x * (1.0 / (MODULUS - 1))) * float(MODULUS - 1)
            rest = jnp.where(rest < 0.0, rest + float(MODULUS - 1), rest)
            rest = jnp.where(rest >= float(MODULUS - 1), rest - float(MODULUS - 1), rest)
            key = rest.astype(jnp.int32) + 1
            unit_phase = fold(fold(key * scale)).astype(F32)
            wide = sub.astype(F32)
            for m in range(2):
                amplitude = (0.35 if m == 0 else 0.6) / math.sqrt(WIDTH)
                first, second, offset = (1.0, 2.0, 0.0) if m == 0 else (3.0, 1.0, 4096.0)
                mid = unit_phase * (wide + (8.0 + first))
                far = unit_phase * (wide + (16.0 + first))

                @pl.loop(0, WIDTH, unroll=2)
                def _(v):
                    times = v.astype(F32) + second
                    step = scaled_cos(unit_phase * (8.0 * times), 2.0)
                    one = scaled_cos(mid * times + offset, amplitude)
                    two = scaled_cos(far * times + offset, amplitude)
                    mats[2 * k + m, v, 8:16] = one
                    mats[2 * k + m, v, 16:24] = two
                    mats[2 * k + m, v, 0:8] = step * one - two
                    mats[2 * k + m, v, 24:32] = step * two - one

    def exchange(send, recv, ss, rs, low, bits, action):
        group = 2 ** bits
        mine = lax.rem(me // 2 ** low, group)

        @pl.loop(1, group)
        def _(i):
            other = lax.rem(mine + i, group)
            here = other if action is finish_recv else mine
            copy = pltpu.make_async_remote_copy(
                send.at[other], recv.at[here], ss.at[other], rs.at[here],
                device_id=(me + (other - mine) * 2 ** low,), device_id_type=MESH)
            action(copy)
        return mine

    def pack(send, group, h):
        places = LANES // group
        for j in range(blocks):
            at = LANES * (blocks * h + j)
            tbuf[j] = cbuf[at:at + LANES, :].T
        for d in range(group):
            for j in range(blocks):
                send[d, places * j:places * (j + 1), :] = tbuf[j, places * d:places * (d + 1), :]

    def unpack(recv, group, h):
        places = LANES // group
        for j in range(blocks):
            for d in range(group):
                tbuf[j, places * d:places * (d + 1), :] = recv[d, places * j:places * (j + 1), :]
        for j in range(blocks):
            at = LANES * (blocks * h + j)
            cbuf[at:at + LANES, :] = tbuf[j].T

    def sketch_of(values, target, make):
        target[...] = jnp.zeros_like(target)

        @pl.loop(0, LEAF // 4)
        def _(c):
            pieces = []
            for i in range(4):
                s = 4 * c + i
                row = pts[columns + 3, pl.ds(s, 1), :]
                high = jnp.floor(row * (1.0 / LOW))
                if make:
                    low = (row - high * LOW).astype(jnp.int32)
                    ids = lax.broadcasted_iota(jnp.int32, (LOW, LANES), 0)
                    onehot[c, :, LANES * i:LANES * (i + 1)] = jnp.where(ids == low, 1.0, 0.0).astype(BF16)
                sign = 2.0 * pts[columns + 4, pl.ds(s, 1), :] - 1.0
                v = values(s) * sign
                top = v.astype(BF16)
                rest = (v - top.astype(F32)).astype(BF16)
                wide = jnp.broadcast_to(high, (columns, LANES))
                masks = [jnp.where(wide == float(g), 1.0, 0.0).astype(BF16) for g in range(HIGH)]
                pieces.append(jnp.concatenate([top * g for g in masks] + [rest * g for g in masks], axis=0))
            left = jnp.concatenate(pieces, axis=1)
            target[...] += lax.dot_general(left, onehot[c], (((1,), (1,)), ((), ())), preferred_element_type=F32)

    nbt = kk

    def start(copy):
        copy.start()

    def finish_recv(copy):
        copy.wait_recv()

    def finish_send(copy):
        copy.wait_send()

    for index, (low, bits) in enumerate(stages):
        group = 2 ** bits
        places = LANES // group

        def outward(h, action):
            at = halves * index + h
            return exchange(a_send.at[at], a_recv.at[at], a_ss.at[at], a_rs.at[at], low, bits, action)

        def homeward(h, action):
            at = halves * index + h
            return exchange(b_send.at[at], b_recv.at[at], b_ss.at[at], b_rs.at[at], low, bits, action)

        for h in range(halves):
            at = halves * index + h
            if index == 0:
                gather_half(h)
            pack(a_send.at[at], group, h)
            if index == 0 and h == 0:
                pl.semaphore_wait(barrier, devices - 1)
            mine = outward(h, start)
            a_recv[at, mine] = a_send[at, mine]
        make_maps(low, bits)
        if index == 0:
            for q in range(columns):
                for s in range(LEAF):
                    nbt[s, q:q + 1, :] = pts[q, s:s + 1, :]
            sketch_of(lambda s: nbt[s], skb, True)
        for h in range(halves):
            at = halves * index + h
            outward(h, finish_recv)
            unpack(a_recv.at[at], group, h)
            half = slice(256 * h, 256 * (h + 1))
            for k in range(low, low + bits):
                span = places * 2 ** (k - low)
                full = cbuf[half, :]
                wide = lax.broadcasted_iota(jnp.int32, full.shape, 1)
                part[half, :] = jnp.where((wide // span) % 2 == 0,
                                          pltpu.roll(full, LANES - span, 1), pltpu.roll(full, span, 1))

                def mix(v, acc):
                    own = [mats[2 * k, v, 8 * t:8 * t + 8] for t in range(4)]
                    cross = [mats[2 * k + 1, v, 8 * t:8 * t + 8] for t in range(4)]
                    out = []
                    for q in range(8):
                        row = cbuf[pl.ds((8 * h + q) * 32 + v, 1), :]
                        other = part[pl.ds((8 * h + q) * 32 + v, 1), :]
                        for t in range(4):
                            out.append(acc[4 * q + t] + own[t] * row + cross[t] * other)
                    return tuple(out)

                init = tuple(0.85 * cbuf[pl.ds((8 * h + q) * 32 + 8 * t, 8), :] for q in range(8) for t in range(4))
                acc = lax.fori_loop(0, WIDTH, mix, init, unroll=2)
                for q in range(8):
                    for t in range(4):
                        cbuf[pl.ds((8 * h + q) * 32 + 8 * t, 8), :] = acc[4 * q + t]
            pack(b_send.at[at], group, h)
            mine = homeward(h, start)
            b_recv[at, mine] = b_send[at, mine]
        for h in range(halves):
            outward(h, finish_send)
        for h in range(halves):
            homeward(h, finish_recv)
            unpack(b_recv.at[halves * index + h], group, h)
        for h in range(halves):
            homeward(h, finish_send)

    for c in range(LEAF // 8):
        def spread_out(w, acc):
            coef = [cbuf[pl.ds(8 * h * 32 + w, 8, stride=32), :] for h in range(halves)]
            out = []
            for s in range(8):
                row = leaf[8 * c + s, pl.ds(w, 1), :]
                for h in range(halves):
                    out.append(acc[halves * s + h] + coef[h] * row)
            return tuple(out)

        init = tuple(
            jnp.broadcast_to(pts[columns + 2, 8 * c + s:8 * c + s + 1, :], (8, LANES)) * nbt[8 * c + s, 8 * h:8 * h + 8]
            for s in range(8) for h in range(halves))
        acc = lax.fori_loop(0, WIDTH, spread_out, init, unroll=2)
        for s in range(8):
            for h in range(halves):
                part[(8 * c + s) * columns + 8 * h:(8 * c + s) * columns + 8 * h + 8, :] = acc[halves * s + h]

    inner = jnp.zeros((columns, LANES), F32)
    square, energy = inner, inner
    for s in range(LEAF):
        v, image = nbt[s], part[s * columns:(s + 1) * columns, :]
        inner, square, energy = inner + v * image, square + v * v, energy + image * image
    lane_q = lax.broadcasted_iota(jnp.int32, (columns, LANES), 1)
    row_q = lax.broadcasted_iota(jnp.int32, (columns, LANES), 0)
    packed = jnp.zeros((columns, LANES), F32)
    for i, value in enumerate((inner, square, energy)):
        packed = jnp.where(lane_q == row_q + columns * i, jnp.sum(value, axis=1, keepdims=True), packed)
    sum_send[...] = jnp.sum(packed, axis=0, keepdims=True)

    def to_all(source, recv, ss, rs, action):
        @pl.loop(1, devices)
        def _(i):
            other = lax.rem(me + i, devices)
            here = other if action is finish_recv else me
            action(pltpu.make_async_remote_copy(
                source(other), recv.at[here], ss.at[other], rs.at[here],
                device_id=(other,), device_id_type=MESH))

    to_all(lambda d: sum_send, sum_recv, s_ss, s_rs, start)
    sum_recv[me] = sum_send[...]
    sketch_of(lambda s: part[pl.ds(pl.multiple_of(s * columns, columns), columns), :], ski, False)
    to_all(lambda d: sum_send, sum_recv, s_ss, s_rs, finish_recv)
    totals = jnp.sum(sum_recv[...], axis=0)

    def column(i):
        picked = jnp.where(lane_q == row_q + columns * i, jnp.broadcast_to(totals, (columns, LANES)), 0.0)
        return jnp.broadcast_to(jnp.sum(picked, axis=1, keepdims=True) * (1.0 / total_points), (columns, LANES))

    inner_mean, square_mean, energy_mean = column(0), column(1), column(2)
    projection = inner_mean / (square_mean + EPSILON)
    energy = energy_mean - 2.0 * projection * inner_mean + projection * projection * square_mean
    spread = jnp.sqrt(energy + EPSILON)
    inverse = 1.0 / spread
    for i, value in enumerate((projection, spread)):
        arn_ref[i:i + 1, :] = jnp.sum(jnp.where(lane_q == row_q, value, 0.0), axis=0, keepdims=True)[:, :columns]

    rows_each = rs_send.shape[1]
    factor = math.sqrt(SKETCH / total_points)
    lowest = HIGH * columns
    part_tiles = LOW // LANES
    for n in range(devices):
        flat = n * rows_each
        tile, row = flat // 8, flat % 8
        strip, side = tile // part_tiles, tile % part_tiles
        top = strip * 8 + row
        q0 = top % columns
        cols = slice(side * LANES, (side + 1) * LANES)
        img = ski[top:top + rows_each, cols] + ski[lowest + top:lowest + top + rows_each, cols]
        bas = skb[top:top + rows_each, cols] + skb[lowest + top:lowest + top + rows_each, cols]
        rs_send[n] = (img - projection[q0:q0 + rows_each] * bas) * (factor * inverse[q0:q0 + rows_each])
    to_all(lambda d: rs_send.at[d], rs_recv, r_ss, r_rs, start)
    rs_recv[me] = rs_send[me]

    for s in range(LEAF):
        pts_rows = (part[s * columns:(s + 1) * columns, :] - projection * nbt[s]) * inverse
        nbt[s] = pts_rows
    for q in range(columns):
        for s in range(LEAF):
            pts[q, s:s + 1, :] = nbt[s, q:q + 1, :]
    for i in range(columns // 4):
        for j in range(4):
            for g in range(4):
                tbuf[0, 32 * g:32 * g + 32, 32 * j:32 * j + 32] = pts[4 * i + j, :, 32 * g:32 * g + 32]
        raw[LANES * i:LANES * (i + 1), :] = tbuf[0].T
    for r in range(LANES // 4):
        for h in range(halves):
            nb_ref[8 * h:8 * h + 8, LANES * r:LANES * (r + 1)] = raw[pl.ds(256 * h + r, 8, stride=32), :]

    to_all(lambda d: rs_send.at[d], rs_recv, r_ss, r_rs, finish_recv)
    own_chunk[...] = jnp.sum(rs_recv[...], axis=0)
    to_all(lambda d: own_chunk, ag_recv, g_ss, g_rs, start)
    ag_recv[me] = own_chunk[...]
    to_all(lambda d: sum_send, sum_recv, s_ss, s_rs, finish_send)
    to_all(lambda d: rs_send.at[d], rs_recv, r_ss, r_rs, finish_send)
    to_all(lambda d: own_chunk, ag_recv, g_ss, g_rs, finish_recv)
    for n in range(devices):
        flat = n * rows_each
        tile, row = flat // 8, flat % 8
        strip, side = tile // part_tiles, tile % part_tiles
        top = strip * 8 + row
        q0, high = top % columns, top // columns
        begin = high * LOW + side * LANES
        sketch_ref[q0:q0 + rows_each, begin:begin + LANES] = ag_recv[n]
    to_all(lambda d: own_chunk, ag_recv, g_ss, g_rs, finish_send)


def split(x):
    top = x.astype(BF16)
    return top, (x - top.astype(F32)).astype(BF16)


def tile_kernel(devices, total_points, scale_ref, v_in, coords_in, diag_in, rows_in, signs_in,
                nb_ref, sketch_ref, arn_ref, v_ref, coords_ref, diag_ref, rows_ref, signs_ref,
                small_send, small, vals, phases, steps, mats, leaf, state, coef,
                image, back, hot, left, masks, proj, sum_send, sum_recv, rb_send, rb_recv, ri_send, ri_recv,
                ag_recv, own_chunk, sems, io_sems):
    me = lax.axis_index("box")
    columns = nb_ref.shape[0]
    sections = devices.bit_length() - 1
    per_tile = LANES // LEAF
    half = LANES // 2
    barrier = pltpu.get_barrier_semaphore()

    @pl.loop(1, devices)
    def _(i):
        pl.semaphore_signal(barrier, inc=1, device_id=(lax.rem(me + i, devices),), device_id_type=MESH)

    incoming = [pltpu.make_async_copy(a, b, io_sems.at[i]) for i, (a, b) in enumerate((
        (v_in, v_ref), (coords_in, coords_ref), (diag_in, diag_ref), (rows_in, rows_ref), (signs_in, signs_ref)))]
    for copy in incoming:
        copy.start()
    lane = lax.broadcasted_iota(jnp.int32, (8, LANES), 1)
    sub = lax.broadcasted_iota(jnp.int32, (8, LANES), 0)
    planes = 4
    plane_size = devices // planes
    plane, seat = me // plane_size, lax.rem(me, plane_size)

    def to_all(source, recv, which, aways=range(planes - 1, -1, -1)):
        for away in aways:
            there = 0
            for b in range(planes.bit_length() - 1):
                bit = lax.rem(plane // 2 ** b, 2)
                there = there + 2 ** b * ((1 - bit) if (away >> b) & 1 else bit)

            @pl.loop(0 if away else 1, plane_size)
            def _(i):
                other = plane_size * there + lax.rem(seat + i, plane_size)
                pltpu.make_async_remote_copy(
                    source(other), recv(me), sems.at[2 * which], sems.at[2 * which + 1],
                    device_id=(other,), device_id_type=MESH).start()

    def finish(ref, which, side):
        pltpu.make_async_copy(ref, ref, sems.at[2 * which + side]).wait()

    def columns_at(ref, tile):
        return ref.at[:, pl.ds(pl.multiple_of(tile * LANES, LANES), LANES)]

    others = pl.ds(0, devices - 1)
    side_rows = 5
    side_part = pl.ds(0, side_rows)

    for copy in incoming:
        copy.wait()
    scale = lax.rem(scale_ref[0], MODULUS)
    rows_f, signs_f = rows_ref[...].astype(F32), signs_ref[...].astype(F32)
    for e in range(devices):
        here = slice(e * LANES, (e + 1) * LANES)
        small_send[e, 0:2, :] = coords_ref[:, here].astype(F32)
        small_send[e, 2:3, :] = diag_ref[e:e + 1, :]
        small_send[e, 3:4, :] = rows_f[e:e + 1, :]
        small_send[e, 4:5, :] = signs_f[e:e + 1, :]
    pl.semaphore_wait(barrier, devices - 1)
    to_all(lambda d: small_send.at[d, side_part], lambda d: small.at[d, side_part], 0)
    to_all(lambda d: columns_at(v_ref, d), lambda d: vals.at[d], 1)
    small[me] = small_send[me]
    vals[me] = columns_at(v_ref, me)[...]

    spot = lane // LEAF
    inner_lane = (lane % LEAF).astype(F32)
    for k in range(sections):
        for g in range(devices // 8):
            ident = ((8 * g + sub) * LANES + per_tile * me + spot) * 37
            x = (ident + 101 * k).astype(F32)
            rest = x - jnp.floor(x * (1.0 / (MODULUS - 1))) * float(MODULUS - 1)
            rest = jnp.where(rest < 0.0, rest + float(MODULUS - 1), rest)
            rest = jnp.where(rest >= float(MODULUS - 1), rest - float(MODULUS - 1), rest)
            key = rest.astype(jnp.int32) + 1
            unit_phase = fold(fold(key * scale)).astype(F32)
            for m, second in enumerate((2.0, 1.0)):
                phi = remainder(unit_phase * (inner_lane + second))
                phases[2 * k + m, 8 * g:8 * g + 8, :] = phi
                steps[2 * k + m, 8 * g:8 * g + 8, :] = scaled_cos(8.0 * phi, 2.0)

    wide_sub = lax.broadcasted_iota(jnp.int32, (WIDTH, LANES), 0)
    wide_lane = lax.broadcasted_iota(jnp.int32, (WIDTH, LANES), 1)
    ident_part = jnp.where(wide_lane % WIDTH == wide_sub, 0.85, 0.0)
    sub_f = sub.astype(F32)
    for k in range(sections):
        stride = 2 ** k

        @pl.loop(0, devices // 2)
        def _(pair):
            first_tile = (pair // stride) * (2 * stride) + pair % stride
            for bit in range(2):
                d = first_tile + stride * bit
                for m in range(2):
                    amplitude = (0.35 if m == 0 else 0.6) / math.sqrt(WIDTH)
                    first, offset = (1.0, 0.0) if m == 0 else (3.0, 4096.0)
                    phi = phases[2 * k + m, pl.ds(d, 1), :]
                    step = steps[2 * k + m, pl.ds(d, 1), :]
                    one = scaled_cos(phi * (sub_f + (8.0 + first)) + offset, amplitude)
                    two = scaled_cos(phi * (sub_f + (16.0 + first)) + offset, amplitude)
                    full = jnp.concatenate([step * one - two, one, two, step * two - one], axis=0)
                    if m == 0:
                        full = full + ident_part
                    top, low = split(full)
                    begin = LANES * (bit if m == 0 else 1 - bit)
                    mats[k, pair, 64 * bit:64 * bit + 32, begin:begin + LANES] = top
                    mats[k, pair, 64 * bit + 32:64 * bit + 64, begin:begin + LANES] = low

    lanes_q = lax.broadcasted_iota(jnp.int32, (columns, LANES), 1)
    rows_q = lax.broadcasted_iota(jnp.int32, (columns, LANES), 0)

    def place(tile):
        return pl.ds(pl.multiple_of(tile * LANES, LANES), LANES)

    def make_hot(row_of, sign_of):
        @pl.loop(0, devices)
        def _(d):
            row = row_of(d)
            high = jnp.floor(row * (1.0 / LOW))
            low = (row - high * LOW).astype(jnp.int32)
            ids = lax.broadcasted_iota(jnp.int32, (LOW, LANES), 0)
            hot[:, place(d)] = jnp.where(ids == low, 1.0, 0.0).astype(BF16)
            sign = jnp.broadcast_to(2.0 * sign_of(d) - 1.0, (columns, LANES))
            wide = jnp.broadcast_to(high, (columns, LANES))
            for g in range(HIGH):
                masks[d, columns * g:columns * (g + 1), :] = jnp.where(wide == float(g), sign, 0.0).astype(BF16)

    def place_values(d, at, value):
        top, rest = split(value)
        for g in range(HIGH):
            mask = masks[d, columns * g:columns * (g + 1), :]
            left[columns * g:columns * (g + 1), at] = top * mask
            left[columns * (HIGH + g):columns * (HIGH + g + 1), at] = rest * mask

    def sketch_product():
        o = lax.dot_general(left[...], hot[...], (((1,), (1,)), ((), ())), preferred_element_type=F32)
        return o[:HIGH * columns] + o[HIGH * columns:]

    rows_each = rb_send.shape[1]
    factor = math.sqrt(SKETCH / total_points)
    part_tiles = LOW // LANES

    def pieces_of(sk, send):
        for n in range(devices):
            flat = n * rows_each
            tile, row = flat // 8, flat % 8
            strip, side = tile // part_tiles, tile % part_tiles
            top = strip * 8 + row
            cols = slice(side * LANES, (side + 1) * LANES)
            send[n] = sk[top:top + rows_each, cols]

    make_hot(lambda d: rows_ref[pl.ds(d, 1), :].astype(F32), lambda d: signs_ref[pl.ds(d, 1), :].astype(F32))

    @pl.loop(0, devices)
    def _(d):
        place_values(d, place(d), v_ref[:, place(d)])

    basis_sketch = sketch_product()
    pieces_of(basis_sketch, rb_send)

    finish(small.at[others, side_part], 0, 1)
    fx = (sub % 4 + 1).astype(F32)
    fy = (sub // 4 + 1).astype(F32)
    unit = 1.0 / math.sqrt(LEAF)

    @pl.loop(0, devices)
    def _(d):
        pair = fold(small[d, 0:2, :].astype(jnp.int32) * scale).astype(F32)
        px, py = pair[0:1], pair[1:2]
        phases_of = [fx * px + (fy + 2.0 * t) * py for t in range(2)]
        full = jnp.concatenate([scaled_cos(n, unit) for n in phases_of] + [scaled_sin(n, unit) for n in phases_of], axis=0)
        top, low = split(full)
        leaf[d, 0:32] = top
        leaf[d, 32:64] = low

    make_hot(lambda d: small[d, 3:4, :], lambda d: small[d, 4:5, :])
    finish(vals.at[others], 1, 1)
    to_all(lambda d: rb_send.at[d], lambda d: rb_recv.at[d], 2)
    rb_recv[me] = rb_send[me]

    point_masks = [jnp.where(lanes_q // LEAF == j, 1.0, 0.0).astype(BF16) for j in range(per_tile)]
    column_masks = [jnp.where((wide_lane % half) // columns == j, 1.0, 0.0).astype(BF16) for j in range(per_tile)]
    first_half = wide_lane < half

    def combine(o):
        s = o[0:32] + o[32:64]
        return s + pltpu.roll(s, half, 1)

    def expand(total):
        top = total.astype(BF16).astype(F32)
        y = jnp.where(first_half, top, total - top).astype(BF16)
        return jnp.concatenate([y * m for m in column_masks], axis=0)

    for d in range(devices):
        top, rest = split(vals[d])
        spread_v = jnp.concatenate([top * m for m in point_masks] + [rest * m for m in point_masks], axis=0)
        o = lax.dot_general(leaf[d], spread_v, (((1,), (1,)), ((), ())), preferred_element_type=F32)
        state[0, d] = expand(combine(o))

    for k in range(sections):
        stride = 2 ** k
        now = k % 2
        for pair in range(devices // 2):
            d0 = (pair // stride) * (2 * stride) + pair % stride
            d1 = d0 + stride
            x = jnp.concatenate([state[now, d0], state[now, d1]], axis=0)
            o = jnp.dot(mats[k, pair], x, preferred_element_type=F32)
            for d, part in ((d0, o[0:64]), (d1, o[64:128])):
                total = combine(part)
                if k == sections - 1:
                    coef[32 * d:32 * d + 32, :] = total
                else:
                    state[1 - now, d] = expand(total)

    tile_lane = lax.broadcasted_iota(jnp.int32, (half, 2 * LANES), 1)
    tile_masks = [jnp.where((tile_lane % LANES) // WIDTH == t, 1.0, 0.0).astype(BF16) for t in range(4)]
    zero = jnp.zeros((columns, LANES), F32)
    inner, square, energy = zero, zero, zero
    for g in range(devices // 4):
        flipped = coef[LANES * g:LANES * (g + 1), :].T
        top, rest = split(flipped[0:half])
        both = jnp.concatenate([top, rest], axis=1)
        lhs = jnp.concatenate([both * m for m in tile_masks], axis=0)
        tops = jnp.concatenate([leaf[4 * g + t, 0:32] for t in range(4)], axis=0)
        lows = jnp.concatenate([leaf[4 * g + t, 32:64] for t in range(4)], axis=0)
        right = jnp.concatenate([tops, lows], axis=1)
        o = jnp.dot(lhs, jnp.concatenate([right, right], axis=0), preferred_element_type=F32)
        o = o[:, 0:LANES] + o[:, LANES:2 * LANES]
        for t in range(4):
            d = 4 * g + t
            v = vals[d]
            img = jnp.broadcast_to(small[d, 2:3, :], (columns, LANES)) * v
            for j in range(per_tile):
                begin = half * t + columns * j
                img = img + jnp.where(lanes_q // LEAF == j, o[begin:begin + columns], 0.0)
            image[d] = img
            place_values(d, slice(LANES * d, LANES * (d + 1)), img)
            inner, square, energy = inner + v * img, square + v * v, energy + img * img

    packed = zero
    for i, value in enumerate((inner, square, energy)):
        packed = jnp.where(lanes_q == rows_q + columns * i, jnp.sum(value, axis=1, keepdims=True), packed)
    sum_send[...] = jnp.sum(packed, axis=0, keepdims=True)
    to_all(lambda d: sum_send, lambda d: sum_recv.at[d], 3)
    sum_recv[me] = sum_send[...]

    to_all(lambda d: image.at[d], lambda d: back.at[d], 5, (3,))
    image_sketch = sketch_product()
    pieces_of(image_sketch, ri_send)
    to_all(lambda d: ri_send.at[d], lambda d: ri_recv.at[d], 4)
    ri_recv[me] = ri_send[me]
    to_all(lambda d: image.at[d], lambda d: back.at[d], 5, (2, 1, 0))
    back[me] = image[me]

    finish(small_send.at[others, side_part], 0, 0)
    finish(vals.at[others], 1, 0)
    finish(rb_send.at[others], 2, 0)
    finish(rb_recv.at[others], 2, 1)
    finish(sum_recv.at[others], 3, 0)
    finish(sum_recv.at[others], 3, 1)
    totals = jnp.sum(sum_recv[...], axis=0)

    def column(i):
        picked = jnp.where(lanes_q == rows_q + columns * i, jnp.broadcast_to(totals, (columns, LANES)), 0.0)
        return jnp.broadcast_to(jnp.sum(picked, axis=1, keepdims=True) * (1.0 / total_points), (columns, LANES))

    inner_mean, square_mean, energy_mean = column(0), column(1), column(2)
    projection = inner_mean / (square_mean + EPSILON)
    energy = energy_mean - 2.0 * projection * inner_mean + projection * projection * square_mean
    spread = jnp.sqrt(energy + EPSILON)
    inverse = 1.0 / spread
    for i, value in enumerate((projection, spread)):
        arn_ref[i:i + 1, :] = jnp.sum(jnp.where(lanes_q == rows_q, value, 0.0), axis=0, keepdims=True)[:, :columns]
    proj[0] = projection
    proj[1] = inverse * factor
    mine = pl.ds(pl.multiple_of(lax.rem((me // part_tiles) * rows_each, columns), rows_each), rows_each)
    base = jnp.sum(rb_recv[...], axis=0) * proj[0, mine, :]

    finish(ri_recv.at[others], 4, 1)
    own_chunk[...] = (jnp.sum(ri_recv[...], axis=0) - base) * proj[1, mine, :]
    to_all(lambda d: own_chunk, lambda d: ag_recv.at[d], 6)
    ag_recv[me] = own_chunk[...]
    finish(back.at[others], 5, 1)
    for e in range(devices):
        here = slice(e * LANES, (e + 1) * LANES)
        nb_ref[:, here] = (back[e] - projection * v_ref[:, here]) * inverse
    finish(image.at[others], 5, 0)
    finish(ri_send.at[others], 4, 0)
    finish(ag_recv.at[others], 6, 0)
    finish(ag_recv.at[others], 6, 1)
    for n in range(devices):
        flat = n * rows_each
        tile, row = flat // 8, flat % 8
        strip, side = tile // part_tiles, tile % part_tiles
        top = strip * 8 + row
        q0, high = top % columns, top // columns
        begin = high * LOW + side * LANES
        sketch_ref[q0:q0 + rows_each, begin:begin + LANES] = ag_recv[n]


def together(devices, basis_vector, diagonal, coords, phase_scale, sketch_rows, sketch_signs):
    columns, local_points = basis_vector.shape
    sections = devices.bit_length() - 1
    plane = (local_points // LANES, LANES)
    rows_each = HIGH * columns * LOW // LANES // devices
    far = pl.BlockSpec(memory_space=pltpu.HBM)
    vmem = pl.BlockSpec(memory_space=pltpu.VMEM)
    tile = pltpu.VMEM((devices, columns, LANES), F32)
    chunk = pltpu.VMEM((devices, rows_each, LANES), F32)
    return pl.pallas_call(
        functools.partial(tile_kernel, devices, local_points * devices),
        out_shape=(
            jax.ShapeDtypeStruct((columns, local_points), F32),
            jax.ShapeDtypeStruct((columns, SKETCH), F32),
            jax.ShapeDtypeStruct((2, columns), F32)),
        in_specs=[pl.BlockSpec(memory_space=pltpu.SMEM)] + [far] * 5,
        out_specs=(vmem,) * 3,
        scratch_shapes=[
            pltpu.VMEM(basis_vector.shape, F32),
            pltpu.VMEM(coords.shape, jnp.int32),
            pltpu.VMEM(plane, F32),
            pltpu.VMEM(plane, jnp.int32),
            pltpu.VMEM(plane, jnp.int32),
            pltpu.VMEM((devices, 8, LANES), F32),
            pltpu.VMEM((devices, 8, LANES), F32),
            tile,
            pltpu.VMEM((2 * sections, devices, LANES), F32),
            pltpu.VMEM((2 * sections, devices, LANES), F32),
            pltpu.VMEM((sections, devices // 2, 4 * WIDTH, 2 * LANES), BF16),
            pltpu.VMEM((devices, 2 * WIDTH, LANES), BF16),
            pltpu.VMEM((2, devices, LANES, LANES), BF16),
            pltpu.VMEM((devices * WIDTH, LANES), F32),
            tile, tile,
            pltpu.VMEM((LOW, local_points), BF16),
            pltpu.VMEM((2 * HIGH * columns, local_points), BF16),
            pltpu.VMEM((devices, HIGH * columns, LANES), BF16),
            pltpu.VMEM((2, columns, LANES), F32),
            pltpu.VMEM((1, LANES), F32),
            pltpu.VMEM((devices, 1, LANES), F32),
            chunk, chunk, chunk, chunk, chunk,
            pltpu.VMEM((rows_each, LANES), F32),
            pltpu.SemaphoreType.DMA((14,)),
            pltpu.SemaphoreType.DMA((5,)),
        ],
        compiler_params=pltpu.CompilerParams(
            collective_id=0, has_side_effects=True, vmem_limit_bytes=24 * 2**20),
        name="gmres",
    )(phase_scale, *(pltpu.with_memory_space_constraint(x, pltpu.HBM) for x in (
        basis_vector, coords, diagonal.reshape(plane), sketch_rows.reshape(plane),
        sketch_signs.reshape(plane))))


def body(basis_vector, diagonal, coords, phase_scale, sketch_rows, sketch_signs):
    columns, local_points = basis_vector.shape
    devices = lax.axis_size("box")
    if devices * LANES == local_points:
        return together(devices, basis_vector, diagonal, coords, phase_scale, sketch_rows, sketch_signs)
    sections = devices.bit_length() - 1
    count = -(-sections // 5)
    stages, low = [], 0
    for i in range(count):
        bits = (sections - low) // (count - i)
        stages.append((low, bits))
        low += bits
    group = 2 ** max(bits for _, bits in stages)
    group_rows = [columns * WIDTH // LANES * (LANES // 2 ** bits) for _, bits in stages]
    plane = (local_points // LANES, LANES)
    rows_each = HIGH * columns * LOW // LANES // devices
    vmem = pl.BlockSpec(memory_space=pltpu.VMEM)
    dma = pltpu.SemaphoreType.DMA
    count_rows = max(group_rows)
    halves = columns // 8
    new_basis, sketch, arn = pl.pallas_call(
        functools.partial(kernel, devices, stages, local_points * devices),
        out_shape=(
            jax.ShapeDtypeStruct((columns, local_points), F32),
            jax.ShapeDtypeStruct((columns, SKETCH), F32),
            jax.ShapeDtypeStruct((2, columns), F32)),
        in_specs=[pl.BlockSpec(memory_space=pltpu.SMEM), vmem, vmem, vmem, vmem, vmem],
        out_specs=(vmem, vmem, vmem),
        scratch_shapes=[
            pltpu.VMEM(((columns + 8) * LEAF, LANES), F32),
            pltpu.VMEM((columns + 8, LEAF, LANES), F32),
            pltpu.VMEM((LEAF, WIDTH, LANES), F32),
            pltpu.VMEM((2 * sections, WIDTH, WIDTH, LANES), F32),
            pltpu.VMEM((LEAF, columns, LANES), F32),
            pltpu.VMEM((columns * WIDTH, LANES), F32),
            pltpu.VMEM((columns * WIDTH, LANES), F32),
            pltpu.VMEM((columns * WIDTH // LANES, LANES, LANES), F32),
            pltpu.VMEM((2, LEAF, LANES), F32),
            pltpu.VMEM((LEAF // 4, LOW, 4 * LANES), BF16),
            pltpu.VMEM((2 * HIGH * columns, LOW), F32),
            pltpu.VMEM((2 * HIGH * columns, LOW), F32),
            pltpu.VMEM((count * halves, group, count_rows // halves, LANES), F32),
            pltpu.VMEM((count * halves, group, count_rows // halves, LANES), F32),
            pltpu.VMEM((count * halves, group, count_rows // halves, LANES), F32),
            pltpu.VMEM((count * halves, group, count_rows // halves, LANES), F32),
            pltpu.VMEM((1, LANES), F32),
            pltpu.VMEM((devices, 1, LANES), F32),
            pltpu.VMEM((devices, rows_each, LANES), F32),
            pltpu.VMEM((devices, rows_each, LANES), F32),
            pltpu.VMEM((devices, rows_each, LANES), F32),
            pltpu.VMEM((rows_each, LANES), F32),
            dma((count * halves, group)), dma((count * halves, group)), dma((count * halves, group)), dma((count * halves, group)),
            dma((devices,)), dma((devices,)), dma((devices,)), dma((devices,)), dma((devices,)), dma((devices,)),
        ],
        compiler_params=pltpu.CompilerParams(
            collective_id=0, has_side_effects=True, vmem_limit_bytes=60 * 2**20),
        name="gmres",
    )(phase_scale, basis_vector, coords, diagonal.reshape(plane), sketch_rows.reshape(plane),
      sketch_signs.reshape(plane))
    return new_basis, sketch, arn


def solution(mesh):
    placed = (P(None, "box"), P("box"), P(None, "box"), P(), P("box"), P("box"))
    return jax.shard_map(
        body, mesh=mesh, in_specs=placed, out_specs=(P(None, "box"), P(), P()), check_vma=False
    )
```

```python
import functools
import math

import jax
import jax.numpy as jnp
import numpy as np
from jax import lax
from jax.experimental import pallas as pl
from jax.experimental.pallas import tpu as pltpu
from jax.sharding import PartitionSpec as P

WIDTH = 32
LEAF = 32
SKETCH = 2048
LANES = 128
HIGH = 8
LOW = SKETCH // HIGH
MODULUS = 8191
EPSILON = 1e-06
MESH = pl.DeviceIdType.MESH
F32 = jnp.float32
BF16 = jnp.bfloat16


def sine_series():
    node = np.cos((np.arange(400) + 0.5) * np.pi / 800)
    basis = np.stack([node ** (2 * i) for i in range(6)], 1)
    exact = np.sin(np.pi * node * 4096 / MODULUS) / node
    return np.linalg.lstsq(basis, exact, rcond=None)[0]


SERIES = sine_series()


def remainder(n):
    return n - jnp.floor(n * (1.0 / MODULUS) + 0.5) * float(MODULUS)


def half_sine(n, gain):
    t = remainder(n) * (1.0 / 4096)
    z = t * t
    total = z * float(SERIES[5] * gain) + float(SERIES[4] * gain)
    for c in SERIES[3::-1]:
        total = total * z + float(c * gain)
    return total * t


def scaled_cos(n, amplitude):
    s = half_sine(n, math.sqrt(2.0 * amplitude))
    return amplitude - s * s


def scaled_sin(n, amplitude):
    return scaled_cos(n - 0.25 * MODULUS, amplitude)


def fold(p):
    return (p & MODULUS) + lax.shift_right_logical(p, 13)


def kernel(devices, stages, total_points, scale_ref, v_ref, coords_ref, diag_ref, rows_ref, signs_ref,
           nb_ref, sketch_ref, arn_ref, raw, pts, leaf, mats, kk, cbuf, part, tbuf, work, onehot, skb, ski,
           a_send, a_recv, b_send, b_recv, sum_send, sum_recv, rs_send, rs_recv, ag_recv, own_chunk,
           a_ss, a_rs, b_ss, b_rs, s_ss, s_rs, r_ss, r_rs, g_ss, g_rs):
    me = lax.axis_index("box")
    columns = nb_ref.shape[0]
    halves = columns // 8
    barrier = pltpu.get_barrier_semaphore()

    @pl.loop(1, devices)
    def _(i):
        pl.semaphore_signal(barrier, inc=1, device_id=(lax.rem(me + i, devices),), device_id_type=MESH)

    lane = lax.broadcasted_iota(jnp.int32, (8, LANES), 1)
    sub = lax.broadcasted_iota(jnp.int32, (8, LANES), 0)
    scale = lax.rem(scale_ref[0], MODULUS)

    for r in range(LANES // 4):
        here = slice(LANES * r, LANES * (r + 1))
        for h in range(halves):
            raw[pl.ds(256 * h + r, 8, stride=32), :] = v_ref[8 * h:8 * h + 8, here]
        pair = coords_ref[:, here].astype(F32)
        raw[columns * 32 + r:columns * 32 + r + 1, :] = pair[0:1]
        raw[columns * 32 + 32 + r:columns * 32 + 33 + r, :] = pair[1:2]
    raw[(columns + 2) * 32:(columns + 3) * 32, :] = diag_ref[...]
    raw[(columns + 3) * 32:(columns + 4) * 32, :] = rows_ref[...].astype(F32)
    raw[(columns + 4) * 32:(columns + 5) * 32, :] = signs_ref[...].astype(F32)
    raw[(columns + 5) * 32:(columns + 8) * 32, :] = jnp.zeros((96, LANES), F32)
    for i in range((columns + 8) // 4):
        flipped = raw[LANES * i:LANES * (i + 1), :].T
        tbuf[0] = flipped
        for j in range(4):
            pts[4 * i + j] = jnp.concatenate(
                [tbuf[0, 32 * g:32 * g + 32, 32 * j:32 * j + 32] for g in range(4)], axis=1)

    def exact_phase(row):
        return fold(pts[columns + row].astype(jnp.int32) * scale).astype(F32)

    work[0] = exact_phase(0)
    work[1] = exact_phase(1)
    fx = (sub % 4 + 1).astype(F32)
    fy = (sub // 4 + 1).astype(F32)
    unit = 1.0 / math.sqrt(LEAF)

    @pl.loop(0, LEAF)
    def _(s):
        px = work[0, pl.ds(s, 1), :]
        py = work[1, pl.ds(s, 1), :]
        for tile in range(2):
            n = fx * px + (fy + 2.0 * tile) * py
            leaf[s, 8 * tile:8 * tile + 8] = scaled_cos(n, unit)
            leaf[s, 16 + 8 * tile:24 + 8 * tile] = scaled_sin(n, unit)

    def gather_half(h):
        def gather(s, acc):
            tiles = [leaf[s, 8 * t:8 * t + 8] for t in range(4)]
            out = []
            for q in range(8):
                row = pts[8 * h + q, pl.ds(s, 1), :]
                for t in range(4):
                    out.append(acc[4 * q + t] + tiles[t] * row)
            return tuple(out)

        acc = lax.fori_loop(0, LEAF, gather, tuple(jnp.zeros((8, LANES), F32) for _ in range(32)), unroll=2)
        for q in range(8):
            for t in range(4):
                cbuf[pl.ds((8 * h + q) * 32 + 8 * t, 8), :] = acc[4 * q + t]

    blocks = 8 * WIDTH // LANES

    def make_maps(low, bits):
        group = 2 ** bits
        places = LANES // group
        mine = lax.rem(me // 2 ** low, group)
        spot = mine * places + lane % places
        box = 4 * (spot % 32) + spot // 32
        member = me + (lane // places - mine) * 2 ** low
        ident = (member * LANES + box) * 37

        @pl.loop(low, low + bits)
        def _(k):
            x = (ident + 101 * k).astype(F32)
            rest = x - jnp.floor(x * (1.0 / (MODULUS - 1))) * float(MODULUS - 1)
            rest = jnp.where(rest < 0.0, rest + float(MODULUS - 1), rest)
            rest = jnp.where(rest >= float(MODULUS - 1), rest - float(MODULUS - 1), rest)
            key = rest.astype(jnp.int32) + 1
            unit_phase = fold(fold(key * scale)).astype(F32)
            wide = sub.astype(F32)
            for m in range(2):
                amplitude = (0.35 if m == 0 else 0.6) / math.sqrt(WIDTH)
                first, second, offset = (1.0, 2.0, 0.0) if m == 0 else (3.0, 1.0, 4096.0)
                mid = unit_phase * (wide + (8.0 + first))
                far = unit_phase * (wide + (16.0 + first))

                @pl.loop(0, WIDTH, unroll=2)
                def _(v):
                    times = v.astype(F32) + second
                    step = scaled_cos(unit_phase * (8.0 * times), 2.0)
                    one = scaled_cos(mid * times + offset, amplitude)
                    two = scaled_cos(far * times + offset, amplitude)
                    mats[2 * k + m, v, 8:16] = one
                    mats[2 * k + m, v, 16:24] = two
                    mats[2 * k + m, v, 0:8] = step * one - two
                    mats[2 * k + m, v, 24:32] = step * two - one

    def exchange(send, recv, ss, rs, low, bits, action):
        group = 2 ** bits
        mine = lax.rem(me // 2 ** low, group)

        @pl.loop(1, group)
        def _(i):
            other = lax.rem(mine + i, group)
            here = other if action is finish_recv else mine
            copy = pltpu.make_async_remote_copy(
                send.at[other], recv.at[here], ss.at[other], rs.at[here],
                device_id=(me + (other - mine) * 2 ** low,), device_id_type=MESH)
            action(copy)
        return mine

    def pack(send, group, h):
        places = LANES // group
        for j in range(blocks):
            at = LANES * (blocks * h + j)
            tbuf[j] = cbuf[at:at + LANES, :].T
        for d in range(group):
            for j in range(blocks):
                send[d, places * j:places * (j + 1), :] = tbuf[j, places * d:places * (d + 1), :]

    def unpack(recv, group, h):
        places = LANES // group
        for j in range(blocks):
            for d in range(group):
                tbuf[j, places * d:places * (d + 1), :] = recv[d, places * j:places * (j + 1), :]
        for j in range(blocks):
            at = LANES * (blocks * h + j)
            cbuf[at:at + LANES, :] = tbuf[j].T

    def sketch_of(values, target, make):
        target[...] = jnp.zeros_like(target)

        @pl.loop(0, LEAF // 4)
        def _(c):
            pieces = []
            for i in range(4):
                s = 4 * c + i
                row = pts[columns + 3, pl.ds(s, 1), :]
                high = jnp.floor(row * (1.0 / LOW))
                if make:
                    low = (row - high * LOW).astype(jnp.int32)
                    ids = lax.broadcasted_iota(jnp.int32, (LOW, LANES), 0)
                    onehot[c, :, LANES * i:LANES * (i + 1)] = jnp.where(ids == low, 1.0, 0.0).astype(BF16)
                sign = 2.0 * pts[columns + 4, pl.ds(s, 1), :] - 1.0
                v = values(s) * sign
                top = v.astype(BF16)
                rest = (v - top.astype(F32)).astype(BF16)
                wide = jnp.broadcast_to(high, (columns, LANES))
                masks = [jnp.where(wide == float(g), 1.0, 0.0).astype(BF16) for g in range(HIGH)]
                pieces.append(jnp.concatenate([top * g for g in masks] + [rest * g for g in masks], axis=0))
            left = jnp.concatenate(pieces, axis=1)
            target[...] += lax.dot_general(left, onehot[c], (((1,), (1,)), ((), ())), preferred_element_type=F32)

    nbt = kk

    def start(copy):
        copy.start()

    def finish_recv(copy):
        copy.wait_recv()

    def finish_send(copy):
        copy.wait_send()

    for index, (low, bits) in enumerate(stages):
        group = 2 ** bits
        places = LANES // group

        def outward(h, action):
            at = halves * index + h
            return exchange(a_send.at[at], a_recv.at[at], a_ss.at[at], a_rs.at[at], low, bits, action)

        def homeward(h, action):
            at = halves * index + h
            return exchange(b_send.at[at], b_recv.at[at], b_ss.at[at], b_rs.at[at], low, bits, action)

        for h in range(halves):
            at = halves * index + h
            if index == 0:
                gather_half(h)
            pack(a_send.at[at], group, h)
            if index == 0 and h == 0:
                pl.semaphore_wait(barrier, devices - 1)
            mine = outward(h, start)
            a_recv[at, mine] = a_send[at, mine]
        make_maps(low, bits)
        if index == 0:
            for q in range(columns):
                for s in range(LEAF):
                    nbt[s, q:q + 1, :] = pts[q, s:s + 1, :]
            sketch_of(lambda s: nbt[s], skb, True)
        for h in range(halves):
            at = halves * index + h
            outward(h, finish_recv)
            unpack(a_recv.at[at], group, h)
            half = slice(256 * h, 256 * (h + 1))
            for k in range(low, low + bits):
                span = places * 2 ** (k - low)
                full = cbuf[half, :]
                wide = lax.broadcasted_iota(jnp.int32, full.shape, 1)
                part[half, :] = jnp.where((wide // span) % 2 == 0,
                                          pltpu.roll(full, LANES - span, 1), pltpu.roll(full, span, 1))

                def mix(v, acc):
                    own = [mats[2 * k, v, 8 * t:8 * t + 8] for t in range(4)]
                    cross = [mats[2 * k + 1, v, 8 * t:8 * t + 8] for t in range(4)]
                    out = []
                    for q in range(8):
                        row = cbuf[pl.ds((8 * h + q) * 32 + v, 1), :]
                        other = part[pl.ds((8 * h + q) * 32 + v, 1), :]
                        for t in range(4):
                            out.append(acc[4 * q + t] + own[t] * row + cross[t] * other)
                    return tuple(out)

                init = tuple(0.85 * cbuf[pl.ds((8 * h + q) * 32 + 8 * t, 8), :] for q in range(8) for t in range(4))
                acc = lax.fori_loop(0, WIDTH, mix, init, unroll=2)
                for q in range(8):
                    for t in range(4):
                        cbuf[pl.ds((8 * h + q) * 32 + 8 * t, 8), :] = acc[4 * q + t]
            pack(b_send.at[at], group, h)
            mine = homeward(h, start)
            b_recv[at, mine] = b_send[at, mine]
        for h in range(halves):
            outward(h, finish_send)
        for h in range(halves):
            homeward(h, finish_recv)
            unpack(b_recv.at[halves * index + h], group, h)
        for h in range(halves):
            homeward(h, finish_send)

    for c in range(LEAF // 8):
        def spread_out(w, acc):
            coef = [cbuf[pl.ds(8 * h * 32 + w, 8, stride=32), :] for h in range(halves)]
            out = []
            for s in range(8):
                row = leaf[8 * c + s, pl.ds(w, 1), :]
                for h in range(halves):
                    out.append(acc[halves * s + h] + coef[h] * row)
            return tuple(out)

        init = tuple(
            jnp.broadcast_to(pts[columns + 2, 8 * c + s:8 * c + s + 1, :], (8, LANES)) * nbt[8 * c + s, 8 * h:8 * h + 8]
            for s in range(8) for h in range(halves))
        acc = lax.fori_loop(0, WIDTH, spread_out, init, unroll=2)
        for s in range(8):
            for h in range(halves):
                part[(8 * c + s) * columns + 8 * h:(8 * c + s) * columns + 8 * h + 8, :] = acc[halves * s + h]

    inner = jnp.zeros((columns, LANES), F32)
    square, energy = inner, inner
    for s in range(LEAF):
        v, image = nbt[s], part[s * columns:(s + 1) * columns, :]
        inner, square, energy = inner + v * image, square + v * v, energy + image * image
    lane_q = lax.broadcasted_iota(jnp.int32, (columns, LANES), 1)
    row_q = lax.broadcasted_iota(jnp.int32, (columns, LANES), 0)
    packed = jnp.zeros((columns, LANES), F32)
    for i, value in enumerate((inner, square, energy)):
        packed = jnp.where(lane_q == row_q + columns * i, jnp.sum(value, axis=1, keepdims=True), packed)
    sum_send[...] = jnp.sum(packed, axis=0, keepdims=True)

    def to_all(source, recv, ss, rs, action):
        @pl.loop(1, devices)
        def _(i):
            other = lax.rem(me + i, devices)
            here = other if action is finish_recv else me
            action(pltpu.make_async_remote_copy(
                source(other), recv.at[here], ss.at[other], rs.at[here],
                device_id=(other,), device_id_type=MESH))

    to_all(lambda d: sum_send, sum_recv, s_ss, s_rs, start)
    sum_recv[me] = sum_send[...]
    sketch_of(lambda s: part[pl.ds(pl.multiple_of(s * columns, columns), columns), :], ski, False)
    to_all(lambda d: sum_send, sum_recv, s_ss, s_rs, finish_recv)
    totals = jnp.sum(sum_recv[...], axis=0)

    def column(i):
        picked = jnp.where(lane_q == row_q + columns * i, jnp.broadcast_to(totals, (columns, LANES)), 0.0)
        return jnp.broadcast_to(jnp.sum(picked, axis=1, keepdims=True) * (1.0 / total_points), (columns, LANES))

    inner_mean, square_mean, energy_mean = column(0), column(1), column(2)
    projection = inner_mean / (square_mean + EPSILON)
    energy = energy_mean - 2.0 * projection * inner_mean + projection * projection * square_mean
    spread = jnp.sqrt(energy + EPSILON)
    inverse = 1.0 / spread
    for i, value in enumerate((projection, spread)):
        arn_ref[i:i + 1, :] = jnp.sum(jnp.where(lane_q == row_q, value, 0.0), axis=0, keepdims=True)[:, :columns]

    rows_each = rs_send.shape[1]
    factor = math.sqrt(SKETCH / total_points)
    lowest = HIGH * columns
    part_tiles = LOW // LANES
    for n in range(devices):
        flat = n * rows_each
        tile, row = flat // 8, flat % 8
        strip, side = tile // part_tiles, tile % part_tiles
        top = strip * 8 + row
        q0 = top % columns
        cols = slice(side * LANES, (side + 1) * LANES)
        img = ski[top:top + rows_each, cols] + ski[lowest + top:lowest + top + rows_each, cols]
        bas = skb[top:top + rows_each, cols] + skb[lowest + top:lowest + top + rows_each, cols]
        rs_send[n] = (img - projection[q0:q0 + rows_each] * bas) * (factor * inverse[q0:q0 + rows_each])
    to_all(lambda d: rs_send.at[d], rs_recv, r_ss, r_rs, start)
    rs_recv[me] = rs_send[me]

    for s in range(LEAF):
        pts_rows = (part[s * columns:(s + 1) * columns, :] - projection * nbt[s]) * inverse
        nbt[s] = pts_rows
    for q in range(columns):
        for s in range(LEAF):
            pts[q, s:s + 1, :] = nbt[s, q:q + 1, :]
    for i in range(columns // 4):
        for j in range(4):
            for g in range(4):
                tbuf[0, 32 * g:32 * g + 32, 32 * j:32 * j + 32] = pts[4 * i + j, :, 32 * g:32 * g + 32]
        raw[LANES * i:LANES * (i + 1), :] = tbuf[0].T
    for r in range(LANES // 4):
        for h in range(halves):
            nb_ref[8 * h:8 * h + 8, LANES * r:LANES * (r + 1)] = raw[pl.ds(256 * h + r, 8, stride=32), :]

    to_all(lambda d: rs_send.at[d], rs_recv, r_ss, r_rs, finish_recv)
    own_chunk[...] = jnp.sum(rs_recv[...], axis=0)
    to_all(lambda d: own_chunk, ag_recv, g_ss, g_rs, start)
    ag_recv[me] = own_chunk[...]
    to_all(lambda d: sum_send, sum_recv, s_ss, s_rs, finish_send)
    to_all(lambda d: rs_send.at[d], rs_recv, r_ss, r_rs, finish_send)
    to_all(lambda d: own_chunk, ag_recv, g_ss, g_rs, finish_recv)
    for n in range(devices):
        flat = n * rows_each
        tile, row = flat // 8, flat % 8
        strip, side = tile // part_tiles, tile % part_tiles
        top = strip * 8 + row
        q0, high = top % columns, top // columns
        begin = high * LOW + side * LANES
        sketch_ref[q0:q0 + rows_each, begin:begin + LANES] = ag_recv[n]
    to_all(lambda d: own_chunk, ag_recv, g_ss, g_rs, finish_send)


def split(x):
    top = x.astype(BF16)
    return top, (x - top.astype(F32)).astype(BF16)


def tile_kernel(devices, total_points, scale_ref, v_in, coords_in, diag_in, rows_in, signs_in,
                nb_ref, sketch_ref, arn_ref, v_ref, coords_ref, diag_ref, rows_ref, signs_ref,
                small_send, small, vals, phases, steps, mats, leaf, state, coef,
                image, back, hot, left, masks, sum_send, sum_recv, sum_total, sum_joined, rb_send,
                rb_recv, rb_total, rb_joined, ri_send, ri_recv, ri_total, ri_joined, ag_recv, own_chunk, sems,
                io_sems):
    me = lax.axis_index("box")
    columns = nb_ref.shape[0]
    sections = devices.bit_length() - 1
    per_tile = LANES // LEAF
    half = LANES // 2
    barrier = pltpu.get_barrier_semaphore()

    @pl.loop(1, devices)
    def _(i):
        pl.semaphore_signal(barrier, inc=1, device_id=(lax.rem(me + i, devices),), device_id_type=MESH)

    incoming = [pltpu.make_async_copy(a, b, io_sems.at[i]) for i, (a, b) in enumerate((
        (v_in, v_ref), (coords_in, coords_ref), (diag_in, diag_ref), (rows_in, rows_ref), (signs_in, signs_ref)))]
    for copy in incoming:
        copy.start()
    lane = lax.broadcasted_iota(jnp.int32, (8, LANES), 1)
    sub = lax.broadcasted_iota(jnp.int32, (8, LANES), 0)
    planes = 4
    plane_size = devices // planes
    plane, seat = me // plane_size, lax.rem(me, plane_size)
    halves = devices // 2
    side = plane // 2

    def facing(away):
        there = 0
        for b in range(planes.bit_length() - 1):
            bit = lax.rem(plane // 2 ** b, 2)
            there = there + 2 ** b * ((1 - bit) if (away >> b) & 1 else bit)
        return there

    def send(source, target, which, other):
        pltpu.make_async_remote_copy(
            source, target, sems.at[2 * which], sems.at[2 * which + 1],
            device_id=(other,), device_id_type=MESH).start()

    def to_all(source, target, which, aways):
        for away in aways:
            there = facing(away)

            @pl.loop(0 if away else 1, plane_size)
            def _(i):
                other = plane_size * there + lax.rem(seat + i, plane_size)
                send(source(other), target, which, other)

    def to_plane(source, target, which):
        @pl.loop(1, plane_size)
        def _(i):
            other = lax.rem(seat + i, plane_size)
            send(source(other), target, which, plane_size * plane + other)

    def to_planes(source, target, which):
        for away in range(planes - 1, 0, -1):
            send(source, target, which, plane_size * facing(away) + seat)

    def finish(ref, which, end):
        pltpu.make_async_copy(ref, ref, sems.at[2 * which + end]).wait()

    def columns_at(ref, tile):
        return ref.at[:, pl.ds(pl.multiple_of(tile * LANES, LANES), LANES)]

    others, mates, peers = pl.ds(0, devices - 1), pl.ds(0, plane_size - 1), pl.ds(0, planes - 1)
    side_rows = 5
    side_part = pl.ds(0, side_rows)

    for copy in incoming:
        copy.wait()
    rows_f, signs_f = rows_ref[...].astype(F32), signs_ref[...].astype(F32)
    for e in range(devices):
        here = slice(e * LANES, (e + 1) * LANES)
        small_send[e, 0:2, :] = coords_ref[:, here].astype(F32)
        small_send[e, 2:3, :] = diag_ref[e:e + 1, :]
        small_send[e, 3:4, :] = rows_f[e:e + 1, :]
        small_send[e, 4:5, :] = signs_f[e:e + 1, :]
    scale = lax.rem(scale_ref[0], MODULUS)
    spot = lane // LEAF
    inner_lane = (lane % LEAF).astype(F32)
    for k in range(sections):
        for g in range(devices // 8):
            ident = ((8 * g + sub) * LANES + per_tile * me + spot) * 37
            x = (ident + 101 * k).astype(F32)
            rest = x - jnp.floor(x * (1.0 / (MODULUS - 1))) * float(MODULUS - 1)
            rest = jnp.where(rest < 0.0, rest + float(MODULUS - 1), rest)
            rest = jnp.where(rest >= float(MODULUS - 1), rest - float(MODULUS - 1), rest)
            key = rest.astype(jnp.int32) + 1
            unit_phase = fold(fold(key * scale)).astype(F32)
            for m, second in enumerate((2.0, 1.0)):
                phi = remainder(unit_phase * (inner_lane + second))
                phases[2 * k + m, 8 * g:8 * g + 8, :] = phi
                steps[2 * k + m, 8 * g:8 * g + 8, :] = scaled_cos(8.0 * phi, 2.0)

    wide_sub = lax.broadcasted_iota(jnp.int32, (WIDTH, LANES), 0)
    wide_lane = lax.broadcasted_iota(jnp.int32, (WIDTH, LANES), 1)
    ident_part = jnp.where(wide_lane % WIDTH == wide_sub, 0.85, 0.0)
    sub_f = sub.astype(F32)
    def make_maps(begins, ends):
        for k in range(sections):
            maps_of(k, begins[k], ends[k])

    def maps_of(k, begin_pair, end_pair):
        stride = 2 ** k

        @pl.loop(begin_pair, end_pair)
        def _(pair):
            first_tile = (pair // stride) * (2 * stride) + pair % stride
            for bit in range(2):
                d = first_tile + stride * bit
                for m in range(2):
                    amplitude = (0.35 if m == 0 else 0.6) / math.sqrt(WIDTH)
                    first, offset = (1.0, 0.0) if m == 0 else (3.0, 4096.0)
                    phi = phases[2 * k + m, pl.ds(d, 1), :]
                    step = steps[2 * k + m, pl.ds(d, 1), :]
                    one = scaled_cos(phi * (sub_f + (8.0 + first)) + offset, amplitude)
                    two = scaled_cos(phi * (sub_f + (16.0 + first)) + offset, amplitude)
                    full = jnp.concatenate([step * one - two, one, two, step * two - one], axis=0)
                    if m == 0:
                        full = full + ident_part
                    top, low = split(full)
                    begin = LANES * (bit if m == 0 else 1 - bit)
                    mats[k, pair, 64 * bit:64 * bit + 32, begin:begin + LANES] = top
                    mats[k, pair, 64 * bit + 32:64 * bit + 64, begin:begin + LANES] = low

    hops = lax.rem(me // 2, 2) + lax.rem(me // 4, 2) + plane
    budget = 18 * (5 - hops) - 8
    early = [jnp.clip(budget - k * (devices // 2), 0, devices // 2) for k in range(sections)]
    make_maps([0] * sections, early)
    pl.semaphore_wait(barrier, devices - 1)
    for which, aways in ((0, (3, 2)), (7, (1, 0))):
        to_all(lambda d: small_send.at[d, side_part], small.at[me, side_part], which, aways)
    for which, aways in ((1, (3, 2)), (8, (1, 0))):
        to_all(lambda d: columns_at(v_ref, d), vals.at[me], which, aways)
    small[me] = small_send[me]
    vals[me] = columns_at(v_ref, me)[...]

    make_maps(early, [devices // 2] * sections)
    lanes_q = lax.broadcasted_iota(jnp.int32, (columns, LANES), 1)
    rows_q = lax.broadcasted_iota(jnp.int32, (columns, LANES), 0)

    def place(tile):
        return pl.ds(pl.multiple_of(tile * LANES, LANES), LANES)

    def make_hot(row_of, sign_of, begin, count):
        @pl.loop(0, count)
        def _(i):
            d = begin + i
            row = row_of(d)
            high = jnp.floor(row * (1.0 / LOW))
            low = (row - high * LOW).astype(jnp.int32)
            ids = lax.broadcasted_iota(jnp.int32, (LOW, LANES), 0)
            hot[:, place(d)] = jnp.where(ids == low, 1.0, 0.0).astype(BF16)
            sign = jnp.broadcast_to(2.0 * sign_of(d) - 1.0, (columns, LANES))
            wide = jnp.broadcast_to(high, (columns, LANES))
            for g in range(HIGH):
                masks[d, columns * g:columns * (g + 1), :] = jnp.where(wide == float(g), sign, 0.0).astype(BF16)

    def place_values(d, at, value):
        top, rest = split(value)
        for g in range(HIGH):
            mask = masks[d, columns * g:columns * (g + 1), :]
            left[columns * g:columns * (g + 1), at] = top * mask
            left[columns * (HIGH + g):columns * (HIGH + g + 1), at] = rest * mask

    def sketch_product():
        o = lax.dot_general(left[...], hot[...], (((1,), (1,)), ((), ())), preferred_element_type=F32)
        return o[:HIGH * columns] + o[HIGH * columns:]

    factor = math.sqrt(SKETCH / total_points)

    def start_reduce(sk, pieces, landed, which):
        for n in range(plane_size):
            pieces[n] = sk[columns * n:columns * (n + 1), :]
        to_plane(lambda n: pieces.at[n], landed.at[seat], which)
        landed[seat] = pieces[seat]

    def next_reduce(landed, total, joined, which, first):
        finish(landed.at[pl.ds(0, plane_size - 1)], first, 1)
        total[...] = jnp.sum(landed[...], axis=0)
        to_planes(total, joined.at[plane], which)
        joined[plane] = total[...]

    make_hot(lambda d: rows_ref[pl.ds(d, 1), :].astype(F32), lambda d: signs_ref[pl.ds(d, 1), :].astype(F32), 0, devices)

    @pl.loop(0, devices)
    def _(d):
        place_values(d, place(d), v_ref[:, place(d)])

    basis_sketch = sketch_product()
    start_reduce(basis_sketch, rb_send, rb_recv, 2)

    fx = (sub % 4 + 1).astype(F32)
    fy = (sub // 4 + 1).astype(F32)
    unit = 1.0 / math.sqrt(LEAF)
    point_masks = [jnp.where(lanes_q // LEAF == j, 1.0, 0.0).astype(BF16) for j in range(per_tile)]
    column_masks = [jnp.where((wide_lane % half) // columns == j, 1.0, 0.0).astype(BF16) for j in range(per_tile)]
    first_half = wide_lane < half

    def combine(o):
        s = o[0:32] + o[32:64]
        return s + pltpu.roll(s, half, 1)

    def expand(total):
        top = total.astype(BF16).astype(F32)
        y = jnp.where(first_half, top, total - top).astype(BF16)
        return jnp.concatenate([y * m for m in column_masks], axis=0)

    def leaves(begin):
        @pl.loop(0, halves)
        def _(i):
            d = begin + i
            pair = fold(small[d, 0:2, :].astype(jnp.int32) * scale).astype(F32)
            px, py = pair[0:1], pair[1:2]
            phases_of = [fx * px + (fy + 2.0 * t) * py for t in range(2)]
            full = jnp.concatenate([scaled_cos(n, unit) for n in phases_of] + [scaled_sin(n, unit) for n in phases_of], axis=0)
            top, low = split(full)
            leaf[d, 0:32] = top
            leaf[d, 32:64] = low

    def gather(begin):
        for i in range(halves):
            d = begin + i
            top, rest = split(vals[d])
            spread_v = jnp.concatenate([top * m for m in point_masks] + [rest * m for m in point_masks], axis=0)
            o = lax.dot_general(leaf[d], spread_v, (((1,), (1,)), ((), ())), preferred_element_type=F32)
            state[0, d] = expand(combine(o))

    def section(k, begin, count):
        stride = 2 ** k
        now = k % 2
        for i in range(count // 2):
            d0 = begin + (i // stride) * (2 * stride) + i % stride
            d1 = d0 + stride
            x = jnp.concatenate([state[now, d0], state[now, d1]], axis=0)
            o = jnp.dot(mats[k, begin // 2 + i], x, preferred_element_type=F32)
            for d, part in ((d0, o[0:64]), (d1, o[64:128])):
                total = combine(part)
                if k == sections - 1:
                    coef[32 * d:32 * d + 32, :] = total
                else:
                    state[1 - now, d] = expand(total)

    near, away = side * halves, (1 - side) * halves
    for begin, small_which, count in ((near, 7, halves - 1), (away, 0, halves)):
        finish(small.at[pl.ds(0, count), side_part], small_which, 1)
        leaves(begin)
        make_hot(lambda d: small[d, 3:4, :], lambda d: small[d, 4:5, :], begin, halves)
    for begin, vals_which, count in ((near, 8, halves - 1), (away, 1, halves)):
        arrived = pl.ds(0, count)
        finish(vals.at[arrived], vals_which, 1)
        gather(begin)
        for k in range(sections - 1):
            section(k, begin, halves)
    next_reduce(rb_recv, rb_total, rb_joined, 9, 2)
    section(sections - 1, 0, devices)
    tile_lane = lax.broadcasted_iota(jnp.int32, (half, 2 * LANES), 1)
    tile_masks = [jnp.where((tile_lane % LANES) // WIDTH == t, 1.0, 0.0).astype(BF16) for t in range(4)]
    zero = jnp.zeros((columns, LANES), F32)
    inner, square, energy = zero, zero, zero
    for g in range(devices // 4):
        flipped = coef[LANES * g:LANES * (g + 1), :].T
        top, rest = split(flipped[0:half])
        both = jnp.concatenate([top, rest], axis=1)
        lhs = jnp.concatenate([both * m for m in tile_masks], axis=0)
        tops = jnp.concatenate([leaf[4 * g + t, 0:32] for t in range(4)], axis=0)
        lows = jnp.concatenate([leaf[4 * g + t, 32:64] for t in range(4)], axis=0)
        right = jnp.concatenate([tops, lows], axis=1)
        o = jnp.dot(lhs, jnp.concatenate([right, right], axis=0), preferred_element_type=F32)
        o = o[:, 0:LANES] + o[:, LANES:2 * LANES]
        for t in range(4):
            d = 4 * g + t
            v = vals[d]
            img = jnp.broadcast_to(small[d, 2:3, :], (columns, LANES)) * v
            for j in range(per_tile):
                begin = half * t + columns * j
                img = img + jnp.where(lanes_q // LEAF == j, o[begin:begin + columns], 0.0)
            image[d] = img
            place_values(d, slice(LANES * d, LANES * (d + 1)), img)
            inner, square, energy = inner + v * img, square + v * v, energy + img * img

    to_all(lambda d: image.at[d], back.at[me], 5, (3, 2, 1, 0))
    packed = zero
    for i, value in enumerate((inner, square, energy)):
        packed = jnp.where(lanes_q == rows_q + columns * i, jnp.sum(value, axis=1, keepdims=True), packed)
    sum_send[...] = jnp.sum(packed, axis=0, keepdims=True)
    image_sketch = sketch_product()
    start_reduce(image_sketch, ri_send, ri_recv, 4)
    to_plane(lambda d: sum_send, sum_recv.at[seat], 3)
    sum_recv[seat] = sum_send[...]
    back[me] = image[me]

    finish(small_send.at[pl.ds(0, halves), side_part], 0, 0)
    finish(small_send.at[pl.ds(0, halves - 1), side_part], 7, 0)
    finish(vals.at[pl.ds(0, halves)], 1, 0)
    finish(vals.at[pl.ds(0, halves - 1)], 8, 0)
    finish(rb_send.at[mates], 2, 0)
    next_reduce(ri_recv, ri_total, ri_joined, 11, 4)
    finish(sum_recv.at[mates], 3, 1)
    sum_total[...] = jnp.sum(sum_recv[...], axis=0)
    to_planes(sum_total, sum_joined.at[plane], 10)
    sum_joined[plane] = sum_total[...]
    finish(rb_joined.at[peers], 9, 0)
    finish(rb_joined.at[peers], 9, 1)
    finish(sum_recv.at[mates], 3, 0)
    finish(ri_send.at[mates], 4, 0)
    basis_total = jnp.sum(rb_joined[...], axis=0)
    finish(sum_joined.at[peers], 10, 1)
    totals = jnp.sum(sum_joined[...], axis=0)

    def column(i):
        picked = jnp.where(lanes_q == rows_q + columns * i, jnp.broadcast_to(totals, (columns, LANES)), 0.0)
        return jnp.broadcast_to(jnp.sum(picked, axis=1, keepdims=True) * (1.0 / total_points), (columns, LANES))

    inner_mean, square_mean, energy_mean = column(0), column(1), column(2)
    projection = inner_mean / (square_mean + EPSILON)
    energy = energy_mean - 2.0 * projection * inner_mean + projection * projection * square_mean
    spread = jnp.sqrt(energy + EPSILON)
    inverse = 1.0 / spread
    for i, value in enumerate((projection, spread)):
        arn_ref[i:i + 1, :] = jnp.sum(jnp.where(lanes_q == rows_q, value, 0.0), axis=0, keepdims=True)[:, :columns]
    finish(ri_joined.at[peers], 11, 1)
    wide = lambda x: jnp.concatenate([x] * (LOW // LANES), axis=1)
    own_chunk[...] = (jnp.sum(ri_joined[...], axis=0) - basis_total * wide(projection)) * wide(factor * inverse)
    to_plane(lambda d: own_chunk, ag_recv.at[seat], 6)
    ag_recv[seat] = own_chunk[...]
    finish(back.at[others], 5, 1)
    for e in range(devices):
        here = slice(e * LANES, (e + 1) * LANES)
        nb_ref[:, here] = (back[e] - projection * v_ref[:, here]) * inverse
    finish(image.at[others], 5, 0)
    finish(ri_joined.at[peers], 11, 0)
    finish(sum_joined.at[peers], 10, 0)
    finish(ag_recv.at[mates], 6, 0)
    finish(ag_recv.at[mates], 6, 1)
    for n in range(plane_size):
        sketch_ref[:, LOW * n:LOW * (n + 1)] = ag_recv[n]


def together(devices, basis_vector, diagonal, coords, phase_scale, sketch_rows, sketch_signs):
    columns, local_points = basis_vector.shape
    sections = devices.bit_length() - 1
    plane = (local_points // LANES, LANES)
    far = pl.BlockSpec(memory_space=pltpu.HBM)
    vmem = pl.BlockSpec(memory_space=pltpu.VMEM)
    tile = pltpu.VMEM((devices, columns, LANES), F32)
    chunk = (columns, LOW)
    pieces = pltpu.VMEM((HIGH,) + chunk, F32)
    reduce_parts = [pieces, pieces, pltpu.VMEM(chunk, F32), pltpu.VMEM((devices // HIGH,) + chunk, F32)]
    return pl.pallas_call(
        functools.partial(tile_kernel, devices, local_points * devices),
        out_shape=(
            jax.ShapeDtypeStruct((columns, local_points), F32),
            jax.ShapeDtypeStruct((columns, SKETCH), F32),
            jax.ShapeDtypeStruct((2, columns), F32)),
        in_specs=[pl.BlockSpec(memory_space=pltpu.SMEM)] + [far] * 5,
        out_specs=(vmem,) * 3,
        scratch_shapes=[
            pltpu.VMEM(basis_vector.shape, F32),
            pltpu.VMEM(coords.shape, jnp.int32),
            pltpu.VMEM(plane, F32),
            pltpu.VMEM(plane, jnp.int32),
            pltpu.VMEM(plane, jnp.int32),
            pltpu.VMEM((devices, 8, LANES), F32),
            pltpu.VMEM((devices, 8, LANES), F32),
            tile,
            pltpu.VMEM((2 * sections, devices, LANES), F32),
            pltpu.VMEM((2 * sections, devices, LANES), F32),
            pltpu.VMEM((sections, devices // 2, 4 * WIDTH, 2 * LANES), BF16),
            pltpu.VMEM((devices, 2 * WIDTH, LANES), BF16),
            pltpu.VMEM((2, devices, LANES, LANES), BF16),
            pltpu.VMEM((devices * WIDTH, LANES), F32),
            tile, tile,
            pltpu.VMEM((LOW, local_points), BF16),
            pltpu.VMEM((2 * HIGH * columns, local_points), BF16),
            pltpu.VMEM((devices, HIGH * columns, LANES), BF16),
            pltpu.VMEM((1, LANES), F32),
            pltpu.VMEM((HIGH, 1, LANES), F32),
            pltpu.VMEM((1, LANES), F32),
            pltpu.VMEM((devices // HIGH, 1, LANES), F32),
            *reduce_parts, *reduce_parts, pieces,
            pltpu.VMEM(chunk, F32),
            pltpu.SemaphoreType.DMA((24,)),
            pltpu.SemaphoreType.DMA((5,)),
        ],
        compiler_params=pltpu.CompilerParams(
            collective_id=0, has_side_effects=True, vmem_limit_bytes=24 * 2**20),
        name="gmres",
    )(phase_scale, *(pltpu.with_memory_space_constraint(x, pltpu.HBM) for x in (
        basis_vector, coords, diagonal.reshape(plane), sketch_rows.reshape(plane),
        sketch_signs.reshape(plane))))


def body(basis_vector, diagonal, coords, phase_scale, sketch_rows, sketch_signs):
    columns, local_points = basis_vector.shape
    devices = lax.axis_size("box")
    if devices * LANES == local_points:
        return together(devices, basis_vector, diagonal, coords, phase_scale, sketch_rows, sketch_signs)
    sections = devices.bit_length() - 1
    count = -(-sections // 5)
    stages, low = [], 0
    for i in range(count):
        bits = (sections - low) // (count - i)
        stages.append((low, bits))
        low += bits
    group = 2 ** max(bits for _, bits in stages)
    group_rows = [columns * WIDTH // LANES * (LANES // 2 ** bits) for _, bits in stages]
    plane = (local_points // LANES, LANES)
    rows_each = HIGH * columns * LOW // LANES // devices
    vmem = pl.BlockSpec(memory_space=pltpu.VMEM)
    dma = pltpu.SemaphoreType.DMA
    count_rows = max(group_rows)
    halves = columns // 8
    new_basis, sketch, arn = pl.pallas_call(
        functools.partial(kernel, devices, stages, local_points * devices),
        out_shape=(
            jax.ShapeDtypeStruct((columns, local_points), F32),
            jax.ShapeDtypeStruct((columns, SKETCH), F32),
            jax.ShapeDtypeStruct((2, columns), F32)),
        in_specs=[pl.BlockSpec(memory_space=pltpu.SMEM), vmem, vmem, vmem, vmem, vmem],
        out_specs=(vmem, vmem, vmem),
        scratch_shapes=[
            pltpu.VMEM(((columns + 8) * LEAF, LANES), F32),
            pltpu.VMEM((columns + 8, LEAF, LANES), F32),
            pltpu.VMEM((LEAF, WIDTH, LANES), F32),
            pltpu.VMEM((2 * sections, WIDTH, WIDTH, LANES), F32),
            pltpu.VMEM((LEAF, columns, LANES), F32),
            pltpu.VMEM((columns * WIDTH, LANES), F32),
            pltpu.VMEM((columns * WIDTH, LANES), F32),
            pltpu.VMEM((columns * WIDTH // LANES, LANES, LANES), F32),
            pltpu.VMEM((2, LEAF, LANES), F32),
            pltpu.VMEM((LEAF // 4, LOW, 4 * LANES), BF16),
            pltpu.VMEM((2 * HIGH * columns, LOW), F32),
            pltpu.VMEM((2 * HIGH * columns, LOW), F32),
            pltpu.VMEM((count * halves, group, count_rows // halves, LANES), F32),
            pltpu.VMEM((count * halves, group, count_rows // halves, LANES), F32),
            pltpu.VMEM((count * halves, group, count_rows // halves, LANES), F32),
            pltpu.VMEM((count * halves, group, count_rows // halves, LANES), F32),
            pltpu.VMEM((1, LANES), F32),
            pltpu.VMEM((devices, 1, LANES), F32),
            pltpu.VMEM((devices, rows_each, LANES), F32),
            pltpu.VMEM((devices, rows_each, LANES), F32),
            pltpu.VMEM((devices, rows_each, LANES), F32),
            pltpu.VMEM((rows_each, LANES), F32),
            dma((count * halves, group)), dma((count * halves, group)), dma((count * halves, group)), dma((count * halves, group)),
            dma((devices,)), dma((devices,)), dma((devices,)), dma((devices,)), dma((devices,)), dma((devices,)),
        ],
        compiler_params=pltpu.CompilerParams(
            collective_id=0, has_side_effects=True, vmem_limit_bytes=60 * 2**20),
        name="gmres",
    )(phase_scale, basis_vector, coords, diagonal.reshape(plane), sketch_rows.reshape(plane),
      sketch_signs.reshape(plane))
    return new_basis, sketch, arn


def solution(mesh):
    placed = (P(None, "box"), P("box"), P(None, "box"), P(), P("box"), P("box"))
    return jax.shard_map(
        body, mesh=mesh, in_specs=placed, out_specs=(P(None, "box"), P(), P()), check_vma=False
    )
```

```python
import functools
import math

import jax
import jax.numpy as jnp
import numpy as np
from jax import lax
from jax.experimental import pallas as pl
from jax.experimental.pallas import tpu as pltpu
from jax.sharding import PartitionSpec as P

WIDTH = 32
LEAF = 32
SKETCH = 2048
LANES = 128
HIGH = 8
LOW = SKETCH // HIGH
MODULUS = 8191
EPSILON = 1e-06
MESH = pl.DeviceIdType.MESH
F32 = jnp.float32
BF16 = jnp.bfloat16


def sine_series():
    node = np.cos((np.arange(400) + 0.5) * np.pi / 800)
    basis = np.stack([node ** (2 * i) for i in range(6)], 1)
    exact = np.sin(np.pi * node * 4096 / MODULUS) / node
    return np.linalg.lstsq(basis, exact, rcond=None)[0]


SERIES = sine_series()


def remainder(n):
    return n - jnp.floor(n * (1.0 / MODULUS) + 0.5) * float(MODULUS)


def half_sine(n, gain):
    t = remainder(n) * (1.0 / 4096)
    z = t * t
    total = z * float(SERIES[5] * gain) + float(SERIES[4] * gain)
    for c in SERIES[3::-1]:
        total = total * z + float(c * gain)
    return total * t


def scaled_cos(n, amplitude):
    s = half_sine(n, math.sqrt(2.0 * amplitude))
    return amplitude - s * s


def scaled_sin(n, amplitude):
    return scaled_cos(n - 0.25 * MODULUS, amplitude)


def fold(p):
    return (p & MODULUS) + lax.shift_right_logical(p, 13)


def kernel(devices, stages, total_points, scale_ref, v_ref, coords_ref, diag_ref, rows_ref, signs_ref,
           nb_ref, sketch_ref, arn_ref, raw, pts, leaf, mats, kk, cbuf, part, tbuf, work, onehot, skb, ski,
           a_send, a_recv, b_send, b_recv, sum_send, sum_recv, rs_send, rs_recv, ag_recv, own_chunk,
           a_ss, a_rs, b_ss, b_rs, s_ss, s_rs, r_ss, r_rs, g_ss, g_rs):
    me = lax.axis_index("box")
    columns = nb_ref.shape[0]
    halves = columns // 8
    barrier = pltpu.get_barrier_semaphore()

    @pl.loop(1, devices)
    def _(i):
        pl.semaphore_signal(barrier, inc=1, device_id=(lax.rem(me + i, devices),), device_id_type=MESH)

    lane = lax.broadcasted_iota(jnp.int32, (8, LANES), 1)
    sub = lax.broadcasted_iota(jnp.int32, (8, LANES), 0)
    scale = lax.rem(scale_ref[0], MODULUS)

    for r in range(LANES // 4):
        here = slice(LANES * r, LANES * (r + 1))
        for h in range(halves):
            raw[pl.ds(256 * h + r, 8, stride=32), :] = v_ref[8 * h:8 * h + 8, here]
        pair = coords_ref[:, here].astype(F32)
        raw[columns * 32 + r:columns * 32 + r + 1, :] = pair[0:1]
        raw[columns * 32 + 32 + r:columns * 32 + 33 + r, :] = pair[1:2]
    raw[(columns + 2) * 32:(columns + 3) * 32, :] = diag_ref[...]
    raw[(columns + 3) * 32:(columns + 4) * 32, :] = rows_ref[...].astype(F32)
    raw[(columns + 4) * 32:(columns + 5) * 32, :] = signs_ref[...].astype(F32)
    raw[(columns + 5) * 32:(columns + 8) * 32, :] = jnp.zeros((96, LANES), F32)
    for i in range((columns + 8) // 4):
        flipped = raw[LANES * i:LANES * (i + 1), :].T
        tbuf[0] = flipped
        for j in range(4):
            pts[4 * i + j] = jnp.concatenate(
                [tbuf[0, 32 * g:32 * g + 32, 32 * j:32 * j + 32] for g in range(4)], axis=1)

    def exact_phase(row):
        return fold(pts[columns + row].astype(jnp.int32) * scale).astype(F32)

    work[0] = exact_phase(0)
    work[1] = exact_phase(1)
    fx = (sub % 4 + 1).astype(F32)
    fy = (sub // 4 + 1).astype(F32)
    unit = 1.0 / math.sqrt(LEAF)

    @pl.loop(0, LEAF)
    def _(s):
        px = work[0, pl.ds(s, 1), :]
        py = work[1, pl.ds(s, 1), :]
        for tile in range(2):
            n = fx * px + (fy + 2.0 * tile) * py
            leaf[s, 8 * tile:8 * tile + 8] = scaled_cos(n, unit)
            leaf[s, 16 + 8 * tile:24 + 8 * tile] = scaled_sin(n, unit)

    def gather_half(h):
        def gather(s, acc):
            tiles = [leaf[s, 8 * t:8 * t + 8] for t in range(4)]
            out = []
            for q in range(8):
                row = pts[8 * h + q, pl.ds(s, 1), :]
                for t in range(4):
                    out.append(acc[4 * q + t] + tiles[t] * row)
            return tuple(out)

        acc = lax.fori_loop(0, LEAF, gather, tuple(jnp.zeros((8, LANES), F32) for _ in range(32)), unroll=2)
        for q in range(8):
            for t in range(4):
                cbuf[pl.ds((8 * h + q) * 32 + 8 * t, 8), :] = acc[4 * q + t]

    blocks = 8 * WIDTH // LANES

    def make_maps(low, bits):
        group = 2 ** bits
        places = LANES // group
        mine = lax.rem(me // 2 ** low, group)
        spot = mine * places + lane % places
        box = 4 * (spot % 32) + spot // 32
        member = me + (lane // places - mine) * 2 ** low
        ident = (member * LANES + box) * 37

        @pl.loop(low, low + bits)
        def _(k):
            x = (ident + 101 * k).astype(F32)
            rest = x - jnp.floor(x * (1.0 / (MODULUS - 1))) * float(MODULUS - 1)
            rest = jnp.where(rest < 0.0, rest + float(MODULUS - 1), rest)
            rest = jnp.where(rest >= float(MODULUS - 1), rest - float(MODULUS - 1), rest)
            key = rest.astype(jnp.int32) + 1
            unit_phase = fold(fold(key * scale)).astype(F32)
            wide = sub.astype(F32)
            for m in range(2):
                amplitude = (0.35 if m == 0 else 0.6) / math.sqrt(WIDTH)
                first, second, offset = (1.0, 2.0, 0.0) if m == 0 else (3.0, 1.0, 4096.0)
                mid = unit_phase * (wide + (8.0 + first))
                far = unit_phase * (wide + (16.0 + first))

                @pl.loop(0, WIDTH, unroll=2)
                def _(v):
                    times = v.astype(F32) + second
                    step = scaled_cos(unit_phase * (8.0 * times), 2.0)
                    one = scaled_cos(mid * times + offset, amplitude)
                    two = scaled_cos(far * times + offset, amplitude)
                    mats[2 * k + m, v, 8:16] = one
                    mats[2 * k + m, v, 16:24] = two
                    mats[2 * k + m, v, 0:8] = step * one - two
                    mats[2 * k + m, v, 24:32] = step * two - one

    def exchange(send, recv, ss, rs, low, bits, action):
        group = 2 ** bits
        mine = lax.rem(me // 2 ** low, group)

        @pl.loop(1, group)
        def _(i):
            other = lax.rem(mine + i, group)
            here = other if action is finish_recv else mine
            copy = pltpu.make_async_remote_copy(
                send.at[other], recv.at[here], ss.at[other], rs.at[here],
                device_id=(me + (other - mine) * 2 ** low,), device_id_type=MESH)
            action(copy)
        return mine

    def pack(send, group, h):
        places = LANES // group
        for j in range(blocks):
            at = LANES * (blocks * h + j)
            tbuf[j] = cbuf[at:at + LANES, :].T
        for d in range(group):
            for j in range(blocks):
                send[d, places * j:places * (j + 1), :] = tbuf[j, places * d:places * (d + 1), :]

    def unpack(recv, group, h):
        places = LANES // group
        for j in range(blocks):
            for d in range(group):
                tbuf[j, places * d:places * (d + 1), :] = recv[d, places * j:places * (j + 1), :]
        for j in range(blocks):
            at = LANES * (blocks * h + j)
            cbuf[at:at + LANES, :] = tbuf[j].T

    def sketch_of(values, target, make):
        target[...] = jnp.zeros_like(target)

        @pl.loop(0, LEAF // 4)
        def _(c):
            pieces = []
            for i in range(4):
                s = 4 * c + i
                row = pts[columns + 3, pl.ds(s, 1), :]
                high = jnp.floor(row * (1.0 / LOW))
                if make:
                    low = (row - high * LOW).astype(jnp.int32)
                    ids = lax.broadcasted_iota(jnp.int32, (LOW, LANES), 0)
                    onehot[c, :, LANES * i:LANES * (i + 1)] = jnp.where(ids == low, 1.0, 0.0).astype(BF16)
                sign = 2.0 * pts[columns + 4, pl.ds(s, 1), :] - 1.0
                v = values(s) * sign
                top = v.astype(BF16)
                rest = (v - top.astype(F32)).astype(BF16)
                wide = jnp.broadcast_to(high, (columns, LANES))
                masks = [jnp.where(wide == float(g), 1.0, 0.0).astype(BF16) for g in range(HIGH)]
                pieces.append(jnp.concatenate([top * g for g in masks] + [rest * g for g in masks], axis=0))
            left = jnp.concatenate(pieces, axis=1)
            target[...] += lax.dot_general(left, onehot[c], (((1,), (1,)), ((), ())), preferred_element_type=F32)

    nbt = kk

    def start(copy):
        copy.start()

    def finish_recv(copy):
        copy.wait_recv()

    def finish_send(copy):
        copy.wait_send()

    for index, (low, bits) in enumerate(stages):
        group = 2 ** bits
        places = LANES // group

        def outward(h, action):
            at = halves * index + h
            return exchange(a_send.at[at], a_recv.at[at], a_ss.at[at], a_rs.at[at], low, bits, action)

        def homeward(h, action):
            at = halves * index + h
            return exchange(b_send.at[at], b_recv.at[at], b_ss.at[at], b_rs.at[at], low, bits, action)

        for h in range(halves):
            at = halves * index + h
            if index == 0:
                gather_half(h)
            pack(a_send.at[at], group, h)
            if index == 0 and h == 0:
                pl.semaphore_wait(barrier, devices - 1)
            mine = outward(h, start)
            a_recv[at, mine] = a_send[at, mine]
        make_maps(low, bits)
        if index == 0:
            for q in range(columns):
                for s in range(LEAF):
                    nbt[s, q:q + 1, :] = pts[q, s:s + 1, :]
            sketch_of(lambda s: nbt[s], skb, True)
        for h in range(halves):
            at = halves * index + h
            outward(h, finish_recv)
            unpack(a_recv.at[at], group, h)
            half = slice(256 * h, 256 * (h + 1))
            for k in range(low, low + bits):
                span = places * 2 ** (k - low)
                full = cbuf[half, :]
                wide = lax.broadcasted_iota(jnp.int32, full.shape, 1)
                part[half, :] = jnp.where((wide // span) % 2 == 0,
                                          pltpu.roll(full, LANES - span, 1), pltpu.roll(full, span, 1))

                def mix(v, acc):
                    own = [mats[2 * k, v, 8 * t:8 * t + 8] for t in range(4)]
                    cross = [mats[2 * k + 1, v, 8 * t:8 * t + 8] for t in range(4)]
                    out = []
                    for q in range(8):
                        row = cbuf[pl.ds((8 * h + q) * 32 + v, 1), :]
                        other = part[pl.ds((8 * h + q) * 32 + v, 1), :]
                        for t in range(4):
                            out.append(acc[4 * q + t] + own[t] * row + cross[t] * other)
                    return tuple(out)

                init = tuple(0.85 * cbuf[pl.ds((8 * h + q) * 32 + 8 * t, 8), :] for q in range(8) for t in range(4))
                acc = lax.fori_loop(0, WIDTH, mix, init, unroll=2)
                for q in range(8):
                    for t in range(4):
                        cbuf[pl.ds((8 * h + q) * 32 + 8 * t, 8), :] = acc[4 * q + t]
            pack(b_send.at[at], group, h)
            mine = homeward(h, start)
            b_recv[at, mine] = b_send[at, mine]
        for h in range(halves):
            outward(h, finish_send)
        for h in range(halves):
            homeward(h, finish_recv)
            unpack(b_recv.at[halves * index + h], group, h)
        for h in range(halves):
            homeward(h, finish_send)

    for c in range(LEAF // 8):
        def spread_out(w, acc):
            coef = [cbuf[pl.ds(8 * h * 32 + w, 8, stride=32), :] for h in range(halves)]
            out = []
            for s in range(8):
                row = leaf[8 * c + s, pl.ds(w, 1), :]
                for h in range(halves):
                    out.append(acc[halves * s + h] + coef[h] * row)
            return tuple(out)

        init = tuple(
            jnp.broadcast_to(pts[columns + 2, 8 * c + s:8 * c + s + 1, :], (8, LANES)) * nbt[8 * c + s, 8 * h:8 * h + 8]
            for s in range(8) for h in range(halves))
        acc = lax.fori_loop(0, WIDTH, spread_out, init, unroll=2)
        for s in range(8):
            for h in range(halves):
                part[(8 * c + s) * columns + 8 * h:(8 * c + s) * columns + 8 * h + 8, :] = acc[halves * s + h]

    inner = jnp.zeros((columns, LANES), F32)
    square, energy = inner, inner
    for s in range(LEAF):
        v, image = nbt[s], part[s * columns:(s + 1) * columns, :]
        inner, square, energy = inner + v * image, square + v * v, energy + image * image
    lane_q = lax.broadcasted_iota(jnp.int32, (columns, LANES), 1)
    row_q = lax.broadcasted_iota(jnp.int32, (columns, LANES), 0)
    packed = jnp.zeros((columns, LANES), F32)
    for i, value in enumerate((inner, square, energy)):
        packed = jnp.where(lane_q == row_q + columns * i, jnp.sum(value, axis=1, keepdims=True), packed)
    sum_send[...] = jnp.sum(packed, axis=0, keepdims=True)

    def to_all(source, recv, ss, rs, action):
        @pl.loop(1, devices)
        def _(i):
            other = lax.rem(me + i, devices)
            here = other if action is finish_recv else me
            action(pltpu.make_async_remote_copy(
                source(other), recv.at[here], ss.at[other], rs.at[here],
                device_id=(other,), device_id_type=MESH))

    to_all(lambda d: sum_send, sum_recv, s_ss, s_rs, start)
    sum_recv[me] = sum_send[...]
    sketch_of(lambda s: part[pl.ds(pl.multiple_of(s * columns, columns), columns), :], ski, False)
    to_all(lambda d: sum_send, sum_recv, s_ss, s_rs, finish_recv)
    totals = jnp.sum(sum_recv[...], axis=0)

    def column(i):
        picked = jnp.where(lane_q == row_q + columns * i, jnp.broadcast_to(totals, (columns, LANES)), 0.0)
        return jnp.broadcast_to(jnp.sum(picked, axis=1, keepdims=True) * (1.0 / total_points), (columns, LANES))

    inner_mean, square_mean, energy_mean = column(0), column(1), column(2)
    projection = inner_mean / (square_mean + EPSILON)
    energy = energy_mean - 2.0 * projection * inner_mean + projection * projection * square_mean
    spread = jnp.sqrt(energy + EPSILON)
    inverse = 1.0 / spread
    for i, value in enumerate((projection, spread)):
        arn_ref[i:i + 1, :] = jnp.sum(jnp.where(lane_q == row_q, value, 0.0), axis=0, keepdims=True)[:, :columns]

    rows_each = rs_send.shape[1]
    factor = math.sqrt(SKETCH / total_points)
    lowest = HIGH * columns
    part_tiles = LOW // LANES
    for n in range(devices):
        flat = n * rows_each
        tile, row = flat // 8, flat % 8
        strip, side = tile // part_tiles, tile % part_tiles
        top = strip * 8 + row
        q0 = top % columns
        cols = slice(side * LANES, (side + 1) * LANES)
        img = ski[top:top + rows_each, cols] + ski[lowest + top:lowest + top + rows_each, cols]
        bas = skb[top:top + rows_each, cols] + skb[lowest + top:lowest + top + rows_each, cols]
        rs_send[n] = (img - projection[q0:q0 + rows_each] * bas) * (factor * inverse[q0:q0 + rows_each])
    to_all(lambda d: rs_send.at[d], rs_recv, r_ss, r_rs, start)
    rs_recv[me] = rs_send[me]

    for s in range(LEAF):
        pts_rows = (part[s * columns:(s + 1) * columns, :] - projection * nbt[s]) * inverse
        nbt[s] = pts_rows
    for q in range(columns):
        for s in range(LEAF):
            pts[q, s:s + 1, :] = nbt[s, q:q + 1, :]
    for i in range(columns // 4):
        for j in range(4):
            for g in range(4):
                tbuf[0, 32 * g:32 * g + 32, 32 * j:32 * j + 32] = pts[4 * i + j, :, 32 * g:32 * g + 32]
        raw[LANES * i:LANES * (i + 1), :] = tbuf[0].T
    for r in range(LANES // 4):
        for h in range(halves):
            nb_ref[8 * h:8 * h + 8, LANES * r:LANES * (r + 1)] = raw[pl.ds(256 * h + r, 8, stride=32), :]

    to_all(lambda d: rs_send.at[d], rs_recv, r_ss, r_rs, finish_recv)
    own_chunk[...] = jnp.sum(rs_recv[...], axis=0)
    to_all(lambda d: own_chunk, ag_recv, g_ss, g_rs, start)
    ag_recv[me] = own_chunk[...]
    to_all(lambda d: sum_send, sum_recv, s_ss, s_rs, finish_send)
    to_all(lambda d: rs_send.at[d], rs_recv, r_ss, r_rs, finish_send)
    to_all(lambda d: own_chunk, ag_recv, g_ss, g_rs, finish_recv)
    for n in range(devices):
        flat = n * rows_each
        tile, row = flat // 8, flat % 8
        strip, side = tile // part_tiles, tile % part_tiles
        top = strip * 8 + row
        q0, high = top % columns, top // columns
        begin = high * LOW + side * LANES
        sketch_ref[q0:q0 + rows_each, begin:begin + LANES] = ag_recv[n]
    to_all(lambda d: own_chunk, ag_recv, g_ss, g_rs, finish_send)


def split(x):
    top = x.astype(BF16)
    return top, (x - top.astype(F32)).astype(BF16)


def tile_kernel(devices, total_points, scale_ref, v_in, coords_in, diag_in, rows_in, signs_in,
                nb_ref, sketch_ref, arn_ref, v_ref, coords_ref, diag_ref, rows_ref, signs_ref,
                small_send, small, vals, phases, steps, mats, leaf, state, coef,
                image, back, hot, left, masks, sum_send, sum_recv, sum_total, sum_joined, rb_send,
                rb_recv, rb_total, rb_joined, ri_send, ri_recv, ri_total, ri_joined, ag_recv, own_chunk, sems,
                io_sems):
    me = lax.axis_index("box")
    columns = nb_ref.shape[0]
    sections = devices.bit_length() - 1
    per_tile = LANES // LEAF
    half = LANES // 2
    barrier = pltpu.get_barrier_semaphore()

    @pl.loop(1, devices)
    def _(i):
        pl.semaphore_signal(barrier, inc=1, device_id=(lax.rem(me + i, devices),), device_id_type=MESH)

    incoming = [pltpu.make_async_copy(a, b, io_sems.at[i]) for i, (a, b) in enumerate((
        (v_in, v_ref), (coords_in, coords_ref), (diag_in, diag_ref), (rows_in, rows_ref), (signs_in, signs_ref)))]
    for copy in incoming:
        copy.start()
    lane = lax.broadcasted_iota(jnp.int32, (8, LANES), 1)
    sub = lax.broadcasted_iota(jnp.int32, (8, LANES), 0)
    planes = 4
    plane_size = devices // planes
    plane, seat = me // plane_size, lax.rem(me, plane_size)
    halves = devices // 2
    side = plane // 2

    def facing(away):
        there = 0
        for b in range(planes.bit_length() - 1):
            bit = lax.rem(plane // 2 ** b, 2)
            there = there + 2 ** b * ((1 - bit) if (away >> b) & 1 else bit)
        return there

    def send(source, target, which, other):
        pltpu.make_async_remote_copy(
            source, target, sems.at[2 * which], sems.at[2 * which + 1],
            device_id=(other,), device_id_type=MESH).start()

    def to_all(source, target, which, aways):
        for away in aways:
            there = {3: (1 - side) * (planes - 1), 2: 2 - side, 1: facing(1), 0: plane}[away]

            @pl.loop(0 if away else 1, plane_size)
            def _(i):
                other = plane_size * there + lax.rem(seat + i, plane_size)
                send(source(other), target, which, other)

    def to_plane(source, target, which):
        @pl.loop(1, plane_size)
        def _(i):
            other = lax.rem(seat + i, plane_size)
            send(source(other), target, which, plane_size * plane + other)

    def to_planes(source, target, which):
        for away in range(planes - 1, 0, -1):
            send(source, target, which, plane_size * facing(away) + seat)

    def finish(ref, which, end):
        pltpu.make_async_copy(ref, ref, sems.at[2 * which + end]).wait()

    def columns_at(ref, tile):
        return ref.at[:, pl.ds(pl.multiple_of(tile * LANES, LANES), LANES)]

    others, mates, peers = pl.ds(0, devices - 1), pl.ds(0, plane_size - 1), pl.ds(0, planes - 1)
    side_rows = 5
    side_part = pl.ds(0, side_rows)

    for copy in incoming:
        copy.wait()
    rows_f, signs_f = rows_ref[...].astype(F32), signs_ref[...].astype(F32)
    for e in range(devices):
        here = slice(e * LANES, (e + 1) * LANES)
        small_send[e, 0:2, :] = coords_ref[:, here].astype(F32)
        small_send[e, 2:3, :] = diag_ref[e:e + 1, :]
        small_send[e, 3:4, :] = rows_f[e:e + 1, :]
        small_send[e, 4:5, :] = signs_f[e:e + 1, :]
    scale = lax.rem(scale_ref[0], MODULUS)
    spot = lane // LEAF
    inner_lane = (lane % LEAF).astype(F32)
    for k in range(sections):
        for g in range(devices // 8):
            ident = ((8 * g + sub) * LANES + per_tile * me + spot) * 37
            x = (ident + 101 * k).astype(F32)
            rest = x - jnp.floor(x * (1.0 / (MODULUS - 1))) * float(MODULUS - 1)
            rest = jnp.where(rest < 0.0, rest + float(MODULUS - 1), rest)
            rest = jnp.where(rest >= float(MODULUS - 1), rest - float(MODULUS - 1), rest)
            key = rest.astype(jnp.int32) + 1
            unit_phase = fold(fold(key * scale)).astype(F32)
            for m, second in enumerate((2.0, 1.0)):
                phi = remainder(unit_phase * (inner_lane + second))
                phases[2 * k + m, 8 * g:8 * g + 8, :] = phi
                steps[2 * k + m, 8 * g:8 * g + 8, :] = scaled_cos(8.0 * phi, 2.0)

    wide_sub = lax.broadcasted_iota(jnp.int32, (WIDTH, LANES), 0)
    wide_lane = lax.broadcasted_iota(jnp.int32, (WIDTH, LANES), 1)
    ident_part = jnp.where(wide_lane % WIDTH == wide_sub, 0.85, 0.0)
    sub_f = sub.astype(F32)
    def make_maps(begins, ends):
        for k in range(sections):
            maps_of(k, begins[k], ends[k])

    def maps_of(k, begin_pair, end_pair):
        stride = 2 ** k

        @pl.loop(begin_pair, end_pair)
        def _(pair):
            first_tile = (pair // stride) * (2 * stride) + pair % stride
            for bit in range(2):
                d = first_tile + stride * bit
                for m in range(2):
                    amplitude = (0.35 if m == 0 else 0.6) / math.sqrt(WIDTH)
                    first, offset = (1.0, 0.0) if m == 0 else (3.0, 4096.0)
                    phi = phases[2 * k + m, pl.ds(d, 1), :]
                    step = steps[2 * k + m, pl.ds(d, 1), :]
                    one = scaled_cos(phi * (sub_f + (8.0 + first)) + offset, amplitude)
                    two = scaled_cos(phi * (sub_f + (16.0 + first)) + offset, amplitude)
                    full = jnp.concatenate([step * one - two, one, two, step * two - one], axis=0)
                    if m == 0:
                        full = full + ident_part
                    top, low = split(full)
                    begin = LANES * (bit if m == 0 else 1 - bit)
                    mats[k, pair, 64 * bit:64 * bit + 32, begin:begin + LANES] = top
                    mats[k, pair, 64 * bit + 32:64 * bit + 64, begin:begin + LANES] = low

    hops = lax.rem(me // 2, 2) + lax.rem(me // 4, 2) + plane
    budget = 18 * (5 - hops) - 8
    early = [jnp.clip(budget - k * (devices // 2), 0, devices // 2) for k in range(sections)]
    make_maps([0] * sections, early)
    pl.semaphore_wait(barrier, devices - 1)
    for which, aways in ((0, (3, 2)), (7, (1, 0))):
        to_all(lambda d: small_send.at[d, side_part], small.at[me, side_part], which, aways)
    for which, aways in ((8, (1, 0)), (1, (3, 2))):
        to_all(lambda d: columns_at(v_ref, d), vals.at[me], which, aways)
    small[me] = small_send[me]
    vals[me] = columns_at(v_ref, me)[...]

    make_maps(early, [devices // 2] * sections)
    lanes_q = lax.broadcasted_iota(jnp.int32, (columns, LANES), 1)
    rows_q = lax.broadcasted_iota(jnp.int32, (columns, LANES), 0)

    def place(tile):
        return pl.ds(pl.multiple_of(tile * LANES, LANES), LANES)

    low_ids = lax.broadcasted_iota(jnp.int32, (LOW, LANES), 0).astype(F32).astype(BF16)
    high_ids = (lax.broadcasted_iota(jnp.int32, (HIGH * columns, LANES), 0) // columns).astype(F32).astype(BF16)
    one, nil = jnp.array(1.0, BF16), jnp.array(0.0, BF16)

    def make_hot(row_of, sign_of, begin, count):
        @pl.loop(0, count, unroll=2)
        def _(i):
            d = begin + i
            row = row_of(d)
            high = jnp.floor(row * (1.0 / LOW))
            low = jnp.broadcast_to((row - high * LOW).astype(BF16), (LOW, LANES))
            hot[:, place(d)] = jnp.where(low_ids == low, one, nil)
            sign = jnp.broadcast_to((2.0 * sign_of(d) - 1.0).astype(BF16), (HIGH * columns, LANES))
            wide = jnp.broadcast_to(high.astype(BF16), (HIGH * columns, LANES))
            masks[d] = jnp.where(high_ids == wide, sign, nil)

    def place_values(d, at, value):
        top, rest = split(value)
        for g in range(HIGH):
            mask = masks[d, columns * g:columns * (g + 1), :]
            left[columns * g:columns * (g + 1), at] = top * mask
            left[columns * (HIGH + g):columns * (HIGH + g + 1), at] = rest * mask

    def sketch_product():
        o = lax.dot_general(left[...], hot[...], (((1,), (1,)), ((), ())), preferred_element_type=F32)
        return o[:HIGH * columns] + o[HIGH * columns:]

    factor = math.sqrt(SKETCH / total_points)

    def start_reduce(sk, pieces, landed, which):
        for n in range(plane_size):
            pieces[n] = sk[columns * n:columns * (n + 1), :]
        to_plane(lambda n: pieces.at[n], landed.at[seat], which)
        landed[seat] = pieces[seat]

    def next_reduce(landed, total, joined, which, first):
        finish(landed.at[pl.ds(0, plane_size - 1)], first, 1)
        total[...] = jnp.sum(landed[...], axis=0)
        to_planes(total, joined.at[plane], which)
        joined[plane] = total[...]

    make_hot(lambda d: rows_ref[pl.ds(d, 1), :].astype(F32), lambda d: signs_ref[pl.ds(d, 1), :].astype(F32), 0, devices)

    @pl.loop(0, devices)
    def _(d):
        place_values(d, place(d), v_ref[:, place(d)])

    basis_sketch = sketch_product()
    start_reduce(basis_sketch, rb_send, rb_recv, 2)

    fx = (sub % 4 + 1).astype(F32)
    fy = (sub // 4 + 1).astype(F32)
    unit = 1.0 / math.sqrt(LEAF)
    point_masks = [jnp.where(lanes_q // LEAF == j, 1.0, 0.0).astype(BF16) for j in range(per_tile)]
    column_masks = [jnp.where((wide_lane % half) // columns == j, 1.0, 0.0).astype(BF16) for j in range(per_tile)]
    first_half = wide_lane < half

    def combine(o):
        s = o[0:32] + o[32:64]
        return s + pltpu.roll(s, half, 1)

    def expand(total):
        top = total.astype(BF16).astype(F32)
        y = jnp.where(first_half, top, total - top).astype(BF16)
        return jnp.concatenate([y * m for m in column_masks], axis=0)

    def leaves(begin):
        @pl.loop(0, halves, unroll=4)
        def _(i):
            d = begin + i
            pair = fold(small[d, 0:2, :].astype(jnp.int32) * scale).astype(F32)
            px, py = pair[0:1], pair[1:2]
            phases_of = [fx * px + (fy + 2.0 * t) * py for t in range(2)]
            full = jnp.concatenate([scaled_cos(n, unit) for n in phases_of] + [scaled_sin(n, unit) for n in phases_of], axis=0)
            top, low = split(full)
            leaf[d, 0:32] = top
            leaf[d, 32:64] = low

    def gather(begin):
        for i in range(halves):
            d = begin + i
            top, rest = split(vals[d])
            spread_v = jnp.concatenate([top * m for m in point_masks] + [rest * m for m in point_masks], axis=0)
            o = lax.dot_general(leaf[d], spread_v, (((1,), (1,)), ((), ())), preferred_element_type=F32)
            state[0, d] = expand(combine(o))

    def section(k, begin, count):
        stride = 2 ** k
        now = k % 2
        for i in range(count // 2):
            d0 = begin + (i // stride) * (2 * stride) + i % stride
            d1 = d0 + stride
            x = jnp.concatenate([state[now, d0], state[now, d1]], axis=0)
            o = jnp.dot(mats[k, begin // 2 + i], x, preferred_element_type=F32)
            for d, part in ((d0, o[0:64]), (d1, o[64:128])):
                total = combine(part)
                if k == sections - 1:
                    coef[32 * d:32 * d + 32, :] = total
                else:
                    state[1 - now, d] = expand(total)

    near, away = side * halves, (1 - side) * halves
    for begin, small_which, count in ((near, 7, halves - 1), (away, 0, halves)):
        finish(small.at[pl.ds(0, count), side_part], small_which, 1)
        leaves(begin)
        make_hot(lambda d: small[d, 3:4, :], lambda d: small[d, 4:5, :], begin, halves)
    for begin, vals_which, count in ((near, 8, halves - 1), (away, 1, halves)):
        arrived = pl.ds(0, count)
        finish(vals.at[arrived], vals_which, 1)
        gather(begin)
        for k in range(sections - 1):
            section(k, begin, halves)
    next_reduce(rb_recv, rb_total, rb_joined, 9, 2)
    section(sections - 1, 0, devices)
    tile_lane = lax.broadcasted_iota(jnp.int32, (half, 2 * LANES), 1)
    tile_masks = [jnp.where((tile_lane % LANES) // WIDTH == t, 1.0, 0.0).astype(BF16) for t in range(4)]
    zero = jnp.zeros((columns, LANES), F32)
    inner, square, energy = zero, zero, zero
    for g in range(devices // 4):
        flipped = coef[LANES * g:LANES * (g + 1), :].T
        top, rest = split(flipped[0:half])
        both = jnp.concatenate([top, rest], axis=1)
        lhs = jnp.concatenate([both * m for m in tile_masks], axis=0)
        tops = jnp.concatenate([leaf[4 * g + t, 0:32] for t in range(4)], axis=0)
        lows = jnp.concatenate([leaf[4 * g + t, 32:64] for t in range(4)], axis=0)
        right = jnp.concatenate([tops, lows], axis=1)
        o = jnp.dot(lhs, jnp.concatenate([right, right], axis=0), preferred_element_type=F32)
        o = o[:, 0:LANES] + o[:, LANES:2 * LANES]
        for t in range(4):
            d = 4 * g + t
            v = vals[d]
            img = jnp.broadcast_to(small[d, 2:3, :], (columns, LANES)) * v
            for j in range(per_tile):
                begin = half * t + columns * j
                img = img + jnp.where(lanes_q // LEAF == j, o[begin:begin + columns], 0.0)
            image[d] = img
            place_values(d, slice(LANES * d, LANES * (d + 1)), img)
            inner, square, energy = inner + v * img, square + v * v, energy + img * img

    to_all(lambda d: image.at[d], back.at[me], 5, (3, 2))
    packed = zero
    for i, value in enumerate((inner, square, energy)):
        packed = jnp.where(lanes_q == rows_q + columns * i, jnp.sum(value, axis=1, keepdims=True), packed)
    sum_send[...] = jnp.sum(packed, axis=0, keepdims=True)
    image_sketch = sketch_product()
    start_reduce(image_sketch, ri_send, ri_recv, 4)
    to_plane(lambda d: sum_send, sum_recv.at[seat], 3)
    to_all(lambda d: image.at[d], back.at[me], 5, (1, 0))
    sum_recv[seat] = sum_send[...]
    back[me] = image[me]

    finish(small_send.at[pl.ds(0, halves), side_part], 0, 0)
    finish(small_send.at[pl.ds(0, halves - 1), side_part], 7, 0)
    finish(vals.at[pl.ds(0, halves)], 1, 0)
    finish(vals.at[pl.ds(0, halves - 1)], 8, 0)
    finish(rb_send.at[mates], 2, 0)
    next_reduce(ri_recv, ri_total, ri_joined, 11, 4)
    finish(sum_recv.at[mates], 3, 1)
    sum_total[...] = jnp.sum(sum_recv[...], axis=0)
    to_planes(sum_total, sum_joined.at[plane], 10)
    sum_joined[plane] = sum_total[...]
    finish(rb_joined.at[peers], 9, 0)
    finish(rb_joined.at[peers], 9, 1)
    finish(sum_recv.at[mates], 3, 0)
    finish(ri_send.at[mates], 4, 0)
    basis_total = jnp.sum(rb_joined[...], axis=0)
    finish(sum_joined.at[peers], 10, 1)
    totals = jnp.sum(sum_joined[...], axis=0)

    def column(i):
        picked = jnp.where(lanes_q == rows_q + columns * i, jnp.broadcast_to(totals, (columns, LANES)), 0.0)
        return jnp.broadcast_to(jnp.sum(picked, axis=1, keepdims=True) * (1.0 / total_points), (columns, LANES))

    inner_mean, square_mean, energy_mean = column(0), column(1), column(2)
    projection = inner_mean / (square_mean + EPSILON)
    energy = energy_mean - 2.0 * projection * inner_mean + projection * projection * square_mean
    spread = jnp.sqrt(energy + EPSILON)
    inverse = 1.0 / spread
    for i, value in enumerate((projection, spread)):
        arn_ref[i:i + 1, :] = jnp.sum(jnp.where(lanes_q == rows_q, value, 0.0), axis=0, keepdims=True)[:, :columns]
    finish(ri_joined.at[peers], 11, 1)
    wide = lambda x: jnp.concatenate([x] * (LOW // LANES), axis=1)
    own_chunk[...] = (jnp.sum(ri_joined[...], axis=0) - basis_total * wide(projection)) * wide(factor * inverse)
    to_plane(lambda d: own_chunk, ag_recv.at[seat], 6)
    ag_recv[seat] = own_chunk[...]
    finish(back.at[others], 5, 1)
    for e in range(devices):
        here = slice(e * LANES, (e + 1) * LANES)
        nb_ref[:, here] = (back[e] - projection * v_ref[:, here]) * inverse
    finish(image.at[others], 5, 0)
    finish(ri_joined.at[peers], 11, 0)
    finish(sum_joined.at[peers], 10, 0)
    finish(ag_recv.at[mates], 6, 0)
    finish(ag_recv.at[mates], 6, 1)
    for n in range(plane_size):
        sketch_ref[:, LOW * n:LOW * (n + 1)] = ag_recv[n]


def deliver(*refs):
    copies = [pltpu.make_async_copy(refs[i], refs[3 + i], refs[6].at[i]) for i in range(3)]
    for copy in copies:
        copy.start()
    for copy in copies:
        copy.wait()


def together(devices, basis_vector, diagonal, coords, phase_scale, sketch_rows, sketch_signs):
    columns, local_points = basis_vector.shape
    sections = devices.bit_length() - 1
    plane = (local_points // LANES, LANES)
    far = pl.BlockSpec(memory_space=pltpu.HBM)
    vmem = pl.BlockSpec(memory_space=pltpu.VMEM)
    tile = pltpu.VMEM((devices, columns, LANES), F32)
    chunk = (columns, LOW)
    pieces = pltpu.VMEM((HIGH,) + chunk, F32)
    reduce_parts = [pieces, pieces, pltpu.VMEM(chunk, F32), pltpu.VMEM((devices // HIGH,) + chunk, F32)]
    results = pl.pallas_call(
        functools.partial(tile_kernel, devices, local_points * devices),
        out_shape=(
            jax.ShapeDtypeStruct((columns, local_points), F32),
            jax.ShapeDtypeStruct((columns, SKETCH), F32),
            jax.ShapeDtypeStruct((2, columns), F32)),
        in_specs=[pl.BlockSpec(memory_space=pltpu.SMEM)] + [far] * 5,
        out_specs=(vmem,) * 3,
        scratch_shapes=[
            pltpu.VMEM(basis_vector.shape, F32),
            pltpu.VMEM(coords.shape, jnp.int32),
            pltpu.VMEM(plane, F32),
            pltpu.VMEM(plane, jnp.int32),
            pltpu.VMEM(plane, jnp.int32),
            pltpu.VMEM((devices, 8, LANES), F32),
            pltpu.VMEM((devices, 8, LANES), F32),
            tile,
            pltpu.VMEM((2 * sections, devices, LANES), F32),
            pltpu.VMEM((2 * sections, devices, LANES), F32),
            pltpu.VMEM((sections, devices // 2, 4 * WIDTH, 2 * LANES), BF16),
            pltpu.VMEM((devices, 2 * WIDTH, LANES), BF16),
            pltpu.VMEM((2, devices, LANES, LANES), BF16),
            pltpu.VMEM((devices * WIDTH, LANES), F32),
            tile, tile,
            pltpu.VMEM((LOW, local_points), BF16),
            pltpu.VMEM((2 * HIGH * columns, local_points), BF16),
            pltpu.VMEM((devices, HIGH * columns, LANES), BF16),
            pltpu.VMEM((1, LANES), F32),
            pltpu.VMEM((HIGH, 1, LANES), F32),
            pltpu.VMEM((1, LANES), F32),
            pltpu.VMEM((devices // HIGH, 1, LANES), F32),
            *reduce_parts, *reduce_parts, pieces,
            pltpu.VMEM(chunk, F32),
            pltpu.SemaphoreType.DMA((24,)),
            pltpu.SemaphoreType.DMA((5,)),
        ],
        compiler_params=pltpu.CompilerParams(
            collective_id=0, has_side_effects=True, vmem_limit_bytes=24 * 2**20),
        name="gmres",
    )(phase_scale, *(pltpu.with_memory_space_constraint(x, pltpu.HBM) for x in (
        basis_vector, coords, diagonal.reshape(plane), sketch_rows.reshape(plane),
        sketch_signs.reshape(plane))))
    return pl.pallas_call(
        deliver,
        out_shape=[jax.ShapeDtypeStruct(x.shape, x.dtype) for x in results],
        in_specs=[vmem] * 3,
        out_specs=[far] * 3,
        scratch_shapes=[pltpu.SemaphoreType.DMA((3,))],
        compiler_params=pltpu.CompilerParams(vmem_limit_bytes=2**20),
        name="deliver",
    )(*results)


def body(basis_vector, diagonal, coords, phase_scale, sketch_rows, sketch_signs):
    columns, local_points = basis_vector.shape
    devices = lax.axis_size("box")
    if devices * LANES == local_points:
        return together(devices, basis_vector, diagonal, coords, phase_scale, sketch_rows, sketch_signs)
    sections = devices.bit_length() - 1
    count = -(-sections // 5)
    stages, low = [], 0
    for i in range(count):
        bits = (sections - low) // (count - i)
        stages.append((low, bits))
        low += bits
    group = 2 ** max(bits for _, bits in stages)
    group_rows = [columns * WIDTH // LANES * (LANES // 2 ** bits) for _, bits in stages]
    plane = (local_points // LANES, LANES)
    rows_each = HIGH * columns * LOW // LANES // devices
    vmem = pl.BlockSpec(memory_space=pltpu.VMEM)
    dma = pltpu.SemaphoreType.DMA
    count_rows = max(group_rows)
    halves = columns // 8
    new_basis, sketch, arn = pl.pallas_call(
        functools.partial(kernel, devices, stages, local_points * devices),
        out_shape=(
            jax.ShapeDtypeStruct((columns, local_points), F32),
            jax.ShapeDtypeStruct((columns, SKETCH), F32),
            jax.ShapeDtypeStruct((2, columns), F32)),
        in_specs=[pl.BlockSpec(memory_space=pltpu.SMEM), vmem, vmem, vmem, vmem, vmem],
        out_specs=(vmem, vmem, vmem),
        scratch_shapes=[
            pltpu.VMEM(((columns + 8) * LEAF, LANES), F32),
            pltpu.VMEM((columns + 8, LEAF, LANES), F32),
            pltpu.VMEM((LEAF, WIDTH, LANES), F32),
            pltpu.VMEM((2 * sections, WIDTH, WIDTH, LANES), F32),
            pltpu.VMEM((LEAF, columns, LANES), F32),
            pltpu.VMEM((columns * WIDTH, LANES), F32),
            pltpu.VMEM((columns * WIDTH, LANES), F32),
            pltpu.VMEM((columns * WIDTH // LANES, LANES, LANES), F32),
            pltpu.VMEM((2, LEAF, LANES), F32),
            pltpu.VMEM((LEAF // 4, LOW, 4 * LANES), BF16),
            pltpu.VMEM((2 * HIGH * columns, LOW), F32),
            pltpu.VMEM((2 * HIGH * columns, LOW), F32),
            pltpu.VMEM((count * halves, group, count_rows // halves, LANES), F32),
            pltpu.VMEM((count * halves, group, count_rows // halves, LANES), F32),
            pltpu.VMEM((count * halves, group, count_rows // halves, LANES), F32),
            pltpu.VMEM((count * halves, group, count_rows // halves, LANES), F32),
            pltpu.VMEM((1, LANES), F32),
            pltpu.VMEM((devices, 1, LANES), F32),
            pltpu.VMEM((devices, rows_each, LANES), F32),
            pltpu.VMEM((devices, rows_each, LANES), F32),
            pltpu.VMEM((devices, rows_each, LANES), F32),
            pltpu.VMEM((rows_each, LANES), F32),
            dma((count * halves, group)), dma((count * halves, group)), dma((count * halves, group)), dma((count * halves, group)),
            dma((devices,)), dma((devices,)), dma((devices,)), dma((devices,)), dma((devices,)), dma((devices,)),
        ],
        compiler_params=pltpu.CompilerParams(
            collective_id=0, has_side_effects=True, vmem_limit_bytes=60 * 2**20),
        name="gmres",
    )(phase_scale, basis_vector, coords, diagonal.reshape(plane), sketch_rows.reshape(plane),
      sketch_signs.reshape(plane))
    return new_basis, sketch, arn


def solution(mesh):
    placed = (P(None, "box"), P("box"), P(None, "box"), P(), P("box"), P("box"))
    return jax.shard_map(
        body, mesh=mesh, in_specs=placed, out_specs=(P(None, "box"), P(), P()), check_vma=False
    )
```

```python
import functools
import math

import jax
import jax.numpy as jnp
import numpy as np
from jax import lax
from jax.experimental import pallas as pl
from jax.experimental.pallas import tpu as pltpu
from jax.sharding import PartitionSpec as P

WIDTH = 32
LEAF = 32
SKETCH = 2048
LANES = 128
HIGH = 8
LOW = SKETCH // HIGH
MODULUS = 8191
EPSILON = 1e-06
MESH = pl.DeviceIdType.MESH
F32 = jnp.float32
BF16 = jnp.bfloat16


def sine_series():
    node = np.cos((np.arange(400) + 0.5) * np.pi / 800)
    basis = np.stack([node ** (2 * i) for i in range(6)], 1)
    exact = np.sin(np.pi * node * 4096 / MODULUS) / node
    return np.linalg.lstsq(basis, exact, rcond=None)[0]


SERIES = sine_series()


def remainder(n):
    return n - jnp.floor(n * (1.0 / MODULUS) + 0.5) * float(MODULUS)


def half_sine(n, gain):
    t = remainder(n) * (1.0 / 4096)
    z = t * t
    total = z * float(SERIES[5] * gain) + float(SERIES[4] * gain)
    for c in SERIES[3::-1]:
        total = total * z + float(c * gain)
    return total * t


def scaled_cos(n, amplitude):
    s = half_sine(n, math.sqrt(2.0 * amplitude))
    return amplitude - s * s


def scaled_sin(n, amplitude):
    return scaled_cos(n - 0.25 * MODULUS, amplitude)


def fold(p):
    return (p & MODULUS) + lax.shift_right_logical(p, 13)


def kernel(devices, stages, total_points, scale_ref, v_ref, coords_ref, diag_ref, rows_ref, signs_ref,
           nb_ref, sketch_ref, arn_ref, raw, pts, leaf, mats, kk, cbuf, part, tbuf, work, onehot, skb, ski,
           a_send, a_recv, b_send, b_recv, sum_send, sum_recv, rs_send, rs_recv, ag_recv, own_chunk,
           a_ss, a_rs, b_ss, b_rs, s_ss, s_rs, r_ss, r_rs, g_ss, g_rs):
    me = lax.axis_index("box")
    columns = nb_ref.shape[0]
    halves = columns // 8
    barrier = pltpu.get_barrier_semaphore()

    @pl.loop(1, devices)
    def _(i):
        pl.semaphore_signal(barrier, inc=1, device_id=(lax.rem(me + i, devices),), device_id_type=MESH)

    lane = lax.broadcasted_iota(jnp.int32, (8, LANES), 1)
    sub = lax.broadcasted_iota(jnp.int32, (8, LANES), 0)
    scale = lax.rem(scale_ref[0], MODULUS)

    for r in range(LANES // 4):
        here = slice(LANES * r, LANES * (r + 1))
        for h in range(halves):
            raw[pl.ds(256 * h + r, 8, stride=32), :] = v_ref[8 * h:8 * h + 8, here]
        pair = coords_ref[:, here].astype(F32)
        raw[columns * 32 + r:columns * 32 + r + 1, :] = pair[0:1]
        raw[columns * 32 + 32 + r:columns * 32 + 33 + r, :] = pair[1:2]
    raw[(columns + 2) * 32:(columns + 3) * 32, :] = diag_ref[...]
    raw[(columns + 3) * 32:(columns + 4) * 32, :] = rows_ref[...].astype(F32)
    raw[(columns + 4) * 32:(columns + 5) * 32, :] = signs_ref[...].astype(F32)
    raw[(columns + 5) * 32:(columns + 8) * 32, :] = jnp.zeros((96, LANES), F32)
    for i in range((columns + 8) // 4):
        flipped = raw[LANES * i:LANES * (i + 1), :].T
        tbuf[0] = flipped
        for j in range(4):
            pts[4 * i + j] = jnp.concatenate(
                [tbuf[0, 32 * g:32 * g + 32, 32 * j:32 * j + 32] for g in range(4)], axis=1)

    def exact_phase(row):
        return fold(pts[columns + row].astype(jnp.int32) * scale).astype(F32)

    work[0] = exact_phase(0)
    work[1] = exact_phase(1)
    fx = (sub % 4 + 1).astype(F32)
    fy = (sub // 4 + 1).astype(F32)
    unit = 1.0 / math.sqrt(LEAF)

    @pl.loop(0, LEAF)
    def _(s):
        px = work[0, pl.ds(s, 1), :]
        py = work[1, pl.ds(s, 1), :]
        for tile in range(2):
            n = fx * px + (fy + 2.0 * tile) * py
            leaf[s, 8 * tile:8 * tile + 8] = scaled_cos(n, unit)
            leaf[s, 16 + 8 * tile:24 + 8 * tile] = scaled_sin(n, unit)

    def gather_half(h):
        def gather(s, acc):
            tiles = [leaf[s, 8 * t:8 * t + 8] for t in range(4)]
            out = []
            for q in range(8):
                row = pts[8 * h + q, pl.ds(s, 1), :]
                for t in range(4):
                    out.append(acc[4 * q + t] + tiles[t] * row)
            return tuple(out)

        acc = lax.fori_loop(0, LEAF, gather, tuple(jnp.zeros((8, LANES), F32) for _ in range(32)), unroll=2)
        for q in range(8):
            for t in range(4):
                cbuf[pl.ds((8 * h + q) * 32 + 8 * t, 8), :] = acc[4 * q + t]

    blocks = 8 * WIDTH // LANES

    def make_maps(low, bits):
        group = 2 ** bits
        places = LANES // group
        mine = lax.rem(me // 2 ** low, group)
        spot = mine * places + lane % places
        box = 4 * (spot % 32) + spot // 32
        member = me + (lane // places - mine) * 2 ** low
        ident = (member * LANES + box) * 37

        @pl.loop(low, low + bits)
        def _(k):
            x = (ident + 101 * k).astype(F32)
            rest = x - jnp.floor(x * (1.0 / (MODULUS - 1))) * float(MODULUS - 1)
            rest = jnp.where(rest < 0.0, rest + float(MODULUS - 1), rest)
            rest = jnp.where(rest >= float(MODULUS - 1), rest - float(MODULUS - 1), rest)
            key = rest.astype(jnp.int32) + 1
            unit_phase = fold(fold(key * scale)).astype(F32)
            wide = sub.astype(F32)
            for m in range(2):
                amplitude = (0.35 if m == 0 else 0.6) / math.sqrt(WIDTH)
                first, second, offset = (1.0, 2.0, 0.0) if m == 0 else (3.0, 1.0, 4096.0)
                mid = unit_phase * (wide + (8.0 + first))
                far = unit_phase * (wide + (16.0 + first))

                @pl.loop(0, WIDTH, unroll=2)
                def _(v):
                    times = v.astype(F32) + second
                    step = scaled_cos(unit_phase * (8.0 * times), 2.0)
                    one = scaled_cos(mid * times + offset, amplitude)
                    two = scaled_cos(far * times + offset, amplitude)
                    mats[2 * k + m, v, 8:16] = one
                    mats[2 * k + m, v, 16:24] = two
                    mats[2 * k + m, v, 0:8] = step * one - two
                    mats[2 * k + m, v, 24:32] = step * two - one

    def exchange(send, recv, ss, rs, low, bits, action):
        group = 2 ** bits
        mine = lax.rem(me // 2 ** low, group)

        @pl.loop(1, group)
        def _(i):
            other = lax.rem(mine + i, group)
            here = other if action is finish_recv else mine
            copy = pltpu.make_async_remote_copy(
                send.at[other], recv.at[here], ss.at[other], rs.at[here],
                device_id=(me + (other - mine) * 2 ** low,), device_id_type=MESH)
            action(copy)
        return mine

    def pack(send, group, h):
        places = LANES // group
        for j in range(blocks):
            at = LANES * (blocks * h + j)
            tbuf[j] = cbuf[at:at + LANES, :].T
        for d in range(group):
            for j in range(blocks):
                send[d, places * j:places * (j + 1), :] = tbuf[j, places * d:places * (d + 1), :]

    def unpack(recv, group, h):
        places = LANES // group
        for j in range(blocks):
            for d in range(group):
                tbuf[j, places * d:places * (d + 1), :] = recv[d, places * j:places * (j + 1), :]
        for j in range(blocks):
            at = LANES * (blocks * h + j)
            cbuf[at:at + LANES, :] = tbuf[j].T

    def sketch_of(values, target, make):
        target[...] = jnp.zeros_like(target)

        @pl.loop(0, LEAF // 4)
        def _(c):
            pieces = []
            for i in range(4):
                s = 4 * c + i
                row = pts[columns + 3, pl.ds(s, 1), :]
                high = jnp.floor(row * (1.0 / LOW))
                if make:
                    low = (row - high * LOW).astype(jnp.int32)
                    ids = lax.broadcasted_iota(jnp.int32, (LOW, LANES), 0)
                    onehot[c, :, LANES * i:LANES * (i + 1)] = jnp.where(ids == low, 1.0, 0.0).astype(BF16)
                sign = 2.0 * pts[columns + 4, pl.ds(s, 1), :] - 1.0
                v = values(s) * sign
                top = v.astype(BF16)
                rest = (v - top.astype(F32)).astype(BF16)
                wide = jnp.broadcast_to(high, (columns, LANES))
                masks = [jnp.where(wide == float(g), 1.0, 0.0).astype(BF16) for g in range(HIGH)]
                pieces.append(jnp.concatenate([top * g for g in masks] + [rest * g for g in masks], axis=0))
            left = jnp.concatenate(pieces, axis=1)
            target[...] += lax.dot_general(left, onehot[c], (((1,), (1,)), ((), ())), preferred_element_type=F32)

    nbt = kk

    def start(copy):
        copy.start()

    def finish_recv(copy):
        copy.wait_recv()

    def finish_send(copy):
        copy.wait_send()

    for index, (low, bits) in enumerate(stages):
        group = 2 ** bits
        places = LANES // group

        def outward(h, action):
            at = halves * index + h
            return exchange(a_send.at[at], a_recv.at[at], a_ss.at[at], a_rs.at[at], low, bits, action)

        def homeward(h, action):
            at = halves * index + h
            return exchange(b_send.at[at], b_recv.at[at], b_ss.at[at], b_rs.at[at], low, bits, action)

        for h in range(halves):
            at = halves * index + h
            if index == 0:
                gather_half(h)
            pack(a_send.at[at], group, h)
            if index == 0 and h == 0:
                pl.semaphore_wait(barrier, devices - 1)
            mine = outward(h, start)
            a_recv[at, mine] = a_send[at, mine]
        make_maps(low, bits)
        if index == 0:
            for q in range(columns):
                for s in range(LEAF):
                    nbt[s, q:q + 1, :] = pts[q, s:s + 1, :]
            sketch_of(lambda s: nbt[s], skb, True)
        for h in range(halves):
            at = halves * index + h
            outward(h, finish_recv)
            unpack(a_recv.at[at], group, h)
            half = slice(256 * h, 256 * (h + 1))
            for k in range(low, low + bits):
                span = places * 2 ** (k - low)
                full = cbuf[half, :]
                wide = lax.broadcasted_iota(jnp.int32, full.shape, 1)
                part[half, :] = jnp.where((wide // span) % 2 == 0,
                                          pltpu.roll(full, LANES - span, 1), pltpu.roll(full, span, 1))

                def mix(v, acc):
                    own = [mats[2 * k, v, 8 * t:8 * t + 8] for t in range(4)]
                    cross = [mats[2 * k + 1, v, 8 * t:8 * t + 8] for t in range(4)]
                    out = []
                    for q in range(8):
                        row = cbuf[pl.ds((8 * h + q) * 32 + v, 1), :]
                        other = part[pl.ds((8 * h + q) * 32 + v, 1), :]
                        for t in range(4):
                            out.append(acc[4 * q + t] + own[t] * row + cross[t] * other)
                    return tuple(out)

                init = tuple(0.85 * cbuf[pl.ds((8 * h + q) * 32 + 8 * t, 8), :] for q in range(8) for t in range(4))
                acc = lax.fori_loop(0, WIDTH, mix, init, unroll=2)
                for q in range(8):
                    for t in range(4):
                        cbuf[pl.ds((8 * h + q) * 32 + 8 * t, 8), :] = acc[4 * q + t]
            pack(b_send.at[at], group, h)
            mine = homeward(h, start)
            b_recv[at, mine] = b_send[at, mine]
        for h in range(halves):
            outward(h, finish_send)
        for h in range(halves):
            homeward(h, finish_recv)
            unpack(b_recv.at[halves * index + h], group, h)
        for h in range(halves):
            homeward(h, finish_send)

    for c in range(LEAF // 8):
        def spread_out(w, acc):
            coef = [cbuf[pl.ds(8 * h * 32 + w, 8, stride=32), :] for h in range(halves)]
            out = []
            for s in range(8):
                row = leaf[8 * c + s, pl.ds(w, 1), :]
                for h in range(halves):
                    out.append(acc[halves * s + h] + coef[h] * row)
            return tuple(out)

        init = tuple(
            jnp.broadcast_to(pts[columns + 2, 8 * c + s:8 * c + s + 1, :], (8, LANES)) * nbt[8 * c + s, 8 * h:8 * h + 8]
            for s in range(8) for h in range(halves))
        acc = lax.fori_loop(0, WIDTH, spread_out, init, unroll=2)
        for s in range(8):
            for h in range(halves):
                part[(8 * c + s) * columns + 8 * h:(8 * c + s) * columns + 8 * h + 8, :] = acc[halves * s + h]

    inner = jnp.zeros((columns, LANES), F32)
    square, energy = inner, inner
    for s in range(LEAF):
        v, image = nbt[s], part[s * columns:(s + 1) * columns, :]
        inner, square, energy = inner + v * image, square + v * v, energy + image * image
    lane_q = lax.broadcasted_iota(jnp.int32, (columns, LANES), 1)
    row_q = lax.broadcasted_iota(jnp.int32, (columns, LANES), 0)
    packed = jnp.zeros((columns, LANES), F32)
    for i, value in enumerate((inner, square, energy)):
        packed = jnp.where(lane_q == row_q + columns * i, jnp.sum(value, axis=1, keepdims=True), packed)
    sum_send[...] = jnp.sum(packed, axis=0, keepdims=True)

    def to_all(source, recv, ss, rs, action):
        @pl.loop(1, devices)
        def _(i):
            other = lax.rem(me + i, devices)
            here = other if action is finish_recv else me
            action(pltpu.make_async_remote_copy(
                source(other), recv.at[here], ss.at[other], rs.at[here],
                device_id=(other,), device_id_type=MESH))

    to_all(lambda d: sum_send, sum_recv, s_ss, s_rs, start)
    sum_recv[me] = sum_send[...]
    sketch_of(lambda s: part[pl.ds(pl.multiple_of(s * columns, columns), columns), :], ski, False)
    to_all(lambda d: sum_send, sum_recv, s_ss, s_rs, finish_recv)
    totals = jnp.sum(sum_recv[...], axis=0)

    def column(i):
        picked = jnp.where(lane_q == row_q + columns * i, jnp.broadcast_to(totals, (columns, LANES)), 0.0)
        return jnp.broadcast_to(jnp.sum(picked, axis=1, keepdims=True) * (1.0 / total_points), (columns, LANES))

    inner_mean, square_mean, energy_mean = column(0), column(1), column(2)
    projection = inner_mean / (square_mean + EPSILON)
    energy = energy_mean - 2.0 * projection * inner_mean + projection * projection * square_mean
    spread = jnp.sqrt(energy + EPSILON)
    inverse = 1.0 / spread
    for i, value in enumerate((projection, spread)):
        arn_ref[i:i + 1, :] = jnp.sum(jnp.where(lane_q == row_q, value, 0.0), axis=0, keepdims=True)[:, :columns]

    rows_each = rs_send.shape[1]
    factor = math.sqrt(SKETCH / total_points)
    lowest = HIGH * columns
    part_tiles = LOW // LANES
    for n in range(devices):
        flat = n * rows_each
        tile, row = flat // 8, flat % 8
        strip, side = tile // part_tiles, tile % part_tiles
        top = strip * 8 + row
        q0 = top % columns
        cols = slice(side * LANES, (side + 1) * LANES)
        img = ski[top:top + rows_each, cols] + ski[lowest + top:lowest + top + rows_each, cols]
        bas = skb[top:top + rows_each, cols] + skb[lowest + top:lowest + top + rows_each, cols]
        rs_send[n] = (img - projection[q0:q0 + rows_each] * bas) * (factor * inverse[q0:q0 + rows_each])
    to_all(lambda d: rs_send.at[d], rs_recv, r_ss, r_rs, start)
    rs_recv[me] = rs_send[me]

    for s in range(LEAF):
        pts_rows = (part[s * columns:(s + 1) * columns, :] - projection * nbt[s]) * inverse
        nbt[s] = pts_rows
    for q in range(columns):
        for s in range(LEAF):
            pts[q, s:s + 1, :] = nbt[s, q:q + 1, :]
    for i in range(columns // 4):
        for j in range(4):
            for g in range(4):
                tbuf[0, 32 * g:32 * g + 32, 32 * j:32 * j + 32] = pts[4 * i + j, :, 32 * g:32 * g + 32]
        raw[LANES * i:LANES * (i + 1), :] = tbuf[0].T
    for r in range(LANES // 4):
        for h in range(halves):
            nb_ref[8 * h:8 * h + 8, LANES * r:LANES * (r + 1)] = raw[pl.ds(256 * h + r, 8, stride=32), :]

    to_all(lambda d: rs_send.at[d], rs_recv, r_ss, r_rs, finish_recv)
    own_chunk[...] = jnp.sum(rs_recv[...], axis=0)
    to_all(lambda d: own_chunk, ag_recv, g_ss, g_rs, start)
    ag_recv[me] = own_chunk[...]
    to_all(lambda d: sum_send, sum_recv, s_ss, s_rs, finish_send)
    to_all(lambda d: rs_send.at[d], rs_recv, r_ss, r_rs, finish_send)
    to_all(lambda d: own_chunk, ag_recv, g_ss, g_rs, finish_recv)
    for n in range(devices):
        flat = n * rows_each
        tile, row = flat // 8, flat % 8
        strip, side = tile // part_tiles, tile % part_tiles
        top = strip * 8 + row
        q0, high = top % columns, top // columns
        begin = high * LOW + side * LANES
        sketch_ref[q0:q0 + rows_each, begin:begin + LANES] = ag_recv[n]
    to_all(lambda d: own_chunk, ag_recv, g_ss, g_rs, finish_send)


def split(x):
    top = x.astype(BF16)
    return top, (x - top.astype(F32)).astype(BF16)


def tile_kernel(devices, total_points, scale_ref, v_in, coords_in, diag_in, rows_in, signs_in,
                nb_ref, sketch_ref, arn_ref, v_ref, coords_ref, diag_ref, rows_ref, signs_ref,
                small_send, small, vals, phases, steps, mats, leaf, state, coef,
                image, back, hot, left, masks, sum_send, sum_recv, sum_total, sum_joined, rb_send,
                rb_recv, rb_total, rb_joined, ri_send, ri_recv, ri_total, ri_joined, ag_recv, own_chunk, sems,
                io_sems):
    me = lax.axis_index("box")
    columns = nb_ref.shape[0]
    sections = devices.bit_length() - 1
    per_tile = LANES // LEAF
    half = LANES // 2
    barrier = pltpu.get_barrier_semaphore()

    @pl.loop(1, devices)
    def _(i):
        pl.semaphore_signal(barrier, inc=1, device_id=(lax.rem(me + i, devices),), device_id_type=MESH)

    incoming = [pltpu.make_async_copy(a, b, io_sems.at[i]) for i, (a, b) in enumerate((
        (v_in, v_ref), (coords_in, coords_ref), (diag_in, diag_ref), (rows_in, rows_ref), (signs_in, signs_ref)))]
    for copy in incoming:
        copy.start()
    lane = lax.broadcasted_iota(jnp.int32, (8, LANES), 1)
    sub = lax.broadcasted_iota(jnp.int32, (8, LANES), 0)
    planes = 4
    plane_size = devices // planes
    plane, seat = me // plane_size, lax.rem(me, plane_size)
    halves = devices // 2
    side = plane // 2

    def facing(away):
        there = 0
        for b in range(planes.bit_length() - 1):
            bit = lax.rem(plane // 2 ** b, 2)
            there = there + 2 ** b * ((1 - bit) if (away >> b) & 1 else bit)
        return there

    def send(source, target, which, other):
        pltpu.make_async_remote_copy(
            source, target, sems.at[2 * which], sems.at[2 * which + 1],
            device_id=(other,), device_id_type=MESH).start()

    def to_all(source, target, which, aways):
        for away in aways:
            there = {3: (1 - side) * (planes - 1), 2: 2 - side, 1: facing(1), 0: plane}[away]

            @pl.loop(0 if away else 1, plane_size)
            def _(i):
                other = plane_size * there + lax.rem(seat + i, plane_size)
                send(source(other), target, which, other)

    def to_plane(source, target, which):
        @pl.loop(1, plane_size)
        def _(i):
            other = lax.rem(seat + i, plane_size)
            send(source(other), target, which, plane_size * plane + other)

    def to_planes(source, target, which):
        for away in range(planes - 1, 0, -1):
            send(source, target, which, plane_size * facing(away) + seat)

    def finish(ref, which, end):
        pltpu.make_async_copy(ref, ref, sems.at[2 * which + end]).wait()

    def columns_at(ref, tile):
        return ref.at[:, pl.ds(pl.multiple_of(tile * LANES, LANES), LANES)]

    others, mates, peers = pl.ds(0, devices - 1), pl.ds(0, plane_size - 1), pl.ds(0, planes - 1)
    side_rows = 5
    side_part = pl.ds(0, side_rows)

    for copy in incoming:
        copy.wait()
    rows_f, signs_f = rows_ref[...].astype(F32), signs_ref[...].astype(F32)
    for e in range(devices):
        here = slice(e * LANES, (e + 1) * LANES)
        small_send[e, 0:2, :] = coords_ref[:, here].astype(F32)
        small_send[e, 2:3, :] = diag_ref[e:e + 1, :]
        small_send[e, 3:4, :] = rows_f[e:e + 1, :]
        small_send[e, 4:5, :] = signs_f[e:e + 1, :]
    scale = lax.rem(scale_ref[0], MODULUS)
    spot = lane // LEAF
    inner_lane = (lane % LEAF).astype(F32)
    for k in range(sections):
        for g in range(devices // 8):
            ident = ((8 * g + sub) * LANES + per_tile * me + spot) * 37
            x = (ident + 101 * k).astype(F32)
            rest = x - jnp.floor(x * (1.0 / (MODULUS - 1))) * float(MODULUS - 1)
            rest = jnp.where(rest < 0.0, rest + float(MODULUS - 1), rest)
            rest = jnp.where(rest >= float(MODULUS - 1), rest - float(MODULUS - 1), rest)
            key = rest.astype(jnp.int32) + 1
            unit_phase = fold(fold(key * scale)).astype(F32)
            for m, second in enumerate((2.0, 1.0)):
                phi = remainder(unit_phase * (inner_lane + second))
                phases[2 * k + m, 8 * g:8 * g + 8, :] = phi
                steps[2 * k + m, 8 * g:8 * g + 8, :] = scaled_cos(8.0 * phi, 2.0)

    wide_sub = lax.broadcasted_iota(jnp.int32, (WIDTH, LANES), 0)
    wide_lane = lax.broadcasted_iota(jnp.int32, (WIDTH, LANES), 1)
    ident_part = jnp.where(wide_lane % WIDTH == wide_sub, 0.85, 0.0)
    sub_f = sub.astype(F32)
    def make_maps(begins, ends):
        for k in range(sections):
            maps_of(k, begins[k], ends[k])

    def maps_of(k, begin_pair, end_pair):
        stride = 2 ** k

        @pl.loop(begin_pair, end_pair)
        def _(pair):
            first_tile = (pair // stride) * (2 * stride) + pair % stride
            for bit in range(2):
                d = first_tile + stride * bit
                for m in range(2):
                    amplitude = (0.35 if m == 0 else 0.6) / math.sqrt(WIDTH)
                    first, offset = (1.0, 0.0) if m == 0 else (3.0, 4096.0)
                    phi = phases[2 * k + m, pl.ds(d, 1), :]
                    step = steps[2 * k + m, pl.ds(d, 1), :]
                    one = scaled_cos(phi * (sub_f + (8.0 + first)) + offset, amplitude)
                    two = scaled_cos(phi * (sub_f + (16.0 + first)) + offset, amplitude)
                    full = jnp.concatenate([step * one - two, one, two, step * two - one], axis=0)
                    if m == 0:
                        full = full + ident_part
                    top, low = split(full)
                    begin = LANES * (bit if m == 0 else 1 - bit)
                    mats[k, pair, 64 * bit:64 * bit + 32, begin:begin + LANES] = top
                    mats[k, pair, 64 * bit + 32:64 * bit + 64, begin:begin + LANES] = low

    hops = lax.rem(me // 2, 2) + lax.rem(me // 4, 2) + plane
    budget = 18 * (5 - hops) - 8
    early = [jnp.clip(budget - k * (devices // 2), 0, devices // 2) for k in range(sections)]
    make_maps([0] * sections, early)
    pl.semaphore_wait(barrier, devices - 1)
    for which, aways in ((0, (3, 2)), (7, (1, 0))):
        to_all(lambda d: small_send.at[d, side_part], small.at[me, side_part], which, aways)
    for which, aways in ((8, (1, 0)), (1, (3, 2))):
        to_all(lambda d: columns_at(v_ref, d), vals.at[me], which, aways)
    small[me] = small_send[me]
    vals[me] = columns_at(v_ref, me)[...]

    make_maps(early, [devices // 2] * sections)
    lanes_q = lax.broadcasted_iota(jnp.int32, (columns, LANES), 1)
    rows_q = lax.broadcasted_iota(jnp.int32, (columns, LANES), 0)

    def place(tile):
        return pl.ds(pl.multiple_of(tile * LANES, LANES), LANES)

    low_ids = lax.broadcasted_iota(jnp.int32, (LOW, LANES), 0).astype(F32).astype(BF16)
    high_ids = (lax.broadcasted_iota(jnp.int32, (HIGH * columns, LANES), 0) // columns).astype(F32).astype(BF16)
    one, nil = jnp.array(1.0, BF16), jnp.array(0.0, BF16)

    def make_hot(row_of, sign_of, begin, count):
        @pl.loop(0, count, unroll=2)
        def _(i):
            d = begin + i
            row = row_of(d)
            high = jnp.floor(row * (1.0 / LOW))
            low = jnp.broadcast_to((row - high * LOW).astype(BF16), (LOW, LANES))
            hot[:, place(d)] = jnp.where(low_ids == low, one, nil)
            flip = (1 - 2 * (d // halves)).astype(F32)
            sign = jnp.broadcast_to(((2.0 * sign_of(d) - 1.0) * flip).astype(BF16), (HIGH * columns, LANES))
            wide = jnp.broadcast_to(high.astype(BF16), (HIGH * columns, LANES))
            masks[d] = jnp.where(high_ids == wide, sign, nil)

    def place_values(d, at, value):
        top, rest = split(value)
        for g in range(HIGH):
            mask = masks[d, columns * g:columns * (g + 1), :]
            left[columns * g:columns * (g + 1), at] = top * mask
            left[columns * (HIGH + g):columns * (HIGH + g + 1), at] = rest * mask

    def sketch_product():
        points = left.shape[1] // 2
        o = [lax.dot_general(left[:, part], hot[:, part], (((1,), (1,)), ((), ())), preferred_element_type=F32)
             for part in (slice(0, points), slice(points, 2 * points))]
        return (o[0][:HIGH * columns] + o[0][HIGH * columns:]) - (o[1][:HIGH * columns] + o[1][HIGH * columns:])

    factor = math.sqrt(SKETCH / total_points)

    def start_reduce(sk, pieces, landed, which):
        for n in range(plane_size):
            pieces[n] = sk[columns * n:columns * (n + 1), :]
        to_plane(lambda n: pieces.at[n], landed.at[seat], which)
        landed[seat] = pieces[seat]

    def next_reduce(landed, total, joined, which, first):
        finish(landed.at[pl.ds(0, plane_size - 1)], first, 1)
        total[...] = jnp.sum(landed[...], axis=0)
        to_planes(total, joined.at[plane], which)
        joined[plane] = total[...]

    make_hot(lambda d: rows_ref[pl.ds(d, 1), :].astype(F32), lambda d: signs_ref[pl.ds(d, 1), :].astype(F32), 0, devices)

    @pl.loop(0, devices)
    def _(d):
        place_values(d, place(d), v_ref[:, place(d)])

    basis_sketch = sketch_product()
    start_reduce(basis_sketch, rb_send, rb_recv, 2)

    fx = (sub % 4 + 1).astype(F32)
    fy = (sub // 4 + 1).astype(F32)
    unit = 1.0 / math.sqrt(LEAF)
    point_masks = [jnp.where(lanes_q // LEAF == j, 1.0, 0.0).astype(BF16) for j in range(per_tile)]
    column_masks = [jnp.where((wide_lane % half) // columns == j, 1.0, 0.0).astype(BF16) for j in range(per_tile)]
    first_half = wide_lane < half

    def combine(o):
        s = o[0:32] + o[32:64]
        return s + pltpu.roll(s, half, 1)

    def expand(total):
        top = total.astype(BF16).astype(F32)
        y = jnp.where(first_half, top, total - top).astype(BF16)
        return jnp.concatenate([y * m for m in column_masks], axis=0)

    def leaves(begin):
        @pl.loop(0, halves, unroll=4)
        def _(i):
            d = begin + i
            pair = fold(small[d, 0:2, :].astype(jnp.int32) * scale).astype(F32)
            px, py = pair[0:1], pair[1:2]
            phases_of = [fx * px + (fy + 2.0 * t) * py for t in range(2)]
            full = jnp.concatenate([scaled_cos(n, unit) for n in phases_of] + [scaled_sin(n, unit) for n in phases_of], axis=0)
            top, low = split(full)
            leaf[d, 0:32] = top
            leaf[d, 32:64] = low

    def gather(begin):
        for i in range(halves):
            d = begin + i
            top, rest = split(vals[d])
            spread_v = jnp.concatenate([top * m for m in point_masks] + [rest * m for m in point_masks], axis=0)
            o = lax.dot_general(leaf[d], spread_v, (((1,), (1,)), ((), ())), preferred_element_type=F32)
            state[0, d] = expand(combine(o))

    def section(k, begin, count):
        stride = 2 ** k
        now = k % 2
        for i in range(count // 2):
            d0 = begin + (i // stride) * (2 * stride) + i % stride
            d1 = d0 + stride
            x = jnp.concatenate([state[now, d0], state[now, d1]], axis=0)
            o = jnp.dot(mats[k, begin // 2 + i], x, preferred_element_type=F32)
            for d, part in ((d0, o[0:64]), (d1, o[64:128])):
                total = combine(part)
                if k == sections - 1:
                    coef[32 * d:32 * d + 32, :] = total
                else:
                    state[1 - now, d] = expand(total)

    near, away = side * halves, (1 - side) * halves
    for begin, small_which, count in ((near, 7, halves - 1), (away, 0, halves)):
        finish(small.at[pl.ds(0, count), side_part], small_which, 1)
        leaves(begin)
        make_hot(lambda d: small[d, 3:4, :], lambda d: small[d, 4:5, :], begin, halves)
    for begin, vals_which, count in ((near, 8, halves - 1), (away, 1, halves)):
        arrived = pl.ds(0, count)
        finish(vals.at[arrived], vals_which, 1)
        gather(begin)
        for k in range(sections - 1):
            section(k, begin, halves)
    next_reduce(rb_recv, rb_total, rb_joined, 9, 2)
    section(sections - 1, 0, devices)
    tile_lane = lax.broadcasted_iota(jnp.int32, (half, 2 * LANES), 1)
    tile_masks = [jnp.where((tile_lane % LANES) // WIDTH == t, 1.0, 0.0).astype(BF16) for t in range(4)]
    zero = jnp.zeros((columns, LANES), F32)
    inner, square, energy = zero, zero, zero
    for g in range(devices // 4):
        flipped = coef[LANES * g:LANES * (g + 1), :].T
        top, rest = split(flipped[0:half])
        both = jnp.concatenate([top, rest], axis=1)
        lhs = jnp.concatenate([both * m for m in tile_masks], axis=0)
        tops = jnp.concatenate([leaf[4 * g + t, 0:32] for t in range(4)], axis=0)
        lows = jnp.concatenate([leaf[4 * g + t, 32:64] for t in range(4)], axis=0)
        right = jnp.concatenate([tops, lows], axis=1)
        o = jnp.dot(lhs, jnp.concatenate([right, right], axis=0), preferred_element_type=F32)
        o = o[:, 0:LANES] + o[:, LANES:2 * LANES]
        for t in range(4):
            d = 4 * g + t
            v = vals[d]
            img = jnp.broadcast_to(small[d, 2:3, :], (columns, LANES)) * v
            for j in range(per_tile):
                begin = half * t + columns * j
                img = img + jnp.where(lanes_q // LEAF == j, o[begin:begin + columns], 0.0)
            image[d] = img
            place_values(d, slice(LANES * d, LANES * (d + 1)), img)
            inner, square, energy = inner + v * img, square + v * v, energy + img * img

    to_all(lambda d: image.at[d], back.at[me], 5, (3, 2, 1, 0))
    packed = zero
    for i, value in enumerate((inner, square, energy)):
        packed = jnp.where(lanes_q == rows_q + columns * i, jnp.sum(value, axis=1, keepdims=True), packed)
    sum_send[...] = jnp.sum(packed, axis=0, keepdims=True)
    image_sketch = sketch_product()
    start_reduce(image_sketch, ri_send, ri_recv, 4)
    to_plane(lambda d: sum_send, sum_recv.at[seat], 3)
    sum_recv[seat] = sum_send[...]
    back[me] = image[me]

    finish(small_send.at[pl.ds(0, halves), side_part], 0, 0)
    finish(small_send.at[pl.ds(0, halves - 1), side_part], 7, 0)
    finish(vals.at[pl.ds(0, halves)], 1, 0)
    finish(vals.at[pl.ds(0, halves - 1)], 8, 0)
    finish(rb_send.at[mates], 2, 0)
    next_reduce(ri_recv, ri_total, ri_joined, 11, 4)
    finish(sum_recv.at[mates], 3, 1)
    sum_total[...] = jnp.sum(sum_recv[...], axis=0)
    to_planes(sum_total, sum_joined.at[plane], 10)
    sum_joined[plane] = sum_total[...]
    finish(rb_joined.at[peers], 9, 0)
    finish(rb_joined.at[peers], 9, 1)
    finish(sum_recv.at[mates], 3, 0)
    finish(ri_send.at[mates], 4, 0)
    basis_total = jnp.sum(rb_joined[...], axis=0)
    finish(sum_joined.at[peers], 10, 1)
    totals = jnp.sum(sum_joined[...], axis=0)

    def column(i):
        picked = jnp.where(lanes_q == rows_q + columns * i, jnp.broadcast_to(totals, (columns, LANES)), 0.0)
        return jnp.broadcast_to(jnp.sum(picked, axis=1, keepdims=True) * (1.0 / total_points), (columns, LANES))

    inner_mean, square_mean, energy_mean = column(0), column(1), column(2)
    projection = inner_mean / (square_mean + EPSILON)
    energy = energy_mean - 2.0 * projection * inner_mean + projection * projection * square_mean
    spread = jnp.sqrt(energy + EPSILON)
    inverse = 1.0 / spread
    for i, value in enumerate((projection, spread)):
        arn_ref[i:i + 1, :] = jnp.sum(jnp.where(lanes_q == rows_q, value, 0.0), axis=0, keepdims=True)[:, :columns]
    finish(ri_joined.at[peers], 11, 1)
    wide = lambda x: jnp.concatenate([x] * (LOW // LANES), axis=1)
    own_chunk[...] = (jnp.sum(ri_joined[...], axis=0) - basis_total * wide(projection)) * wide(factor * inverse)
    to_plane(lambda d: own_chunk, ag_recv.at[seat], 6)
    ag_recv[seat] = own_chunk[...]
    finish(back.at[others], 5, 1)
    for e in range(devices):
        here = slice(e * LANES, (e + 1) * LANES)
        nb_ref[:, here] = (back[e] - projection * v_ref[:, here]) * inverse
    finish(image.at[others], 5, 0)
    finish(ri_joined.at[peers], 11, 0)
    finish(sum_joined.at[peers], 10, 0)
    finish(ag_recv.at[mates], 6, 0)
    finish(ag_recv.at[mates], 6, 1)
    for n in range(plane_size):
        sketch_ref[:, LOW * n:LOW * (n + 1)] = ag_recv[n]


def deliver(*refs):
    copies = [pltpu.make_async_copy(refs[i], refs[3 + i], refs[6].at[i]) for i in range(3)]
    for copy in copies:
        copy.start()
    for copy in copies:
        copy.wait()


def together(devices, basis_vector, diagonal, coords, phase_scale, sketch_rows, sketch_signs):
    columns, local_points = basis_vector.shape
    sections = devices.bit_length() - 1
    plane = (local_points // LANES, LANES)
    far = pl.BlockSpec(memory_space=pltpu.HBM)
    vmem = pl.BlockSpec(memory_space=pltpu.VMEM)
    tile = pltpu.VMEM((devices, columns, LANES), F32)
    chunk = (columns, LOW)
    pieces = pltpu.VMEM((HIGH,) + chunk, F32)
    reduce_parts = [pieces, pieces, pltpu.VMEM(chunk, F32), pltpu.VMEM((devices // HIGH,) + chunk, F32)]
    results = pl.pallas_call(
        functools.partial(tile_kernel, devices, local_points * devices),
        out_shape=(
            jax.ShapeDtypeStruct((columns, local_points), F32),
            jax.ShapeDtypeStruct((columns, SKETCH), F32),
            jax.ShapeDtypeStruct((2, columns), F32)),
        in_specs=[pl.BlockSpec(memory_space=pltpu.SMEM)] + [far] * 5,
        out_specs=(vmem,) * 3,
        scratch_shapes=[
            pltpu.VMEM(basis_vector.shape, F32),
            pltpu.VMEM(coords.shape, jnp.int32),
            pltpu.VMEM(plane, F32),
            pltpu.VMEM(plane, jnp.int32),
            pltpu.VMEM(plane, jnp.int32),
            pltpu.VMEM((devices, 8, LANES), F32),
            pltpu.VMEM((devices, 8, LANES), F32),
            tile,
            pltpu.VMEM((2 * sections, devices, LANES), F32),
            pltpu.VMEM((2 * sections, devices, LANES), F32),
            pltpu.VMEM((sections, devices // 2, 4 * WIDTH, 2 * LANES), BF16),
            pltpu.VMEM((devices, 2 * WIDTH, LANES), BF16),
            pltpu.VMEM((2, devices, LANES, LANES), BF16),
            pltpu.VMEM((devices * WIDTH, LANES), F32),
            tile, tile,
            pltpu.VMEM((LOW, local_points), BF16),
            pltpu.VMEM((2 * HIGH * columns, local_points), BF16),
            pltpu.VMEM((devices, HIGH * columns, LANES), BF16),
            pltpu.VMEM((1, LANES), F32),
            pltpu.VMEM((HIGH, 1, LANES), F32),
            pltpu.VMEM((1, LANES), F32),
            pltpu.VMEM((devices // HIGH, 1, LANES), F32),
            *reduce_parts, *reduce_parts, pieces,
            pltpu.VMEM(chunk, F32),
            pltpu.SemaphoreType.DMA((24,)),
            pltpu.SemaphoreType.DMA((5,)),
        ],
        compiler_params=pltpu.CompilerParams(
            collective_id=0, has_side_effects=True, vmem_limit_bytes=24 * 2**20),
        name="gmres",
    )(phase_scale, *(pltpu.with_memory_space_constraint(x, pltpu.HBM) for x in (
        basis_vector, coords, diagonal.reshape(plane), sketch_rows.reshape(plane),
        sketch_signs.reshape(plane))))
    return pl.pallas_call(
        deliver,
        out_shape=[jax.ShapeDtypeStruct(x.shape, x.dtype) for x in results],
        in_specs=[vmem] * 3,
        out_specs=[far] * 3,
        scratch_shapes=[pltpu.SemaphoreType.DMA((3,))],
        compiler_params=pltpu.CompilerParams(vmem_limit_bytes=2**20),
        name="deliver",
    )(*results)


def body(basis_vector, diagonal, coords, phase_scale, sketch_rows, sketch_signs):
    columns, local_points = basis_vector.shape
    devices = lax.axis_size("box")
    if devices * LANES == local_points:
        return together(devices, basis_vector, diagonal, coords, phase_scale, sketch_rows, sketch_signs)
    sections = devices.bit_length() - 1
    count = -(-sections // 5)
    stages, low = [], 0
    for i in range(count):
        bits = (sections - low) // (count - i)
        stages.append((low, bits))
        low += bits
    group = 2 ** max(bits for _, bits in stages)
    group_rows = [columns * WIDTH // LANES * (LANES // 2 ** bits) for _, bits in stages]
    plane = (local_points // LANES, LANES)
    rows_each = HIGH * columns * LOW // LANES // devices
    vmem = pl.BlockSpec(memory_space=pltpu.VMEM)
    dma = pltpu.SemaphoreType.DMA
    count_rows = max(group_rows)
    halves = columns // 8
    new_basis, sketch, arn = pl.pallas_call(
        functools.partial(kernel, devices, stages, local_points * devices),
        out_shape=(
            jax.ShapeDtypeStruct((columns, local_points), F32),
            jax.ShapeDtypeStruct((columns, SKETCH), F32),
            jax.ShapeDtypeStruct((2, columns), F32)),
        in_specs=[pl.BlockSpec(memory_space=pltpu.SMEM), vmem, vmem, vmem, vmem, vmem],
        out_specs=(vmem, vmem, vmem),
        scratch_shapes=[
            pltpu.VMEM(((columns + 8) * LEAF, LANES), F32),
            pltpu.VMEM((columns + 8, LEAF, LANES), F32),
            pltpu.VMEM((LEAF, WIDTH, LANES), F32),
            pltpu.VMEM((2 * sections, WIDTH, WIDTH, LANES), F32),
            pltpu.VMEM((LEAF, columns, LANES), F32),
            pltpu.VMEM((columns * WIDTH, LANES), F32),
            pltpu.VMEM((columns * WIDTH, LANES), F32),
            pltpu.VMEM((columns * WIDTH // LANES, LANES, LANES), F32),
            pltpu.VMEM((2, LEAF, LANES), F32),
            pltpu.VMEM((LEAF // 4, LOW, 4 * LANES), BF16),
            pltpu.VMEM((2 * HIGH * columns, LOW), F32),
            pltpu.VMEM((2 * HIGH * columns, LOW), F32),
            pltpu.VMEM((count * halves, group, count_rows // halves, LANES), F32),
            pltpu.VMEM((count * halves, group, count_rows // halves, LANES), F32),
            pltpu.VMEM((count * halves, group, count_rows // halves, LANES), F32),
            pltpu.VMEM((count * halves, group, count_rows // halves, LANES), F32),
            pltpu.VMEM((1, LANES), F32),
            pltpu.VMEM((devices, 1, LANES), F32),
            pltpu.VMEM((devices, rows_each, LANES), F32),
            pltpu.VMEM((devices, rows_each, LANES), F32),
            pltpu.VMEM((devices, rows_each, LANES), F32),
            pltpu.VMEM((rows_each, LANES), F32),
            dma((count * halves, group)), dma((count * halves, group)), dma((count * halves, group)), dma((count * halves, group)),
            dma((devices,)), dma((devices,)), dma((devices,)), dma((devices,)), dma((devices,)), dma((devices,)),
        ],
        compiler_params=pltpu.CompilerParams(
            collective_id=0, has_side_effects=True, vmem_limit_bytes=60 * 2**20),
        name="gmres",
    )(phase_scale, basis_vector, coords, diagonal.reshape(plane), sketch_rows.reshape(plane),
      sketch_signs.reshape(plane))
    return new_basis, sketch, arn


def solution(mesh):
    placed = (P(None, "box"), P("box"), P(None, "box"), P(), P("box"), P("box"))
    return jax.shard_map(
        body, mesh=mesh, in_specs=placed, out_specs=(P(None, "box"), P(), P()), check_vma=False
    )
```

```python
import functools
import math

import jax
import jax.numpy as jnp
import numpy as np
from jax import lax
from jax.experimental import pallas as pl
from jax.experimental.pallas import tpu as pltpu
from jax.sharding import PartitionSpec as P

WIDTH = 32
LEAF = 32
SKETCH = 2048
LANES = 128
HIGH = 8
LOW = SKETCH // HIGH
MODULUS = 8191
EPSILON = 1e-06
MESH = pl.DeviceIdType.MESH
F32 = jnp.float32
BF16 = jnp.bfloat16


def sine_series():
    node = np.cos((np.arange(400) + 0.5) * np.pi / 800)
    basis = np.stack([node ** (2 * i) for i in range(6)], 1)
    exact = np.sin(np.pi * node * 4096 / MODULUS) / node
    return np.linalg.lstsq(basis, exact, rcond=None)[0]


SERIES = sine_series()


def remainder(n):
    return n - jnp.floor(n * (1.0 / MODULUS) + 0.5) * float(MODULUS)


def half_sine(n, gain):
    t = remainder(n) * (1.0 / 4096)
    z = t * t
    total = z * float(SERIES[5] * gain) + float(SERIES[4] * gain)
    for c in SERIES[3::-1]:
        total = total * z + float(c * gain)
    return total * t


def scaled_cos(n, amplitude):
    s = half_sine(n, math.sqrt(2.0 * amplitude))
    return amplitude - s * s


def scaled_sin(n, amplitude):
    return scaled_cos(n - 0.25 * MODULUS, amplitude)


def fold(p):
    return (p & MODULUS) + lax.shift_right_logical(p, 13)


def kernel(devices, stages, total_points, scale_ref, v_ref, coords_ref, diag_ref, rows_ref, signs_ref,
           nb_ref, sketch_ref, arn_ref, raw, pts, leaf, mats, kk, cbuf, part, tbuf, work, onehot, skb, ski,
           a_send, a_recv, b_send, b_recv, sum_send, sum_recv, rs_send, rs_recv, ag_recv, own_chunk,
           a_ss, a_rs, b_ss, b_rs, s_ss, s_rs, r_ss, r_rs, g_ss, g_rs):
    me = lax.axis_index("box")
    columns = nb_ref.shape[0]
    halves = columns // 8
    barrier = pltpu.get_barrier_semaphore()

    @pl.loop(1, devices)
    def _(i):
        pl.semaphore_signal(barrier, inc=1, device_id=(lax.rem(me + i, devices),), device_id_type=MESH)

    lane = lax.broadcasted_iota(jnp.int32, (8, LANES), 1)
    sub = lax.broadcasted_iota(jnp.int32, (8, LANES), 0)
    scale = lax.rem(scale_ref[0], MODULUS)

    for r in range(LANES // 4):
        here = slice(LANES * r, LANES * (r + 1))
        for h in range(halves):
            raw[pl.ds(256 * h + r, 8, stride=32), :] = v_ref[8 * h:8 * h + 8, here]
        pair = coords_ref[:, here].astype(F32)
        raw[columns * 32 + r:columns * 32 + r + 1, :] = pair[0:1]
        raw[columns * 32 + 32 + r:columns * 32 + 33 + r, :] = pair[1:2]
    raw[(columns + 2) * 32:(columns + 3) * 32, :] = diag_ref[...]
    raw[(columns + 3) * 32:(columns + 4) * 32, :] = rows_ref[...].astype(F32)
    raw[(columns + 4) * 32:(columns + 5) * 32, :] = signs_ref[...].astype(F32)
    raw[(columns + 5) * 32:(columns + 8) * 32, :] = jnp.zeros((96, LANES), F32)
    for i in range((columns + 8) // 4):
        flipped = raw[LANES * i:LANES * (i + 1), :].T
        tbuf[0] = flipped
        for j in range(4):
            pts[4 * i + j] = jnp.concatenate(
                [tbuf[0, 32 * g:32 * g + 32, 32 * j:32 * j + 32] for g in range(4)], axis=1)

    def exact_phase(row):
        return fold(pts[columns + row].astype(jnp.int32) * scale).astype(F32)

    work[0] = exact_phase(0)
    work[1] = exact_phase(1)
    fx = (sub % 4 + 1).astype(F32)
    fy = (sub // 4 + 1).astype(F32)
    unit = 1.0 / math.sqrt(LEAF)

    @pl.loop(0, LEAF)
    def _(s):
        px = work[0, pl.ds(s, 1), :]
        py = work[1, pl.ds(s, 1), :]
        for tile in range(2):
            n = fx * px + (fy + 2.0 * tile) * py
            leaf[s, 8 * tile:8 * tile + 8] = scaled_cos(n, unit)
            leaf[s, 16 + 8 * tile:24 + 8 * tile] = scaled_sin(n, unit)

    def gather_half(h):
        def gather(s, acc):
            tiles = [leaf[s, 8 * t:8 * t + 8] for t in range(4)]
            out = []
            for q in range(8):
                row = pts[8 * h + q, pl.ds(s, 1), :]
                for t in range(4):
                    out.append(acc[4 * q + t] + tiles[t] * row)
            return tuple(out)

        acc = lax.fori_loop(0, LEAF, gather, tuple(jnp.zeros((8, LANES), F32) for _ in range(32)), unroll=2)
        for q in range(8):
            for t in range(4):
                cbuf[pl.ds((8 * h + q) * 32 + 8 * t, 8), :] = acc[4 * q + t]

    blocks = 8 * WIDTH // LANES

    def make_maps(low, bits):
        group = 2 ** bits
        places = LANES // group
        mine = lax.rem(me // 2 ** low, group)
        spot = mine * places + lane % places
        box = 4 * (spot % 32) + spot // 32
        member = me + (lane // places - mine) * 2 ** low
        ident = (member * LANES + box) * 37

        @pl.loop(low, low + bits)
        def _(k):
            x = (ident + 101 * k).astype(F32)
            rest = x - jnp.floor(x * (1.0 / (MODULUS - 1))) * float(MODULUS - 1)
            rest = jnp.where(rest < 0.0, rest + float(MODULUS - 1), rest)
            rest = jnp.where(rest >= float(MODULUS - 1), rest - float(MODULUS - 1), rest)
            key = rest.astype(jnp.int32) + 1
            unit_phase = fold(fold(key * scale)).astype(F32)
            wide = sub.astype(F32)
            for m in range(2):
                amplitude = (0.35 if m == 0 else 0.6) / math.sqrt(WIDTH)
                first, second, offset = (1.0, 2.0, 0.0) if m == 0 else (3.0, 1.0, 4096.0)
                mid = unit_phase * (wide + (8.0 + first))
                far = unit_phase * (wide + (16.0 + first))

                @pl.loop(0, WIDTH, unroll=2)
                def _(v):
                    times = v.astype(F32) + second
                    step = scaled_cos(unit_phase * (8.0 * times), 2.0)
                    one = scaled_cos(mid * times + offset, amplitude)
                    two = scaled_cos(far * times + offset, amplitude)
                    mats[2 * k + m, v, 8:16] = one
                    mats[2 * k + m, v, 16:24] = two
                    mats[2 * k + m, v, 0:8] = step * one - two
                    mats[2 * k + m, v, 24:32] = step * two - one

    def exchange(send, recv, ss, rs, low, bits, action):
        group = 2 ** bits
        mine = lax.rem(me // 2 ** low, group)

        @pl.loop(1, group)
        def _(i):
            other = lax.rem(mine + i, group)
            here = other if action is finish_recv else mine
            copy = pltpu.make_async_remote_copy(
                send.at[other], recv.at[here], ss.at[other], rs.at[here],
                device_id=(me + (other - mine) * 2 ** low,), device_id_type=MESH)
            action(copy)
        return mine

    def pack(send, group, h):
        places = LANES // group
        for j in range(blocks):
            at = LANES * (blocks * h + j)
            tbuf[j] = cbuf[at:at + LANES, :].T
        for d in range(group):
            for j in range(blocks):
                send[d, places * j:places * (j + 1), :] = tbuf[j, places * d:places * (d + 1), :]

    def unpack(recv, group, h):
        places = LANES // group
        for j in range(blocks):
            for d in range(group):
                tbuf[j, places * d:places * (d + 1), :] = recv[d, places * j:places * (j + 1), :]
        for j in range(blocks):
            at = LANES * (blocks * h + j)
            cbuf[at:at + LANES, :] = tbuf[j].T

    def sketch_of(values, target, make):
        target[...] = jnp.zeros_like(target)

        @pl.loop(0, LEAF // 4)
        def _(c):
            pieces = []
            for i in range(4):
                s = 4 * c + i
                row = pts[columns + 3, pl.ds(s, 1), :]
                high = jnp.floor(row * (1.0 / LOW))
                if make:
                    low = (row - high * LOW).astype(jnp.int32)
                    ids = lax.broadcasted_iota(jnp.int32, (LOW, LANES), 0)
                    onehot[c, :, LANES * i:LANES * (i + 1)] = jnp.where(ids == low, 1.0, 0.0).astype(BF16)
                sign = 2.0 * pts[columns + 4, pl.ds(s, 1), :] - 1.0
                v = values(s) * sign
                top = v.astype(BF16)
                rest = (v - top.astype(F32)).astype(BF16)
                wide = jnp.broadcast_to(high, (columns, LANES))
                masks = [jnp.where(wide == float(g), 1.0, 0.0).astype(BF16) for g in range(HIGH)]
                pieces.append(jnp.concatenate([top * g for g in masks] + [rest * g for g in masks], axis=0))
            left = jnp.concatenate(pieces, axis=1)
            target[...] += lax.dot_general(left, onehot[c], (((1,), (1,)), ((), ())), preferred_element_type=F32)

    nbt = kk

    def start(copy):
        copy.start()

    def finish_recv(copy):
        copy.wait_recv()

    def finish_send(copy):
        copy.wait_send()

    for index, (low, bits) in enumerate(stages):
        group = 2 ** bits
        places = LANES // group

        def outward(h, action):
            at = halves * index + h
            return exchange(a_send.at[at], a_recv.at[at], a_ss.at[at], a_rs.at[at], low, bits, action)

        def homeward(h, action):
            at = halves * index + h
            return exchange(b_send.at[at], b_recv.at[at], b_ss.at[at], b_rs.at[at], low, bits, action)

        for h in range(halves):
            at = halves * index + h
            if index == 0:
                gather_half(h)
            pack(a_send.at[at], group, h)
            if index == 0 and h == 0:
                pl.semaphore_wait(barrier, devices - 1)
            mine = outward(h, start)
            a_recv[at, mine] = a_send[at, mine]
        make_maps(low, bits)
        if index == 0:
            for q in range(columns):
                for s in range(LEAF):
                    nbt[s, q:q + 1, :] = pts[q, s:s + 1, :]
            sketch_of(lambda s: nbt[s], skb, True)
        for h in range(halves):
            at = halves * index + h
            outward(h, finish_recv)
            unpack(a_recv.at[at], group, h)
            half = slice(256 * h, 256 * (h + 1))
            for k in range(low, low + bits):
                span = places * 2 ** (k - low)
                full = cbuf[half, :]
                wide = lax.broadcasted_iota(jnp.int32, full.shape, 1)
                part[half, :] = jnp.where((wide // span) % 2 == 0,
                                          pltpu.roll(full, LANES - span, 1), pltpu.roll(full, span, 1))

                def mix(v, acc):
                    own = [mats[2 * k, v, 8 * t:8 * t + 8] for t in range(4)]
                    cross = [mats[2 * k + 1, v, 8 * t:8 * t + 8] for t in range(4)]
                    out = []
                    for q in range(8):
                        row = cbuf[pl.ds((8 * h + q) * 32 + v, 1), :]
                        other = part[pl.ds((8 * h + q) * 32 + v, 1), :]
                        for t in range(4):
                            out.append(acc[4 * q + t] + own[t] * row + cross[t] * other)
                    return tuple(out)

                init = tuple(0.85 * cbuf[pl.ds((8 * h + q) * 32 + 8 * t, 8), :] for q in range(8) for t in range(4))
                acc = lax.fori_loop(0, WIDTH, mix, init, unroll=2)
                for q in range(8):
                    for t in range(4):
                        cbuf[pl.ds((8 * h + q) * 32 + 8 * t, 8), :] = acc[4 * q + t]
            pack(b_send.at[at], group, h)
            mine = homeward(h, start)
            b_recv[at, mine] = b_send[at, mine]
        for h in range(halves):
            outward(h, finish_send)
        for h in range(halves):
            homeward(h, finish_recv)
            unpack(b_recv.at[halves * index + h], group, h)
        for h in range(halves):
            homeward(h, finish_send)

    for c in range(LEAF // 8):
        def spread_out(w, acc):
            coef = [cbuf[pl.ds(8 * h * 32 + w, 8, stride=32), :] for h in range(halves)]
            out = []
            for s in range(8):
                row = leaf[8 * c + s, pl.ds(w, 1), :]
                for h in range(halves):
                    out.append(acc[halves * s + h] + coef[h] * row)
            return tuple(out)

        init = tuple(
            jnp.broadcast_to(pts[columns + 2, 8 * c + s:8 * c + s + 1, :], (8, LANES)) * nbt[8 * c + s, 8 * h:8 * h + 8]
            for s in range(8) for h in range(halves))
        acc = lax.fori_loop(0, WIDTH, spread_out, init, unroll=2)
        for s in range(8):
            for h in range(halves):
                part[(8 * c + s) * columns + 8 * h:(8 * c + s) * columns + 8 * h + 8, :] = acc[halves * s + h]

    inner = jnp.zeros((columns, LANES), F32)
    square, energy = inner, inner
    for s in range(LEAF):
        v, image = nbt[s], part[s * columns:(s + 1) * columns, :]
        inner, square, energy = inner + v * image, square + v * v, energy + image * image
    lane_q = lax.broadcasted_iota(jnp.int32, (columns, LANES), 1)
    row_q = lax.broadcasted_iota(jnp.int32, (columns, LANES), 0)
    packed = jnp.zeros((columns, LANES), F32)
    for i, value in enumerate((inner, square, energy)):
        packed = jnp.where(lane_q == row_q + columns * i, jnp.sum(value, axis=1, keepdims=True), packed)
    sum_send[...] = jnp.sum(packed, axis=0, keepdims=True)

    def to_all(source, recv, ss, rs, action):
        @pl.loop(1, devices)
        def _(i):
            other = lax.rem(me + i, devices)
            here = other if action is finish_recv else me
            action(pltpu.make_async_remote_copy(
                source(other), recv.at[here], ss.at[other], rs.at[here],
                device_id=(other,), device_id_type=MESH))

    to_all(lambda d: sum_send, sum_recv, s_ss, s_rs, start)
    sum_recv[me] = sum_send[...]
    sketch_of(lambda s: part[pl.ds(pl.multiple_of(s * columns, columns), columns), :], ski, False)
    to_all(lambda d: sum_send, sum_recv, s_ss, s_rs, finish_recv)
    totals = jnp.sum(sum_recv[...], axis=0)

    def column(i):
        picked = jnp.where(lane_q == row_q + columns * i, jnp.broadcast_to(totals, (columns, LANES)), 0.0)
        return jnp.broadcast_to(jnp.sum(picked, axis=1, keepdims=True) * (1.0 / total_points), (columns, LANES))

    inner_mean, square_mean, energy_mean = column(0), column(1), column(2)
    projection = inner_mean / (square_mean + EPSILON)
    energy = energy_mean - 2.0 * projection * inner_mean + projection * projection * square_mean
    spread = jnp.sqrt(energy + EPSILON)
    inverse = 1.0 / spread
    for i, value in enumerate((projection, spread)):
        arn_ref[i:i + 1, :] = jnp.sum(jnp.where(lane_q == row_q, value, 0.0), axis=0, keepdims=True)[:, :columns]

    rows_each = rs_send.shape[1]
    factor = math.sqrt(SKETCH / total_points)
    lowest = HIGH * columns
    part_tiles = LOW // LANES
    for n in range(devices):
        flat = n * rows_each
        tile, row = flat // 8, flat % 8
        strip, side = tile // part_tiles, tile % part_tiles
        top = strip * 8 + row
        q0 = top % columns
        cols = slice(side * LANES, (side + 1) * LANES)
        img = ski[top:top + rows_each, cols] + ski[lowest + top:lowest + top + rows_each, cols]
        bas = skb[top:top + rows_each, cols] + skb[lowest + top:lowest + top + rows_each, cols]
        rs_send[n] = (img - projection[q0:q0 + rows_each] * bas) * (factor * inverse[q0:q0 + rows_each])
    to_all(lambda d: rs_send.at[d], rs_recv, r_ss, r_rs, start)
    rs_recv[me] = rs_send[me]

    for s in range(LEAF):
        pts_rows = (part[s * columns:(s + 1) * columns, :] - projection * nbt[s]) * inverse
        nbt[s] = pts_rows
    for q in range(columns):
        for s in range(LEAF):
            pts[q, s:s + 1, :] = nbt[s, q:q + 1, :]
    for i in range(columns // 4):
        for j in range(4):
            for g in range(4):
                tbuf[0, 32 * g:32 * g + 32, 32 * j:32 * j + 32] = pts[4 * i + j, :, 32 * g:32 * g + 32]
        raw[LANES * i:LANES * (i + 1), :] = tbuf[0].T
    for r in range(LANES // 4):
        for h in range(halves):
            nb_ref[8 * h:8 * h + 8, LANES * r:LANES * (r + 1)] = raw[pl.ds(256 * h + r, 8, stride=32), :]

    to_all(lambda d: rs_send.at[d], rs_recv, r_ss, r_rs, finish_recv)
    own_chunk[...] = jnp.sum(rs_recv[...], axis=0)
    to_all(lambda d: own_chunk, ag_recv, g_ss, g_rs, start)
    ag_recv[me] = own_chunk[...]
    to_all(lambda d: sum_send, sum_recv, s_ss, s_rs, finish_send)
    to_all(lambda d: rs_send.at[d], rs_recv, r_ss, r_rs, finish_send)
    to_all(lambda d: own_chunk, ag_recv, g_ss, g_rs, finish_recv)
    for n in range(devices):
        flat = n * rows_each
        tile, row = flat // 8, flat % 8
        strip, side = tile // part_tiles, tile % part_tiles
        top = strip * 8 + row
        q0, high = top % columns, top // columns
        begin = high * LOW + side * LANES
        sketch_ref[q0:q0 + rows_each, begin:begin + LANES] = ag_recv[n]
    to_all(lambda d: own_chunk, ag_recv, g_ss, g_rs, finish_send)


def split(x):
    top = x.astype(BF16)
    return top, (x - top.astype(F32)).astype(BF16)


def tile_kernel(devices, total_points, scale_ref, v_in, coords_in, diag_in, rows_in, signs_in,
                nb_ref, sketch_ref, arn_ref, v_ref, coords_ref, diag_ref, rows_ref, signs_ref,
                small_send, small, vals, phases, steps, mats, leaf, state, coef,
                image, back, hot, left, masks, sum_send, sum_recv, sum_total, sum_joined, rb_send,
                rb_recv, rb_total, rb_joined, ri_send, ri_recv, ri_total, ri_joined, ag_recv, own_chunk, sems,
                io_sems):
    me = lax.axis_index("box")
    columns = nb_ref.shape[0]
    sections = devices.bit_length() - 1
    per_tile = LANES // LEAF
    half = LANES // 2
    barrier = pltpu.get_barrier_semaphore()

    @pl.loop(1, devices)
    def _(i):
        pl.semaphore_signal(barrier, inc=1, device_id=(lax.rem(me + i, devices),), device_id_type=MESH)

    incoming = [pltpu.make_async_copy(a, b, io_sems.at[i]) for i, (a, b) in enumerate((
        (v_in, v_ref), (coords_in, coords_ref), (diag_in, diag_ref), (rows_in, rows_ref), (signs_in, signs_ref)))]
    for copy in incoming:
        copy.start()
    lane = lax.broadcasted_iota(jnp.int32, (8, LANES), 1)
    sub = lax.broadcasted_iota(jnp.int32, (8, LANES), 0)
    planes = 4
    plane_size = devices // planes
    plane, seat = me // plane_size, lax.rem(me, plane_size)
    halves = devices // 2
    side = plane // 2

    def facing(away):
        there = 0
        for b in range(planes.bit_length() - 1):
            bit = lax.rem(plane // 2 ** b, 2)
            there = there + 2 ** b * ((1 - bit) if (away >> b) & 1 else bit)
        return there

    def send(source, target, which, other):
        pltpu.make_async_remote_copy(
            source, target, sems.at[2 * which], sems.at[2 * which + 1],
            device_id=(other,), device_id_type=MESH).start()

    def to_all(source, target, which, aways):
        for away in aways:
            there = {3: (1 - side) * (planes - 1), 2: 2 - side, 1: facing(1), 0: plane}[away]

            @pl.loop(0 if away else 1, plane_size, unroll=True)
            def _(i):
                other = plane_size * there + lax.rem(seat + i, plane_size)
                send(source(other), target, which, other)

    def to_plane(source, target, which):
        @pl.loop(1, plane_size, unroll=True)
        def _(i):
            other = lax.rem(seat + i, plane_size)
            send(source(other), target, which, plane_size * plane + other)

    def to_planes(source, target, which):
        for away in range(planes - 1, 0, -1):
            send(source, target, which, plane_size * facing(away) + seat)

    def finish(ref, which, end):
        pltpu.make_async_copy(ref, ref, sems.at[2 * which + end]).wait()

    def columns_at(ref, tile):
        return ref.at[:, pl.ds(pl.multiple_of(tile * LANES, LANES), LANES)]

    others, mates, peers = pl.ds(0, devices - 1), pl.ds(0, plane_size - 1), pl.ds(0, planes - 1)
    side_rows = 5
    side_part = pl.ds(0, side_rows)

    for copy in incoming:
        copy.wait()
    rows_f, signs_f = rows_ref[...].astype(F32), signs_ref[...].astype(F32)
    for e in range(devices):
        here = slice(e * LANES, (e + 1) * LANES)
        small_send[e, 0:2, :] = coords_ref[:, here].astype(F32)
        small_send[e, 2:3, :] = diag_ref[e:e + 1, :]
        small_send[e, 3:4, :] = rows_f[e:e + 1, :]
        small_send[e, 4:5, :] = signs_f[e:e + 1, :]
    scale = lax.rem(scale_ref[0], MODULUS)
    spot = lane // LEAF
    inner_lane = (lane % LEAF).astype(F32)
    for k in range(sections):
        for g in range(devices // 8):
            ident = ((8 * g + sub) * LANES + per_tile * me + spot) * 37
            x = (ident + 101 * k).astype(F32)
            rest = x - jnp.floor(x * (1.0 / (MODULUS - 1))) * float(MODULUS - 1)
            rest = jnp.where(rest < 0.0, rest + float(MODULUS - 1), rest)
            rest = jnp.where(rest >= float(MODULUS - 1), rest - float(MODULUS - 1), rest)
            key = rest.astype(jnp.int32) + 1
            unit_phase = fold(fold(key * scale)).astype(F32)
            for m, second in enumerate((2.0, 1.0)):
                phi = remainder(unit_phase * (inner_lane + second))
                phases[2 * k + m, 8 * g:8 * g + 8, :] = phi
                steps[2 * k + m, 8 * g:8 * g + 8, :] = scaled_cos(8.0 * phi, 2.0)

    wide_sub = lax.broadcasted_iota(jnp.int32, (WIDTH, LANES), 0)
    wide_lane = lax.broadcasted_iota(jnp.int32, (WIDTH, LANES), 1)
    ident_part = jnp.where(wide_lane % WIDTH == wide_sub, 0.85, 0.0)
    sub_f = sub.astype(F32)
    def make_maps(begins, ends):
        for k in range(sections):
            maps_of(k, begins[k], ends[k])

    def maps_of(k, begin_pair, end_pair):
        stride = 2 ** k

        @pl.loop(begin_pair, end_pair)
        def _(pair):
            first_tile = (pair // stride) * (2 * stride) + pair % stride
            for bit in range(2):
                d = first_tile + stride * bit
                for m in range(2):
                    amplitude = (0.35 if m == 0 else 0.6) / math.sqrt(WIDTH)
                    first, offset = (1.0, 0.0) if m == 0 else (3.0, 4096.0)
                    phi = phases[2 * k + m, pl.ds(d, 1), :]
                    step = steps[2 * k + m, pl.ds(d, 1), :]
                    one = scaled_cos(phi * (sub_f + (8.0 + first)) + offset, amplitude)
                    two = scaled_cos(phi * (sub_f + (16.0 + first)) + offset, amplitude)
                    full = jnp.concatenate([step * one - two, one, two, step * two - one], axis=0)
                    if m == 0:
                        full = full + ident_part
                    top, low = split(full)
                    begin = LANES * (bit if m == 0 else 1 - bit)
                    mats[k, pair, 64 * bit:64 * bit + 32, begin:begin + LANES] = top
                    mats[k, pair, 64 * bit + 32:64 * bit + 64, begin:begin + LANES] = low

    hops = lax.rem(me // 2, 2) + lax.rem(me // 4, 2) + plane
    budget = 18 * (5 - hops) - 8
    early = [jnp.clip(budget - k * (devices // 2), 0, devices // 2) for k in range(sections)]
    make_maps([0] * sections, early)
    pl.semaphore_wait(barrier, devices - 1)
    for which, aways in ((0, (3, 2)), (7, (1, 0))):
        to_all(lambda d: small_send.at[d, side_part], small.at[me, side_part], which, aways)
    for which, aways in ((8, (1, 0)), (1, (3, 2))):
        to_all(lambda d: columns_at(v_ref, d), vals.at[me], which, aways)
    small[me] = small_send[me]
    vals[me] = columns_at(v_ref, me)[...]

    make_maps(early, [devices // 2] * sections)
    lanes_q = lax.broadcasted_iota(jnp.int32, (columns, LANES), 1)
    rows_q = lax.broadcasted_iota(jnp.int32, (columns, LANES), 0)

    def place(tile):
        return pl.ds(pl.multiple_of(tile * LANES, LANES), LANES)

    low_ids = lax.broadcasted_iota(jnp.int32, (LOW, LANES), 0).astype(F32).astype(BF16)
    high_ids = (lax.broadcasted_iota(jnp.int32, (HIGH * columns, LANES), 0) // columns).astype(F32).astype(BF16)
    one, nil = jnp.array(1.0, BF16), jnp.array(0.0, BF16)

    def make_hot(row_of, sign_of, begin, count):
        @pl.loop(0, count, unroll=2)
        def _(i):
            d = begin + i
            row = row_of(d)
            high = jnp.floor(row * (1.0 / LOW))
            low = jnp.broadcast_to((row - high * LOW).astype(BF16), (LOW, LANES))
            hot[:, place(d)] = jnp.where(low_ids == low, one, nil)
            flip = (1 - 2 * (d // halves)).astype(F32)
            sign = jnp.broadcast_to(((2.0 * sign_of(d) - 1.0) * flip).astype(BF16), (HIGH * columns, LANES))
            wide = jnp.broadcast_to(high.astype(BF16), (HIGH * columns, LANES))
            masks[d] = jnp.where(high_ids == wide, sign, nil)

    def place_values(d, at, value):
        top, rest = split(value)
        for g in range(HIGH):
            mask = masks[d, columns * g:columns * (g + 1), :]
            left[columns * g:columns * (g + 1), at] = top * mask
            left[columns * (HIGH + g):columns * (HIGH + g + 1), at] = rest * mask

    def sketch_product():
        points = left.shape[1] // 2
        o = [lax.dot_general(left[:, part], hot[:, part], (((1,), (1,)), ((), ())), preferred_element_type=F32)
             for part in (slice(0, points), slice(points, 2 * points))]
        return (o[0][:HIGH * columns] + o[0][HIGH * columns:]) - (o[1][:HIGH * columns] + o[1][HIGH * columns:])

    factor = math.sqrt(SKETCH / total_points)

    def start_reduce(sk, pieces, landed, which):
        for n in range(plane_size):
            pieces[n] = sk[columns * n:columns * (n + 1), :]
        to_plane(lambda n: pieces.at[n], landed.at[seat], which)
        landed[seat] = pieces[seat]

    def next_reduce(landed, total, joined, which, first):
        finish(landed.at[pl.ds(0, plane_size - 1)], first, 1)
        total[...] = jnp.sum(landed[...], axis=0)
        to_planes(total, joined.at[plane], which)
        joined[plane] = total[...]

    make_hot(lambda d: rows_ref[pl.ds(d, 1), :].astype(F32), lambda d: signs_ref[pl.ds(d, 1), :].astype(F32), 0, devices)

    @pl.loop(0, devices)
    def _(d):
        place_values(d, place(d), v_ref[:, place(d)])

    basis_sketch = sketch_product()
    start_reduce(basis_sketch, rb_send, rb_recv, 2)

    fx = (sub % 4 + 1).astype(F32)
    fy = (sub // 4 + 1).astype(F32)
    unit = 1.0 / math.sqrt(LEAF)
    point_masks = [jnp.where(lanes_q // LEAF == j, 1.0, 0.0).astype(BF16) for j in range(per_tile)]
    column_masks = [jnp.where((wide_lane % half) // columns == j, 1.0, 0.0).astype(BF16) for j in range(per_tile)]
    first_half = wide_lane < half

    def combine(o):
        s = o[0:32] + o[32:64]
        return s + pltpu.roll(s, half, 1)

    def expand(total):
        top = total.astype(BF16).astype(F32)
        y = jnp.where(first_half, top, total - top).astype(BF16)
        return jnp.concatenate([y * m for m in column_masks], axis=0)

    def leaves(begin):
        @pl.loop(0, halves, unroll=4)
        def _(i):
            d = begin + i
            pair = fold(small[d, 0:2, :].astype(jnp.int32) * scale).astype(F32)
            px, py = pair[0:1], pair[1:2]
            phases_of = [fx * px + (fy + 2.0 * t) * py for t in range(2)]
            full = jnp.concatenate([scaled_cos(n, unit) for n in phases_of] + [scaled_sin(n, unit) for n in phases_of], axis=0)
            top, low = split(full)
            leaf[d, 0:32] = top
            leaf[d, 32:64] = low

    def gather(begin):
        for i in range(halves):
            d = begin + i
            top, rest = split(vals[d])
            spread_v = jnp.concatenate([top * m for m in point_masks] + [rest * m for m in point_masks], axis=0)
            o = lax.dot_general(leaf[d], spread_v, (((1,), (1,)), ((), ())), preferred_element_type=F32)
            state[0, d] = expand(combine(o))

    def section(k, begin, count):
        stride = 2 ** k
        now = k % 2
        for i in range(count // 2):
            d0 = begin + (i // stride) * (2 * stride) + i % stride
            d1 = d0 + stride
            x = jnp.concatenate([state[now, d0], state[now, d1]], axis=0)
            o = jnp.dot(mats[k, begin // 2 + i], x, preferred_element_type=F32)
            for d, part in ((d0, o[0:64]), (d1, o[64:128])):
                total = combine(part)
                if k == sections - 1:
                    coef[32 * d:32 * d + 32, :] = total
                else:
                    state[1 - now, d] = expand(total)

    near, away = side * halves, (1 - side) * halves
    for begin, small_which, count in ((near, 7, halves - 1), (away, 0, halves)):
        finish(small.at[pl.ds(0, count), side_part], small_which, 1)
        leaves(begin)
        make_hot(lambda d: small[d, 3:4, :], lambda d: small[d, 4:5, :], begin, halves)
    for begin, vals_which, count in ((near, 8, halves - 1), (away, 1, halves)):
        arrived = pl.ds(0, count)
        finish(vals.at[arrived], vals_which, 1)
        gather(begin)
        for k in range(sections - 1):
            section(k, begin, halves)
    next_reduce(rb_recv, rb_total, rb_joined, 9, 2)
    section(sections - 1, 0, devices)
    tile_lane = lax.broadcasted_iota(jnp.int32, (half, 2 * LANES), 1)
    tile_masks = [jnp.where((tile_lane % LANES) // WIDTH == t, 1.0, 0.0).astype(BF16) for t in range(4)]
    zero = jnp.zeros((columns, LANES), F32)
    inner, square, energy = zero, zero, zero
    for g in range(devices // 4):
        flipped = coef[LANES * g:LANES * (g + 1), :].T
        top, rest = split(flipped[0:half])
        both = jnp.concatenate([top, rest], axis=1)
        lhs = jnp.concatenate([both * m for m in tile_masks], axis=0)
        tops = jnp.concatenate([leaf[4 * g + t, 0:32] for t in range(4)], axis=0)
        lows = jnp.concatenate([leaf[4 * g + t, 32:64] for t in range(4)], axis=0)
        right = jnp.concatenate([tops, lows], axis=1)
        o = jnp.dot(lhs, jnp.concatenate([right, right], axis=0), preferred_element_type=F32)
        o = o[:, 0:LANES] + o[:, LANES:2 * LANES]
        for t in range(4):
            d = 4 * g + t
            v = vals[d]
            img = jnp.broadcast_to(small[d, 2:3, :], (columns, LANES)) * v
            for j in range(per_tile):
                begin = half * t + columns * j
                img = img + jnp.where(lanes_q // LEAF == j, o[begin:begin + columns], 0.0)
            image[d] = img
            place_values(d, slice(LANES * d, LANES * (d + 1)), img)
            inner, square, energy = inner + v * img, square + v * v, energy + img * img

    to_all(lambda d: image.at[d], back.at[me], 5, (3, 2, 1, 0))
    packed = zero
    for i, value in enumerate((inner, square, energy)):
        packed = jnp.where(lanes_q == rows_q + columns * i, jnp.sum(value, axis=1, keepdims=True), packed)
    sum_send[...] = jnp.sum(packed, axis=0, keepdims=True)
    image_sketch = sketch_product()
    start_reduce(image_sketch, ri_send, ri_recv, 4)
    to_plane(lambda d: sum_send, sum_recv.at[seat], 3)
    sum_recv[seat] = sum_send[...]
    back[me] = image[me]

    finish(small_send.at[pl.ds(0, halves), side_part], 0, 0)
    finish(small_send.at[pl.ds(0, halves - 1), side_part], 7, 0)
    finish(vals.at[pl.ds(0, halves)], 1, 0)
    finish(vals.at[pl.ds(0, halves - 1)], 8, 0)
    finish(rb_send.at[mates], 2, 0)
    next_reduce(ri_recv, ri_total, ri_joined, 11, 4)
    finish(sum_recv.at[mates], 3, 1)
    sum_total[...] = jnp.sum(sum_recv[...], axis=0)
    to_planes(sum_total, sum_joined.at[plane], 10)
    sum_joined[plane] = sum_total[...]
    finish(rb_joined.at[peers], 9, 0)
    finish(rb_joined.at[peers], 9, 1)
    finish(sum_recv.at[mates], 3, 0)
    finish(ri_send.at[mates], 4, 0)
    basis_total = jnp.sum(rb_joined[...], axis=0)
    finish(sum_joined.at[peers], 10, 1)
    totals = jnp.sum(sum_joined[...], axis=0)

    def column(i):
        picked = jnp.where(lanes_q == rows_q + columns * i, jnp.broadcast_to(totals, (columns, LANES)), 0.0)
        return jnp.broadcast_to(jnp.sum(picked, axis=1, keepdims=True) * (1.0 / total_points), (columns, LANES))

    inner_mean, square_mean, energy_mean = column(0), column(1), column(2)
    projection = inner_mean / (square_mean + EPSILON)
    energy = energy_mean - 2.0 * projection * inner_mean + projection * projection * square_mean
    spread = jnp.sqrt(energy + EPSILON)
    inverse = 1.0 / spread
    for i, value in enumerate((projection, spread)):
        arn_ref[i:i + 1, :] = jnp.sum(jnp.where(lanes_q == rows_q, value, 0.0), axis=0, keepdims=True)[:, :columns]
    finish(ri_joined.at[peers], 11, 1)
    wide = lambda x: jnp.concatenate([x] * (LOW // LANES), axis=1)
    own_chunk[...] = (jnp.sum(ri_joined[...], axis=0) - basis_total * wide(projection)) * wide(factor * inverse)
    to_plane(lambda d: own_chunk, ag_recv.at[seat], 6)
    ag_recv[seat] = own_chunk[...]
    finish(back.at[others], 5, 1)
    for e in range(devices):
        here = slice(e * LANES, (e + 1) * LANES)
        nb_ref[:, here] = (back[e] - projection * v_ref[:, here]) * inverse
    finish(image.at[others], 5, 0)
    finish(ri_joined.at[peers], 11, 0)
    finish(sum_joined.at[peers], 10, 0)
    finish(ag_recv.at[mates], 6, 0)
    finish(ag_recv.at[mates], 6, 1)
    for n in range(plane_size):
        sketch_ref[:, LOW * n:LOW * (n + 1)] = ag_recv[n]


def deliver(*refs):
    copies = [pltpu.make_async_copy(refs[i], refs[3 + i], refs[6].at[i]) for i in range(3)]
    for copy in copies:
        copy.start()
    for copy in copies:
        copy.wait()


def together(devices, basis_vector, diagonal, coords, phase_scale, sketch_rows, sketch_signs):
    columns, local_points = basis_vector.shape
    sections = devices.bit_length() - 1
    plane = (local_points // LANES, LANES)
    far = pl.BlockSpec(memory_space=pltpu.HBM)
    vmem = pl.BlockSpec(memory_space=pltpu.VMEM)
    tile = pltpu.VMEM((devices, columns, LANES), F32)
    chunk = (columns, LOW)
    pieces = pltpu.VMEM((HIGH,) + chunk, F32)
    reduce_parts = [pieces, pieces, pltpu.VMEM(chunk, F32), pltpu.VMEM((devices // HIGH,) + chunk, F32)]
    results = pl.pallas_call(
        functools.partial(tile_kernel, devices, local_points * devices),
        out_shape=(
            jax.ShapeDtypeStruct((columns, local_points), F32),
            jax.ShapeDtypeStruct((columns, SKETCH), F32),
            jax.ShapeDtypeStruct((2, columns), F32)),
        in_specs=[pl.BlockSpec(memory_space=pltpu.SMEM)] + [far] * 5,
        out_specs=(vmem,) * 3,
        scratch_shapes=[
            pltpu.VMEM(basis_vector.shape, F32),
            pltpu.VMEM(coords.shape, jnp.int32),
            pltpu.VMEM(plane, F32),
            pltpu.VMEM(plane, jnp.int32),
            pltpu.VMEM(plane, jnp.int32),
            pltpu.VMEM((devices, 8, LANES), F32),
            pltpu.VMEM((devices, 8, LANES), F32),
            tile,
            pltpu.VMEM((2 * sections, devices, LANES), F32),
            pltpu.VMEM((2 * sections, devices, LANES), F32),
            pltpu.VMEM((sections, devices // 2, 4 * WIDTH, 2 * LANES), BF16),
            pltpu.VMEM((devices, 2 * WIDTH, LANES), BF16),
            pltpu.VMEM((2, devices, LANES, LANES), BF16),
            pltpu.VMEM((devices * WIDTH, LANES), F32),
            tile, tile,
            pltpu.VMEM((LOW, local_points), BF16),
            pltpu.VMEM((2 * HIGH * columns, local_points), BF16),
            pltpu.VMEM((devices, HIGH * columns, LANES), BF16),
            pltpu.VMEM((1, LANES), F32),
            pltpu.VMEM((HIGH, 1, LANES), F32),
            pltpu.VMEM((1, LANES), F32),
            pltpu.VMEM((devices // HIGH, 1, LANES), F32),
            *reduce_parts, *reduce_parts, pieces,
            pltpu.VMEM(chunk, F32),
            pltpu.SemaphoreType.DMA((24,)),
            pltpu.SemaphoreType.DMA((5,)),
        ],
        compiler_params=pltpu.CompilerParams(
            collective_id=0, has_side_effects=True, vmem_limit_bytes=24 * 2**20),
        name="gmres",
    )(phase_scale, *(pltpu.with_memory_space_constraint(x, pltpu.HBM) for x in (
        basis_vector, coords, diagonal.reshape(plane), sketch_rows.reshape(plane),
        sketch_signs.reshape(plane))))
    return pl.pallas_call(
        deliver,
        out_shape=[jax.ShapeDtypeStruct(x.shape, x.dtype) for x in results],
        in_specs=[vmem] * 3,
        out_specs=[far] * 3,
        scratch_shapes=[pltpu.SemaphoreType.DMA((3,))],
        compiler_params=pltpu.CompilerParams(vmem_limit_bytes=2**20),
        name="deliver",
    )(*results)


def body(basis_vector, diagonal, coords, phase_scale, sketch_rows, sketch_signs):
    columns, local_points = basis_vector.shape
    devices = lax.axis_size("box")
    if devices * LANES == local_points:
        return together(devices, basis_vector, diagonal, coords, phase_scale, sketch_rows, sketch_signs)
    sections = devices.bit_length() - 1
    count = -(-sections // 5)
    stages, low = [], 0
    for i in range(count):
        bits = (sections - low) // (count - i)
        stages.append((low, bits))
        low += bits
    group = 2 ** max(bits for _, bits in stages)
    group_rows = [columns * WIDTH // LANES * (LANES // 2 ** bits) for _, bits in stages]
    plane = (local_points // LANES, LANES)
    rows_each = HIGH * columns * LOW // LANES // devices
    vmem = pl.BlockSpec(memory_space=pltpu.VMEM)
    dma = pltpu.SemaphoreType.DMA
    count_rows = max(group_rows)
    halves = columns // 8
    new_basis, sketch, arn = pl.pallas_call(
        functools.partial(kernel, devices, stages, local_points * devices),
        out_shape=(
            jax.ShapeDtypeStruct((columns, local_points), F32),
            jax.ShapeDtypeStruct((columns, SKETCH), F32),
            jax.ShapeDtypeStruct((2, columns), F32)),
        in_specs=[pl.BlockSpec(memory_space=pltpu.SMEM), vmem, vmem, vmem, vmem, vmem],
        out_specs=(vmem, vmem, vmem),
        scratch_shapes=[
            pltpu.VMEM(((columns + 8) * LEAF, LANES), F32),
            pltpu.VMEM((columns + 8, LEAF, LANES), F32),
            pltpu.VMEM((LEAF, WIDTH, LANES), F32),
            pltpu.VMEM((2 * sections, WIDTH, WIDTH, LANES), F32),
            pltpu.VMEM((LEAF, columns, LANES), F32),
            pltpu.VMEM((columns * WIDTH, LANES), F32),
            pltpu.VMEM((columns * WIDTH, LANES), F32),
            pltpu.VMEM((columns * WIDTH // LANES, LANES, LANES), F32),
            pltpu.VMEM((2, LEAF, LANES), F32),
            pltpu.VMEM((LEAF // 4, LOW, 4 * LANES), BF16),
            pltpu.VMEM((2 * HIGH * columns, LOW), F32),
            pltpu.VMEM((2 * HIGH * columns, LOW), F32),
            pltpu.VMEM((count * halves, group, count_rows // halves, LANES), F32),
            pltpu.VMEM((count * halves, group, count_rows // halves, LANES), F32),
            pltpu.VMEM((count * halves, group, count_rows // halves, LANES), F32),
            pltpu.VMEM((count * halves, group, count_rows // halves, LANES), F32),
            pltpu.VMEM((1, LANES), F32),
            pltpu.VMEM((devices, 1, LANES), F32),
            pltpu.VMEM((devices, rows_each, LANES), F32),
            pltpu.VMEM((devices, rows_each, LANES), F32),
            pltpu.VMEM((devices, rows_each, LANES), F32),
            pltpu.VMEM((rows_each, LANES), F32),
            dma((count * halves, group)), dma((count * halves, group)), dma((count * halves, group)), dma((count * halves, group)),
            dma((devices,)), dma((devices,)), dma((devices,)), dma((devices,)), dma((devices,)), dma((devices,)),
        ],
        compiler_params=pltpu.CompilerParams(
            collective_id=0, has_side_effects=True, vmem_limit_bytes=60 * 2**20),
        name="gmres",
    )(phase_scale, basis_vector, coords, diagonal.reshape(plane), sketch_rows.reshape(plane),
      sketch_signs.reshape(plane))
    return new_basis, sketch, arn


def solution(mesh):
    placed = (P(None, "box"), P("box"), P(None, "box"), P(), P("box"), P("box"))
    return jax.shard_map(
        body, mesh=mesh, in_specs=placed, out_specs=(P(None, "box"), P(), P()), check_vma=False
    )
```

```python
import functools
import math

import jax
import jax.numpy as jnp
import numpy as np
from jax import lax
from jax.experimental import pallas as pl
from jax.experimental.pallas import tpu as pltpu
from jax.sharding import PartitionSpec as P

WIDTH = 32
LEAF = 32
SKETCH = 2048
LANES = 128
HIGH = 8
LOW = SKETCH // HIGH
MODULUS = 8191
EPSILON = 1e-06
MESH = pl.DeviceIdType.MESH
F32 = jnp.float32
BF16 = jnp.bfloat16


def sine_series():
    node = np.cos((np.arange(400) + 0.5) * np.pi / 800)
    basis = np.stack([node ** (2 * i) for i in range(6)], 1)
    exact = np.sin(np.pi * node * 4096 / MODULUS) / node
    return np.linalg.lstsq(basis, exact, rcond=None)[0]


SERIES = sine_series()


def remainder(n):
    return n - jnp.floor(n * (1.0 / MODULUS) + 0.5) * float(MODULUS)


def half_sine(n, gain):
    t = remainder(n) * (1.0 / 4096)
    z = t * t
    total = z * float(SERIES[5] * gain) + float(SERIES[4] * gain)
    for c in SERIES[3::-1]:
        total = total * z + float(c * gain)
    return total * t


def scaled_cos(n, amplitude):
    s = half_sine(n, math.sqrt(2.0 * amplitude))
    return amplitude - s * s


def scaled_sin(n, amplitude):
    return scaled_cos(n - 0.25 * MODULUS, amplitude)


def fold(p):
    return (p & MODULUS) + lax.shift_right_logical(p, 13)


def kernel(devices, stages, total_points, scale_ref, v_ref, coords_ref, diag_ref, rows_ref, signs_ref,
           nb_ref, sketch_ref, arn_ref, raw, pts, leaf, mats, kk, cbuf, part, tbuf, work, onehot, skb, ski,
           a_send, a_recv, b_send, b_recv, sum_send, sum_recv, rs_send, rs_recv, ag_recv, own_chunk,
           a_ss, a_rs, b_ss, b_rs, s_ss, s_rs, r_ss, r_rs, g_ss, g_rs):
    me = lax.axis_index("box")
    columns = nb_ref.shape[0]
    halves = columns // 8
    barrier = pltpu.get_barrier_semaphore()

    @pl.loop(1, devices)
    def _(i):
        pl.semaphore_signal(barrier, inc=1, device_id=(lax.rem(me + i, devices),), device_id_type=MESH)

    lane = lax.broadcasted_iota(jnp.int32, (8, LANES), 1)
    sub = lax.broadcasted_iota(jnp.int32, (8, LANES), 0)
    scale = lax.rem(scale_ref[0], MODULUS)

    for r in range(LANES // 4):
        here = slice(LANES * r, LANES * (r + 1))
        for h in range(halves):
            raw[pl.ds(256 * h + r, 8, stride=32), :] = v_ref[8 * h:8 * h + 8, here]
        pair = coords_ref[:, here].astype(F32)
        raw[columns * 32 + r:columns * 32 + r + 1, :] = pair[0:1]
        raw[columns * 32 + 32 + r:columns * 32 + 33 + r, :] = pair[1:2]
    raw[(columns + 2) * 32:(columns + 3) * 32, :] = diag_ref[...]
    raw[(columns + 3) * 32:(columns + 4) * 32, :] = rows_ref[...].astype(F32)
    raw[(columns + 4) * 32:(columns + 5) * 32, :] = signs_ref[...].astype(F32)
    raw[(columns + 5) * 32:(columns + 8) * 32, :] = jnp.zeros((96, LANES), F32)
    for i in range((columns + 8) // 4):
        flipped = raw[LANES * i:LANES * (i + 1), :].T
        tbuf[0] = flipped
        for j in range(4):
            pts[4 * i + j] = jnp.concatenate(
                [tbuf[0, 32 * g:32 * g + 32, 32 * j:32 * j + 32] for g in range(4)], axis=1)

    def exact_phase(row):
        return fold(pts[columns + row].astype(jnp.int32) * scale).astype(F32)

    work[0] = exact_phase(0)
    work[1] = exact_phase(1)
    fx = (sub % 4 + 1).astype(F32)
    fy = (sub // 4 + 1).astype(F32)
    unit = 1.0 / math.sqrt(LEAF)

    @pl.loop(0, LEAF)
    def _(s):
        px = work[0, pl.ds(s, 1), :]
        py = work[1, pl.ds(s, 1), :]
        for tile in range(2):
            n = fx * px + (fy + 2.0 * tile) * py
            leaf[s, 8 * tile:8 * tile + 8] = scaled_cos(n, unit)
            leaf[s, 16 + 8 * tile:24 + 8 * tile] = scaled_sin(n, unit)

    def gather_half(h):
        def gather(s, acc):
            tiles = [leaf[s, 8 * t:8 * t + 8] for t in range(4)]
            out = []
            for q in range(8):
                row = pts[8 * h + q, pl.ds(s, 1), :]
                for t in range(4):
                    out.append(acc[4 * q + t] + tiles[t] * row)
            return tuple(out)

        acc = lax.fori_loop(0, LEAF, gather, tuple(jnp.zeros((8, LANES), F32) for _ in range(32)), unroll=2)
        for q in range(8):
            for t in range(4):
                cbuf[pl.ds((8 * h + q) * 32 + 8 * t, 8), :] = acc[4 * q + t]

    blocks = 8 * WIDTH // LANES

    def make_maps(low, bits):
        group = 2 ** bits
        places = LANES // group
        mine = lax.rem(me // 2 ** low, group)
        spot = mine * places + lane % places
        box = 4 * (spot % 32) + spot // 32
        member = me + (lane // places - mine) * 2 ** low
        ident = (member * LANES + box) * 37

        @pl.loop(low, low + bits)
        def _(k):
            x = (ident + 101 * k).astype(F32)
            rest = x - jnp.floor(x * (1.0 / (MODULUS - 1))) * float(MODULUS - 1)
            rest = jnp.where(rest < 0.0, rest + float(MODULUS - 1), rest)
            rest = jnp.where(rest >= float(MODULUS - 1), rest - float(MODULUS - 1), rest)
            key = rest.astype(jnp.int32) + 1
            unit_phase = fold(fold(key * scale)).astype(F32)
            wide = sub.astype(F32)
            for m in range(2):
                amplitude = (0.35 if m == 0 else 0.6) / math.sqrt(WIDTH)
                first, second, offset = (1.0, 2.0, 0.0) if m == 0 else (3.0, 1.0, 4096.0)
                mid = unit_phase * (wide + (8.0 + first))
                far = unit_phase * (wide + (16.0 + first))

                @pl.loop(0, WIDTH, unroll=2)
                def _(v):
                    times = v.astype(F32) + second
                    step = scaled_cos(unit_phase * (8.0 * times), 2.0)
                    one = scaled_cos(mid * times + offset, amplitude)
                    two = scaled_cos(far * times + offset, amplitude)
                    mats[2 * k + m, v, 8:16] = one
                    mats[2 * k + m, v, 16:24] = two
                    mats[2 * k + m, v, 0:8] = step * one - two
                    mats[2 * k + m, v, 24:32] = step * two - one

    def exchange(send, recv, ss, rs, low, bits, action):
        group = 2 ** bits
        mine = lax.rem(me // 2 ** low, group)

        @pl.loop(1, group)
        def _(i):
            other = lax.rem(mine + i, group)
            here = other if action is finish_recv else mine
            copy = pltpu.make_async_remote_copy(
                send.at[other], recv.at[here], ss.at[other], rs.at[here],
                device_id=(me + (other - mine) * 2 ** low,), device_id_type=MESH)
            action(copy)
        return mine

    def pack(send, group, h):
        places = LANES // group
        for j in range(blocks):
            at = LANES * (blocks * h + j)
            tbuf[j] = cbuf[at:at + LANES, :].T
        for d in range(group):
            for j in range(blocks):
                send[d, places * j:places * (j + 1), :] = tbuf[j, places * d:places * (d + 1), :]

    def unpack(recv, group, h):
        places = LANES // group
        for j in range(blocks):
            for d in range(group):
                tbuf[j, places * d:places * (d + 1), :] = recv[d, places * j:places * (j + 1), :]
        for j in range(blocks):
            at = LANES * (blocks * h + j)
            cbuf[at:at + LANES, :] = tbuf[j].T

    def sketch_of(values, target, make):
        target[...] = jnp.zeros_like(target)

        @pl.loop(0, LEAF // 4)
        def _(c):
            pieces = []
            for i in range(4):
                s = 4 * c + i
                row = pts[columns + 3, pl.ds(s, 1), :]
                high = jnp.floor(row * (1.0 / LOW))
                if make:
                    low = (row - high * LOW).astype(jnp.int32)
                    ids = lax.broadcasted_iota(jnp.int32, (LOW, LANES), 0)
                    onehot[c, :, LANES * i:LANES * (i + 1)] = jnp.where(ids == low, 1.0, 0.0).astype(BF16)
                sign = 2.0 * pts[columns + 4, pl.ds(s, 1), :] - 1.0
                v = values(s) * sign
                top = v.astype(BF16)
                rest = (v - top.astype(F32)).astype(BF16)
                wide = jnp.broadcast_to(high, (columns, LANES))
                masks = [jnp.where(wide == float(g), 1.0, 0.0).astype(BF16) for g in range(HIGH)]
                pieces.append(jnp.concatenate([top * g for g in masks] + [rest * g for g in masks], axis=0))
            left = jnp.concatenate(pieces, axis=1)
            target[...] += lax.dot_general(left, onehot[c], (((1,), (1,)), ((), ())), preferred_element_type=F32)

    nbt = kk

    def start(copy):
        copy.start()

    def finish_recv(copy):
        copy.wait_recv()

    def finish_send(copy):
        copy.wait_send()

    for index, (low, bits) in enumerate(stages):
        group = 2 ** bits
        places = LANES // group

        def outward(h, action):
            at = halves * index + h
            return exchange(a_send.at[at], a_recv.at[at], a_ss.at[at], a_rs.at[at], low, bits, action)

        def homeward(h, action):
            at = halves * index + h
            return exchange(b_send.at[at], b_recv.at[at], b_ss.at[at], b_rs.at[at], low, bits, action)

        for h in range(halves):
            at = halves * index + h
            if index == 0:
                gather_half(h)
            pack(a_send.at[at], group, h)
            if index == 0 and h == 0:
                pl.semaphore_wait(barrier, devices - 1)
            mine = outward(h, start)
            a_recv[at, mine] = a_send[at, mine]
        make_maps(low, bits)
        if index == 0:
            for q in range(columns):
                for s in range(LEAF):
                    nbt[s, q:q + 1, :] = pts[q, s:s + 1, :]
            sketch_of(lambda s: nbt[s], skb, True)
        for h in range(halves):
            at = halves * index + h
            outward(h, finish_recv)
            unpack(a_recv.at[at], group, h)
            half = slice(256 * h, 256 * (h + 1))
            for k in range(low, low + bits):
                span = places * 2 ** (k - low)
                full = cbuf[half, :]
                wide = lax.broadcasted_iota(jnp.int32, full.shape, 1)
                part[half, :] = jnp.where((wide // span) % 2 == 0,
                                          pltpu.roll(full, LANES - span, 1), pltpu.roll(full, span, 1))

                def mix(v, acc):
                    own = [mats[2 * k, v, 8 * t:8 * t + 8] for t in range(4)]
                    cross = [mats[2 * k + 1, v, 8 * t:8 * t + 8] for t in range(4)]
                    out = []
                    for q in range(8):
                        row = cbuf[pl.ds((8 * h + q) * 32 + v, 1), :]
                        other = part[pl.ds((8 * h + q) * 32 + v, 1), :]
                        for t in range(4):
                            out.append(acc[4 * q + t] + own[t] * row + cross[t] * other)
                    return tuple(out)

                init = tuple(0.85 * cbuf[pl.ds((8 * h + q) * 32 + 8 * t, 8), :] for q in range(8) for t in range(4))
                acc = lax.fori_loop(0, WIDTH, mix, init, unroll=2)
                for q in range(8):
                    for t in range(4):
                        cbuf[pl.ds((8 * h + q) * 32 + 8 * t, 8), :] = acc[4 * q + t]
            pack(b_send.at[at], group, h)
            mine = homeward(h, start)
            b_recv[at, mine] = b_send[at, mine]
        for h in range(halves):
            outward(h, finish_send)
        for h in range(halves):
            homeward(h, finish_recv)
            unpack(b_recv.at[halves * index + h], group, h)
        for h in range(halves):
            homeward(h, finish_send)

    for c in range(LEAF // 8):
        def spread_out(w, acc):
            coef = [cbuf[pl.ds(8 * h * 32 + w, 8, stride=32), :] for h in range(halves)]
            out = []
            for s in range(8):
                row = leaf[8 * c + s, pl.ds(w, 1), :]
                for h in range(halves):
                    out.append(acc[halves * s + h] + coef[h] * row)
            return tuple(out)

        init = tuple(
            jnp.broadcast_to(pts[columns + 2, 8 * c + s:8 * c + s + 1, :], (8, LANES)) * nbt[8 * c + s, 8 * h:8 * h + 8]
            for s in range(8) for h in range(halves))
        acc = lax.fori_loop(0, WIDTH, spread_out, init, unroll=2)
        for s in range(8):
            for h in range(halves):
                part[(8 * c + s) * columns + 8 * h:(8 * c + s) * columns + 8 * h + 8, :] = acc[halves * s + h]

    inner = jnp.zeros((columns, LANES), F32)
    square, energy = inner, inner
    for s in range(LEAF):
        v, image = nbt[s], part[s * columns:(s + 1) * columns, :]
        inner, square, energy = inner + v * image, square + v * v, energy + image * image
    lane_q = lax.broadcasted_iota(jnp.int32, (columns, LANES), 1)
    row_q = lax.broadcasted_iota(jnp.int32, (columns, LANES), 0)
    packed = jnp.zeros((columns, LANES), F32)
    for i, value in enumerate((inner, square, energy)):
        packed = jnp.where(lane_q == row_q + columns * i, jnp.sum(value, axis=1, keepdims=True), packed)
    sum_send[...] = jnp.sum(packed, axis=0, keepdims=True)

    def to_all(source, recv, ss, rs, action):
        @pl.loop(1, devices)
        def _(i):
            other = lax.rem(me + i, devices)
            here = other if action is finish_recv else me
            action(pltpu.make_async_remote_copy(
                source(other), recv.at[here], ss.at[other], rs.at[here],
                device_id=(other,), device_id_type=MESH))

    to_all(lambda d: sum_send, sum_recv, s_ss, s_rs, start)
    sum_recv[me] = sum_send[...]
    sketch_of(lambda s: part[pl.ds(pl.multiple_of(s * columns, columns), columns), :], ski, False)
    to_all(lambda d: sum_send, sum_recv, s_ss, s_rs, finish_recv)
    totals = jnp.sum(sum_recv[...], axis=0)

    def column(i):
        picked = jnp.where(lane_q == row_q + columns * i, jnp.broadcast_to(totals, (columns, LANES)), 0.0)
        return jnp.broadcast_to(jnp.sum(picked, axis=1, keepdims=True) * (1.0 / total_points), (columns, LANES))

    inner_mean, square_mean, energy_mean = column(0), column(1), column(2)
    projection = inner_mean / (square_mean + EPSILON)
    energy = energy_mean - 2.0 * projection * inner_mean + projection * projection * square_mean
    spread = jnp.sqrt(energy + EPSILON)
    inverse = 1.0 / spread
    for i, value in enumerate((projection, spread)):
        arn_ref[i:i + 1, :] = jnp.sum(jnp.where(lane_q == row_q, value, 0.0), axis=0, keepdims=True)[:, :columns]

    rows_each = rs_send.shape[1]
    factor = math.sqrt(SKETCH / total_points)
    lowest = HIGH * columns
    part_tiles = LOW // LANES
    for n in range(devices):
        flat = n * rows_each
        tile, row = flat // 8, flat % 8
        strip, side = tile // part_tiles, tile % part_tiles
        top = strip * 8 + row
        q0 = top % columns
        cols = slice(side * LANES, (side + 1) * LANES)
        img = ski[top:top + rows_each, cols] + ski[lowest + top:lowest + top + rows_each, cols]
        bas = skb[top:top + rows_each, cols] + skb[lowest + top:lowest + top + rows_each, cols]
        rs_send[n] = (img - projection[q0:q0 + rows_each] * bas) * (factor * inverse[q0:q0 + rows_each])
    to_all(lambda d: rs_send.at[d], rs_recv, r_ss, r_rs, start)
    rs_recv[me] = rs_send[me]

    for s in range(LEAF):
        pts_rows = (part[s * columns:(s + 1) * columns, :] - projection * nbt[s]) * inverse
        nbt[s] = pts_rows
    for q in range(columns):
        for s in range(LEAF):
            pts[q, s:s + 1, :] = nbt[s, q:q + 1, :]
    for i in range(columns // 4):
        for j in range(4):
            for g in range(4):
                tbuf[0, 32 * g:32 * g + 32, 32 * j:32 * j + 32] = pts[4 * i + j, :, 32 * g:32 * g + 32]
        raw[LANES * i:LANES * (i + 1), :] = tbuf[0].T
    for r in range(LANES // 4):
        for h in range(halves):
            nb_ref[8 * h:8 * h + 8, LANES * r:LANES * (r + 1)] = raw[pl.ds(256 * h + r, 8, stride=32), :]

    to_all(lambda d: rs_send.at[d], rs_recv, r_ss, r_rs, finish_recv)
    own_chunk[...] = jnp.sum(rs_recv[...], axis=0)
    to_all(lambda d: own_chunk, ag_recv, g_ss, g_rs, start)
    ag_recv[me] = own_chunk[...]
    to_all(lambda d: sum_send, sum_recv, s_ss, s_rs, finish_send)
    to_all(lambda d: rs_send.at[d], rs_recv, r_ss, r_rs, finish_send)
    to_all(lambda d: own_chunk, ag_recv, g_ss, g_rs, finish_recv)
    for n in range(devices):
        flat = n * rows_each
        tile, row = flat // 8, flat % 8
        strip, side = tile // part_tiles, tile % part_tiles
        top = strip * 8 + row
        q0, high = top % columns, top // columns
        begin = high * LOW + side * LANES
        sketch_ref[q0:q0 + rows_each, begin:begin + LANES] = ag_recv[n]
    to_all(lambda d: own_chunk, ag_recv, g_ss, g_rs, finish_send)


def split(x):
    top = x.astype(BF16)
    return top, (x - top.astype(F32)).astype(BF16)


def tile_kernel(devices, total_points, scale_ref, v_in, coords_in, diag_in, rows_in, signs_in,
                nb_ref, sketch_ref, arn_ref, v_ref, coords_ref, diag_ref, rows_ref, signs_ref,
                small_send, small, vals, phases, steps, mats, leaf, state, coef,
                image, back, hot, left, masks, sum_send, sum_recv, sum_total, sum_joined, rb_send,
                rb_recv, rb_total, rb_joined, ri_send, ri_recv, ri_total, ri_joined, ag_recv, own_chunk, sems,
                io_sems):
    me = lax.axis_index("box")
    columns = nb_ref.shape[0]
    sections = devices.bit_length() - 1
    per_tile = LANES // LEAF
    half = LANES // 2
    barrier = pltpu.get_barrier_semaphore()

    @pl.loop(1, devices)
    def _(i):
        pl.semaphore_signal(barrier, inc=1, device_id=(lax.rem(me + i, devices),), device_id_type=MESH)

    incoming = [pltpu.make_async_copy(a, b, io_sems.at[i]) for i, (a, b) in enumerate((
        (v_in, v_ref), (coords_in, coords_ref), (diag_in, diag_ref), (rows_in, rows_ref), (signs_in, signs_ref)))]
    for copy in incoming:
        copy.start()
    lane = lax.broadcasted_iota(jnp.int32, (8, LANES), 1)
    sub = lax.broadcasted_iota(jnp.int32, (8, LANES), 0)
    planes = 4
    plane_size = devices // planes
    plane, seat = me // plane_size, lax.rem(me, plane_size)
    halves = devices // 2
    side = plane // 2

    def facing(away):
        there = 0
        for b in range(planes.bit_length() - 1):
            bit = lax.rem(plane // 2 ** b, 2)
            there = there + 2 ** b * ((1 - bit) if (away >> b) & 1 else bit)
        return there

    def send(source, target, which, other):
        pltpu.make_async_remote_copy(
            source, target, sems.at[2 * which], sems.at[2 * which + 1],
            device_id=(other,), device_id_type=MESH).start()

    def to_all(source, target, which, aways):
        for away in aways:
            there = {3: (1 - side) * (planes - 1), 2: 2 - side, 1: facing(1), 0: plane}[away]

            @pl.loop(0 if away else 1, plane_size)
            def _(i):
                other = plane_size * there + lax.rem(seat + i, plane_size)
                send(source(other), target, which, other)

    def to_plane(source, target, which):
        @pl.loop(1, plane_size)
        def _(i):
            other = lax.rem(seat + i, plane_size)
            send(source(other), target, which, plane_size * plane + other)

    def to_planes(source, target, which):
        for away in range(planes - 1, 0, -1):
            send(source, target, which, plane_size * facing(away) + seat)

    def finish(ref, which, end):
        pltpu.make_async_copy(ref, ref, sems.at[2 * which + end]).wait()

    def columns_at(ref, tile):
        return ref.at[:, pl.ds(pl.multiple_of(tile * LANES, LANES), LANES)]

    others, mates, peers = pl.ds(0, devices - 1), pl.ds(0, plane_size - 1), pl.ds(0, planes - 1)
    side_rows = 5
    side_part = pl.ds(0, side_rows)

    for copy in incoming:
        copy.wait()
    rows_f, signs_f = rows_ref[...].astype(F32), signs_ref[...].astype(F32)
    for e in range(devices):
        here = slice(e * LANES, (e + 1) * LANES)
        small_send[e, 0:2, :] = coords_ref[:, here].astype(F32)
        small_send[e, 2:3, :] = diag_ref[e:e + 1, :]
        small_send[e, 3:4, :] = rows_f[e:e + 1, :]
        small_send[e, 4:5, :] = signs_f[e:e + 1, :]
    scale = lax.rem(scale_ref[0], MODULUS)
    spot = lane // LEAF
    inner_lane = (lane % LEAF).astype(F32)
    for k in range(sections):
        for g in range(devices // 8):
            ident = ((8 * g + sub) * LANES + per_tile * me + spot) * 37
            x = (ident + 101 * k).astype(F32)
            rest = x - jnp.floor(x * (1.0 / (MODULUS - 1))) * float(MODULUS - 1)
            rest = jnp.where(rest < 0.0, rest + float(MODULUS - 1), rest)
            rest = jnp.where(rest >= float(MODULUS - 1), rest - float(MODULUS - 1), rest)
            key = rest.astype(jnp.int32) + 1
            unit_phase = fold(fold(key * scale)).astype(F32)
            for m, second in enumerate((2.0, 1.0)):
                phi = remainder(unit_phase * (inner_lane + second))
                phases[2 * k + m, 8 * g:8 * g + 8, :] = phi
                steps[2 * k + m, 8 * g:8 * g + 8, :] = scaled_cos(8.0 * phi, 2.0)

    wide_sub = lax.broadcasted_iota(jnp.int32, (WIDTH, LANES), 0)
    wide_lane = lax.broadcasted_iota(jnp.int32, (WIDTH, LANES), 1)
    ident_part = jnp.where(wide_lane % WIDTH == wide_sub, 0.85, 0.0)
    sub_f = sub.astype(F32)
    def make_maps(begins, ends):
        for k in range(sections):
            maps_of(k, begins[k], ends[k])

    def maps_of(k, begin_pair, end_pair):
        stride = 2 ** k

        @pl.loop(begin_pair, end_pair)
        def _(pair):
            first_tile = (pair // stride) * (2 * stride) + pair % stride
            for bit in range(2):
                d = first_tile + stride * bit
                for m in range(2):
                    amplitude = (0.35 if m == 0 else 0.6) / math.sqrt(WIDTH)
                    first, offset = (1.0, 0.0) if m == 0 else (3.0, 4096.0)
                    phi = phases[2 * k + m, pl.ds(d, 1), :]
                    step = steps[2 * k + m, pl.ds(d, 1), :]
                    one = scaled_cos(phi * (sub_f + (8.0 + first)) + offset, amplitude)
                    two = scaled_cos(phi * (sub_f + (16.0 + first)) + offset, amplitude)
                    full = jnp.concatenate([step * one - two, one, two, step * two - one], axis=0)
                    if m == 0:
                        full = full + ident_part
                    top, low = split(full)
                    begin = LANES * (bit if m == 0 else 1 - bit)
                    mats[k, pair, 64 * bit:64 * bit + 32, begin:begin + LANES] = top
                    mats[k, pair, 64 * bit + 32:64 * bit + 64, begin:begin + LANES] = low

    hops = lax.rem(me // 2, 2) + lax.rem(me // 4, 2) + plane
    budget = 18 * (5 - hops) - 8
    early = [jnp.clip(budget - k * (devices // 2), 0, devices // 2) for k in range(sections)]
    make_maps([0] * sections, early)
    pl.semaphore_wait(barrier, devices - 1)
    for which, aways in ((0, (3, 2)), (7, (1, 0))):
        to_all(lambda d: small_send.at[d, side_part], small.at[me, side_part], which, aways)
    for which, aways in ((8, (1, 0)), (1, (3, 2))):
        to_all(lambda d: columns_at(v_ref, d), vals.at[me], which, aways)
    small[me] = small_send[me]
    vals[me] = columns_at(v_ref, me)[...]

    make_maps(early, [devices // 2] * sections)
    lanes_q = lax.broadcasted_iota(jnp.int32, (columns, LANES), 1)
    rows_q = lax.broadcasted_iota(jnp.int32, (columns, LANES), 0)

    def place(tile):
        return pl.ds(pl.multiple_of(tile * LANES, LANES), LANES)

    low_ids = lax.broadcasted_iota(jnp.int32, (LOW, LANES), 0).astype(F32).astype(BF16)
    high_ids = (lax.broadcasted_iota(jnp.int32, (HIGH * columns, LANES), 0) // columns).astype(F32).astype(BF16)
    one, nil = jnp.array(1.0, BF16), jnp.array(0.0, BF16)

    def make_hot(row_of, sign_of, begin, count):
        @pl.loop(0, count, unroll=2)
        def _(i):
            d = begin + i
            row = row_of(d)
            high = jnp.floor(row * (1.0 / LOW))
            low = jnp.broadcast_to((row - high * LOW).astype(BF16), (LOW, LANES))
            hot[:, place(d)] = jnp.where(low_ids == low, one, nil)
            flip = (1 - 2 * (d // halves)).astype(F32)
            sign = jnp.broadcast_to(((2.0 * sign_of(d) - 1.0) * flip).astype(BF16), (HIGH * columns, LANES))
            wide = jnp.broadcast_to(high.astype(BF16), (HIGH * columns, LANES))
            masks[d] = jnp.where(high_ids == wide, sign, nil)

    def place_values(d, at, value):
        top, rest = split(value)
        for g in range(HIGH):
            mask = masks[d, columns * g:columns * (g + 1), :]
            left[columns * g:columns * (g + 1), at] = top * mask
            left[columns * (HIGH + g):columns * (HIGH + g + 1), at] = rest * mask

    def sketch_product():
        points = left.shape[1] // 2
        o = [lax.dot_general(left[:, part], hot[:, part], (((1,), (1,)), ((), ())), preferred_element_type=F32)
             for part in (slice(0, points), slice(points, 2 * points))]
        return (o[0][:HIGH * columns] + o[0][HIGH * columns:]) - (o[1][:HIGH * columns] + o[1][HIGH * columns:])

    factor = math.sqrt(SKETCH / total_points)

    def start_reduce(sk, pieces, landed, which):
        for n in range(plane_size):
            pieces[n] = sk[columns * n:columns * (n + 1), :]
        to_plane(lambda n: pieces.at[n], landed.at[seat], which)
        landed[seat] = pieces[seat]

    def next_reduce(landed, total, joined, which, first):
        finish(landed.at[pl.ds(0, plane_size - 1)], first, 1)
        total[...] = jnp.sum(landed[...], axis=0)
        to_planes(total, joined.at[plane], which)
        joined[plane] = total[...]

    make_hot(lambda d: rows_ref[pl.ds(d, 1), :].astype(F32), lambda d: signs_ref[pl.ds(d, 1), :].astype(F32), 0, devices)

    @pl.loop(0, devices)
    def _(d):
        place_values(d, place(d), v_ref[:, place(d)])

    basis_sketch = sketch_product()
    start_reduce(basis_sketch, rb_send, rb_recv, 2)

    fx = (sub % 4 + 1).astype(F32)
    fy = (sub // 4 + 1).astype(F32)
    unit = 1.0 / math.sqrt(LEAF)
    point_masks = [jnp.where(lanes_q // LEAF == j, 1.0, 0.0).astype(BF16) for j in range(per_tile)]
    column_masks = [jnp.where((wide_lane % half) // columns == j, 1.0, 0.0).astype(BF16) for j in range(per_tile)]
    first_half = wide_lane < half

    def combine(o):
        s = o[0:32] + o[32:64]
        return s + pltpu.roll(s, half, 1)

    def expand(total):
        top = total.astype(BF16).astype(F32)
        y = jnp.where(first_half, top, total - top).astype(BF16)
        return jnp.concatenate([y * m for m in column_masks], axis=0)

    def leaves(begin):
        @pl.loop(0, halves, unroll=4)
        def _(i):
            d = begin + i
            pair = fold(small[d, 0:2, :].astype(jnp.int32) * scale).astype(F32)
            px, py = pair[0:1], pair[1:2]
            phases_of = [fx * px + (fy + 2.0 * t) * py for t in range(2)]
            full = jnp.concatenate([scaled_cos(n, unit) for n in phases_of] + [scaled_sin(n, unit) for n in phases_of], axis=0)
            top, low = split(full)
            leaf[d, 0:32] = top
            leaf[d, 32:64] = low

    def gather(begin):
        for i in range(halves):
            d = begin + i
            top, rest = split(vals[d])
            spread_v = jnp.concatenate([top * m for m in point_masks] + [rest * m for m in point_masks], axis=0)
            o = lax.dot_general(leaf[d], spread_v, (((1,), (1,)), ((), ())), preferred_element_type=F32)
            state[0, d] = expand(combine(o))

    def section(k, begin, count):
        stride = 2 ** k
        now = k % 2
        for i in range(count // 2):
            d0 = begin + (i // stride) * (2 * stride) + i % stride
            d1 = d0 + stride
            x = jnp.concatenate([state[now, d0], state[now, d1]], axis=0)
            o = jnp.dot(mats[k, begin // 2 + i], x, preferred_element_type=F32)
            for d, part in ((d0, o[0:64]), (d1, o[64:128])):
                total = combine(part)
                if k == sections - 1:
                    coef[32 * d:32 * d + 32, :] = total
                else:
                    state[1 - now, d] = expand(total)

    near, away = side * halves, (1 - side) * halves
    for begin, small_which, count in ((near, 7, halves - 1), (away, 0, halves)):
        finish(small.at[pl.ds(0, count), side_part], small_which, 1)
        leaves(begin)
        make_hot(lambda d: small[d, 3:4, :], lambda d: small[d, 4:5, :], begin, halves)
    for begin, vals_which, count in ((near, 8, halves - 1), (away, 1, halves)):
        arrived = pl.ds(0, count)
        finish(vals.at[arrived], vals_which, 1)
        gather(begin)
        for k in range(sections - 1):
            section(k, begin, halves)
    next_reduce(rb_recv, rb_total, rb_joined, 9, 2)
    section(sections - 1, 0, devices)
    tile_lane = lax.broadcasted_iota(jnp.int32, (half, 2 * LANES), 1)
    tile_masks = [jnp.where((tile_lane % LANES) // WIDTH == t, 1.0, 0.0).astype(BF16) for t in range(4)]
    zero = jnp.zeros((columns, LANES), F32)
    inner, square, energy = zero, zero, zero
    for g in range(devices // 4):
        flipped = coef[LANES * g:LANES * (g + 1), :].T
        top, rest = split(flipped[0:half])
        both = jnp.concatenate([top, rest], axis=1)
        lhs = jnp.concatenate([both * m for m in tile_masks], axis=0)
        tops = jnp.concatenate([leaf[4 * g + t, 0:32] for t in range(4)], axis=0)
        lows = jnp.concatenate([leaf[4 * g + t, 32:64] for t in range(4)], axis=0)
        right = jnp.concatenate([tops, lows], axis=1)
        o = jnp.dot(lhs, jnp.concatenate([right, right], axis=0), preferred_element_type=F32)
        o = o[:, 0:LANES] + o[:, LANES:2 * LANES]
        for t in range(4):
            d = 4 * g + t
            v = vals[d]
            img = jnp.broadcast_to(small[d, 2:3, :], (columns, LANES)) * v
            for j in range(per_tile):
                begin = half * t + columns * j
                img = img + jnp.where(lanes_q // LEAF == j, o[begin:begin + columns], 0.0)
            image[d] = img
            place_values(d, slice(LANES * d, LANES * (d + 1)), img)
            inner, square, energy = inner + v * img, square + v * v, energy + img * img

    to_all(lambda d: image.at[d], back.at[me], 5, (3, 2))
    packed = zero
    for i, value in enumerate((inner, square, energy)):
        packed = jnp.where(lanes_q == rows_q + columns * i, jnp.sum(value, axis=1, keepdims=True), packed)
    sum_send[...] = jnp.sum(packed, axis=0, keepdims=True)
    image_sketch = sketch_product()
    start_reduce(image_sketch, ri_send, ri_recv, 4)
    to_plane(lambda d: sum_send, sum_recv.at[seat], 3)
    sum_recv[seat] = sum_send[...]
    back[me] = image[me]

    finish(small_send.at[pl.ds(0, halves), side_part], 0, 0)
    finish(small_send.at[pl.ds(0, halves - 1), side_part], 7, 0)
    finish(vals.at[pl.ds(0, halves)], 1, 0)
    finish(vals.at[pl.ds(0, halves - 1)], 8, 0)
    finish(rb_send.at[mates], 2, 0)
    next_reduce(ri_recv, ri_total, ri_joined, 11, 4)
    to_all(lambda d: image.at[d], back.at[me], 5, (1, 0))
    finish(sum_recv.at[mates], 3, 1)
    sum_total[...] = jnp.sum(sum_recv[...], axis=0)
    to_planes(sum_total, sum_joined.at[plane], 10)
    sum_joined[plane] = sum_total[...]
    finish(rb_joined.at[peers], 9, 0)
    finish(rb_joined.at[peers], 9, 1)
    finish(sum_recv.at[mates], 3, 0)
    finish(ri_send.at[mates], 4, 0)
    basis_total = jnp.sum(rb_joined[...], axis=0)
    finish(sum_joined.at[peers], 10, 1)
    totals = jnp.sum(sum_joined[...], axis=0)

    def column(i):
        picked = jnp.where(lanes_q == rows_q + columns * i, jnp.broadcast_to(totals, (columns, LANES)), 0.0)
        return jnp.broadcast_to(jnp.sum(picked, axis=1, keepdims=True) * (1.0 / total_points), (columns, LANES))

    inner_mean, square_mean, energy_mean = column(0), column(1), column(2)
    projection = inner_mean / (square_mean + EPSILON)
    energy = energy_mean - 2.0 * projection * inner_mean + projection * projection * square_mean
    spread = jnp.sqrt(energy + EPSILON)
    inverse = 1.0 / spread
    for i, value in enumerate((projection, spread)):
        arn_ref[i:i + 1, :] = jnp.sum(jnp.where(lanes_q == rows_q, value, 0.0), axis=0, keepdims=True)[:, :columns]
    finish(ri_joined.at[peers], 11, 1)
    wide = lambda x: jnp.concatenate([x] * (LOW // LANES), axis=1)
    own_chunk[...] = (jnp.sum(ri_joined[...], axis=0) - basis_total * wide(projection)) * wide(factor * inverse)
    to_plane(lambda d: own_chunk, ag_recv.at[seat], 6)
    ag_recv[seat] = own_chunk[...]
    finish(back.at[others], 5, 1)
    for e in range(devices):
        here = slice(e * LANES, (e + 1) * LANES)
        nb_ref[:, here] = (back[e] - projection * v_ref[:, here]) * inverse
    finish(image.at[others], 5, 0)
    finish(ri_joined.at[peers], 11, 0)
    finish(sum_joined.at[peers], 10, 0)
    finish(ag_recv.at[mates], 6, 0)
    finish(ag_recv.at[mates], 6, 1)
    for n in range(plane_size):
        sketch_ref[:, LOW * n:LOW * (n + 1)] = ag_recv[n]


def deliver(*refs):
    copies = [pltpu.make_async_copy(refs[i], refs[3 + i], refs[6].at[i]) for i in range(3)]
    for copy in copies:
        copy.start()
    for copy in copies:
        copy.wait()


def together(devices, basis_vector, diagonal, coords, phase_scale, sketch_rows, sketch_signs):
    columns, local_points = basis_vector.shape
    sections = devices.bit_length() - 1
    plane = (local_points // LANES, LANES)
    far = pl.BlockSpec(memory_space=pltpu.HBM)
    vmem = pl.BlockSpec(memory_space=pltpu.VMEM)
    tile = pltpu.VMEM((devices, columns, LANES), F32)
    chunk = (columns, LOW)
    pieces = pltpu.VMEM((HIGH,) + chunk, F32)
    reduce_parts = [pieces, pieces, pltpu.VMEM(chunk, F32), pltpu.VMEM((devices // HIGH,) + chunk, F32)]
    results = pl.pallas_call(
        functools.partial(tile_kernel, devices, local_points * devices),
        out_shape=(
            jax.ShapeDtypeStruct((columns, local_points), F32),
            jax.ShapeDtypeStruct((columns, SKETCH), F32),
            jax.ShapeDtypeStruct((2, columns), F32)),
        in_specs=[pl.BlockSpec(memory_space=pltpu.SMEM)] + [far] * 5,
        out_specs=(vmem,) * 3,
        scratch_shapes=[
            pltpu.VMEM(basis_vector.shape, F32),
            pltpu.VMEM(coords.shape, jnp.int32),
            pltpu.VMEM(plane, F32),
            pltpu.VMEM(plane, jnp.int32),
            pltpu.VMEM(plane, jnp.int32),
            pltpu.VMEM((devices, 8, LANES), F32),
            pltpu.VMEM((devices, 8, LANES), F32),
            tile,
            pltpu.VMEM((2 * sections, devices, LANES), F32),
            pltpu.VMEM((2 * sections, devices, LANES), F32),
            pltpu.VMEM((sections, devices // 2, 4 * WIDTH, 2 * LANES), BF16),
            pltpu.VMEM((devices, 2 * WIDTH, LANES), BF16),
            pltpu.VMEM((2, devices, LANES, LANES), BF16),
            pltpu.VMEM((devices * WIDTH, LANES), F32),
            tile, tile,
            pltpu.VMEM((LOW, local_points), BF16),
            pltpu.VMEM((2 * HIGH * columns, local_points), BF16),
            pltpu.VMEM((devices, HIGH * columns, LANES), BF16),
            pltpu.VMEM((1, LANES), F32),
            pltpu.VMEM((HIGH, 1, LANES), F32),
            pltpu.VMEM((1, LANES), F32),
            pltpu.VMEM((devices // HIGH, 1, LANES), F32),
            *reduce_parts, *reduce_parts, pieces,
            pltpu.VMEM(chunk, F32),
            pltpu.SemaphoreType.DMA((24,)),
            pltpu.SemaphoreType.DMA((5,)),
        ],
        compiler_params=pltpu.CompilerParams(
            collective_id=0, has_side_effects=True, vmem_limit_bytes=24 * 2**20),
        name="gmres",
    )(phase_scale, *(pltpu.with_memory_space_constraint(x, pltpu.HBM) for x in (
        basis_vector, coords, diagonal.reshape(plane), sketch_rows.reshape(plane),
        sketch_signs.reshape(plane))))
    return pl.pallas_call(
        deliver,
        out_shape=[jax.ShapeDtypeStruct(x.shape, x.dtype) for x in results],
        in_specs=[vmem] * 3,
        out_specs=[far] * 3,
        scratch_shapes=[pltpu.SemaphoreType.DMA((3,))],
        compiler_params=pltpu.CompilerParams(vmem_limit_bytes=2**20),
        name="deliver",
    )(*results)


def body(basis_vector, diagonal, coords, phase_scale, sketch_rows, sketch_signs):
    columns, local_points = basis_vector.shape
    devices = lax.axis_size("box")
    if devices * LANES == local_points:
        return together(devices, basis_vector, diagonal, coords, phase_scale, sketch_rows, sketch_signs)
    sections = devices.bit_length() - 1
    count = -(-sections // 5)
    stages, low = [], 0
    for i in range(count):
        bits = (sections - low) // (count - i)
        stages.append((low, bits))
        low += bits
    group = 2 ** max(bits for _, bits in stages)
    group_rows = [columns * WIDTH // LANES * (LANES // 2 ** bits) for _, bits in stages]
    plane = (local_points // LANES, LANES)
    rows_each = HIGH * columns * LOW // LANES // devices
    vmem = pl.BlockSpec(memory_space=pltpu.VMEM)
    dma = pltpu.SemaphoreType.DMA
    count_rows = max(group_rows)
    halves = columns // 8
    new_basis, sketch, arn = pl.pallas_call(
        functools.partial(kernel, devices, stages, local_points * devices),
        out_shape=(
            jax.ShapeDtypeStruct((columns, local_points), F32),
            jax.ShapeDtypeStruct((columns, SKETCH), F32),
            jax.ShapeDtypeStruct((2, columns), F32)),
        in_specs=[pl.BlockSpec(memory_space=pltpu.SMEM), vmem, vmem, vmem, vmem, vmem],
        out_specs=(vmem, vmem, vmem),
        scratch_shapes=[
            pltpu.VMEM(((columns + 8) * LEAF, LANES), F32),
            pltpu.VMEM((columns + 8, LEAF, LANES), F32),
            pltpu.VMEM((LEAF, WIDTH, LANES), F32),
            pltpu.VMEM((2 * sections, WIDTH, WIDTH, LANES), F32),
            pltpu.VMEM((LEAF, columns, LANES), F32),
            pltpu.VMEM((columns * WIDTH, LANES), F32),
            pltpu.VMEM((columns * WIDTH, LANES), F32),
            pltpu.VMEM((columns * WIDTH // LANES, LANES, LANES), F32),
            pltpu.VMEM((2, LEAF, LANES), F32),
            pltpu.VMEM((LEAF // 4, LOW, 4 * LANES), BF16),
            pltpu.VMEM((2 * HIGH * columns, LOW), F32),
            pltpu.VMEM((2 * HIGH * columns, LOW), F32),
            pltpu.VMEM((count * halves, group, count_rows // halves, LANES), F32),
            pltpu.VMEM((count * halves, group, count_rows // halves, LANES), F32),
            pltpu.VMEM((count * halves, group, count_rows // halves, LANES), F32),
            pltpu.VMEM((count * halves, group, count_rows // halves, LANES), F32),
            pltpu.VMEM((1, LANES), F32),
            pltpu.VMEM((devices, 1, LANES), F32),
            pltpu.VMEM((devices, rows_each, LANES), F32),
            pltpu.VMEM((devices, rows_each, LANES), F32),
            pltpu.VMEM((devices, rows_each, LANES), F32),
            pltpu.VMEM((rows_each, LANES), F32),
            dma((count * halves, group)), dma((count * halves, group)), dma((count * halves, group)), dma((count * halves, group)),
            dma((devices,)), dma((devices,)), dma((devices,)), dma((devices,)), dma((devices,)), dma((devices,)),
        ],
        compiler_params=pltpu.CompilerParams(
            collective_id=0, has_side_effects=True, vmem_limit_bytes=60 * 2**20),
        name="gmres",
    )(phase_scale, basis_vector, coords, diagonal.reshape(plane), sketch_rows.reshape(plane),
      sketch_signs.reshape(plane))
    return new_basis, sketch, arn


def solution(mesh):
    placed = (P(None, "box"), P("box"), P(None, "box"), P(), P("box"), P("box"))
    return jax.shard_map(
        body, mesh=mesh, in_specs=placed, out_specs=(P(None, "box"), P(), P()), check_vma=False
    )
```
